32 devices in a mesh: rep: 2 (over y), shard: 16 (over z, x, core).
Axes of the slice: x: 2, y: 2, z: 4, core: 2. Of those that a mesh axis runs over, the one named last changes fastest.
Arguments:
- hidden: bfloat16 [8192, 1536], P(('rep', 'shard')), may hold values from -6 to 6
- text_states: bfloat16 [7, 64, 1536], replicated, may hold values from -6 to 6
- clip_index: int32 [8192], P(('rep', 'shard')), may hold values from 0 to 6, as said below
- frame_offset: int32 [8192], P(('rep', 'shard')), may hold values from 0 to 1279, as said below
- self_gain: bfloat16 [1536], P('shard'), may hold values from 0.5 to 1.5
- self_bias: bfloat16 [1536], P('shard'), may hold values from -2.5 to 2.5
- w_query: bfloat16 [1536, 1536], P('shard'), may hold values from -0.15625 to 0.15625
- w_key: bfloat16 [1536, 1536], P('shard'), may hold values from -0.15625 to 0.15625
- w_value: bfloat16 [1536, 1536], P('shard'), may hold values from -0.15625 to 0.15625
- w_output: bfloat16 [1536, 1536], P('shard'), may hold values from -1.75 to 1.75
- cross_gain: bfloat16 [1536], P('shard'), may hold values from 0.5 to 1.5
- cross_bias: bfloat16 [1536], P('shard'), may hold values from -2.5 to 2.5
- x_query: bfloat16 [1536, 1536], P('shard'), may hold values from -0.15625 to 0.15625
- x_key: bfloat16 [1536, 1536], P('shard'), may hold values from -0.15625 to 0.15625
- x_value: bfloat16 [1536, 1536], P('shard'), may hold values from -0.15625 to 0.15625
- x_output: bfloat16 [1536, 1536], P('shard'), may hold values from -0.625 to 0.625
- final_gain: bfloat16 [1536], P('shard'), may hold values from 0.5 to 1.5
- final_bias: bfloat16 [1536], P('shard'), may hold values from -2.5 to 2.5
- w_up: bfloat16 [1536, 6144], P('shard'), may hold values from -0.15625 to 0.15625
- w_down: bfloat16 [6144, 1536], P('shard'), may hold values from -0.078125 to 0.078125
- cotangent: bfloat16 [8192, 1536], P(('rep', 'shard')), may hold values from -6 to 6
Outputs:
- block_out: bfloat16 [8192, 1536], P(('rep', 'shard'))
- grad_hidden: bfloat16 [8192, 1536], P(('rep', 'shard'))
- grad_text: float32 [7, 64, 1536], replicated
- grad_self_gain: float32 [1536], P('shard')
- grad_self_bias: float32 [1536], P('shard')
- grad_w_query: float32 [1536, 1536], P('shard')
- grad_w_key: float32 [1536, 1536], P('shard')
- grad_w_value: float32 [1536, 1536], P('shard')
- grad_w_output: float32 [1536, 1536], P('shard')
- grad_cross_gain: float32 [1536], P('shard')
- grad_cross_bias: float32 [1536], P('shard')
- grad_x_query: float32 [1536, 1536], P('shard')
- grad_x_key: float32 [1536, 1536], P('shard')
- grad_x_value: float32 [1536, 1536], P('shard')
- grad_x_output: float32 [1536, 1536], P('shard')
- grad_final_gain: float32 [1536], P('shard')
- grad_final_bias: float32 [1536], P('shard')
- grad_w_up: float32 [1536, 6144], P('shard')
- grad_w_down: float32 [6144, 1536], P('shard')
The draws below stay inside these ranges and needn't reach their ends.
Inputs may be any that keep to these rules, and one draw needn't show every extreme that they name: `clip_index`: clip of each token in order: 0 at the first token, rising by one at each clip's first token. Every clip holds at most 1280 tokens, the first exactly 1280, and every clip but the last more than 256. `frame_offset`: position of each token inside its clip, counted from 0 at the clip's first token.
All inputs are finite; a program needn't handle non-finite values.
Results may differ from the reference program's by a relative error of at most 0.017.
Values may be sent and summed in bfloat16 or wider, within the bound.
A program may use at most 384 MiB of HBM per device.

```python
import jax
import jax.numpy as jnp
from jax import lax

D = 1536
HEADS = 24
HD = 64
FF = 6144
TEXT = 64
CLIP_MAX = 1280
TOK_DEV = 256
TOKENS = 8192
NCLIPS = 7
NEIGHBORS = 5


def clip_layout(key):
    clip_count = (TOKENS - 1) // CLIP_MAX + 1
    spare_rows = clip_count * CLIP_MAX - TOKENS
    shares = jax.random.randint(key, (clip_count,), 2, 4, dtype=jnp.int32)
    shares = jnp.where(jnp.arange(clip_count, dtype=jnp.int32) == 0, 0, shares)
    running = jnp.cumsum(shares)
    cut_marks = spare_rows * running // running[-1]
    prior_marks = jnp.concatenate([jnp.zeros((1,), jnp.int32), cut_marks[:-1]])
    lengths = CLIP_MAX - (cut_marks - prior_marks)
    clip_ends = jnp.cumsum(lengths)
    position = jnp.arange(TOKENS, dtype=jnp.int32)
    passed = position[:, None] >= clip_ends[None, :]
    clip_ids = jnp.sum(passed.astype(jnp.int32), axis=1)
    clip_begin = jnp.sum(jnp.where(passed, lengths[None, :], 0), axis=1)
    return (clip_ids, position - clip_begin)


def draw_clip_index(key, part):
    return clip_layout(jax.random.fold_in(key, 11))[0]


def draw_frame_offset(key, part):
    return clip_layout(jax.random.fold_in(key, 11))[1]


def block_scale(own_key, dims, pieces, low, high):
    gain = 1.0
    for axis_at, parts in pieces:
        heights = jax.random.uniform(jax.random.fold_in(jax.random.fold_in(own_key, 6), axis_at), (parts,), jnp.float32, low / len(pieces), high / len(pieces))
        gain = gain * jnp.repeat(jnp.exp(heights), dims[axis_at] // parts).reshape((-1,) + (1,) * (len(dims) - 1 - axis_at))
    return gain


def noise(rng, shape, scale, bound, cuts=(), kind=jnp.bfloat16):
    drawn = jax.random.normal(rng, shape, jnp.float32) * scale
    if len(cuts) > 0:
        drawn = block_scale(rng, shape, cuts, -0.22, 0.18) * drawn
    return jnp.clip(drawn, min=-bound, max=bound).astype(kind)


def setup_inputs(seed: int = 0) -> dict:
    key_list = jax.random.split(jax.random.key(seed), 22)
    hidden = noise(key_list[0], (TOKENS, D), 1.0, 6.0, ((0, 32),))
    text_states = noise(key_list[1], (NCLIPS, TEXT, D), 1.0, 6.0)
    clip_index = draw_clip_index(jax.random.fold_in(key_list[21], 71), 0)
    frame_offset = draw_frame_offset(jax.random.fold_in(key_list[21], 71), 0)
    self_gain = jnp.clip(1.0 + 0.1 * jax.random.normal(key_list[4], (D,), jnp.float32), 0.5, 1.5).astype(jnp.bfloat16)
    self_bias = noise(key_list[5], (D,), 0.5, 2.5, ((0, 16),))
    w_query = noise(key_list[6], (D, D), D ** -0.5, 0.15625, ((0, 16),))
    w_key = noise(key_list[7], (D, D), D ** -0.5, 0.15625, ((0, 16),))
    w_value = noise(key_list[8], (D, D), D ** -0.5, 0.15625, ((0, 16),))
    w_output = noise(key_list[9], (D, D), (max(D // 128, 1)) ** -0.5, 1.75, ((0, 16),))
    cross_gain = jnp.clip(1.0 + 0.1 * jax.random.normal(key_list[10], (D,), jnp.float32), 0.5, 1.5).astype(jnp.bfloat16)
    cross_bias = noise(key_list[11], (D,), 0.5, 2.5, ((0, 16),))
    x_query = noise(key_list[12], (D, D), D ** -0.5, 0.15625, ((0, 16),))
    x_key = noise(key_list[13], (D, D), D ** -0.5, 0.15625, ((0, 16),))
    x_value = noise(key_list[14], (D, D), D ** -0.5, 0.15625, ((0, 16),))
    x_output = noise(key_list[15], (D, D), (max(D // 16, 1)) ** -0.5, 0.625, ((0, 16),))
    final_gain = jnp.clip(1.0 + 0.1 * jax.random.normal(key_list[16], (D,), jnp.float32), 0.5, 1.5).astype(jnp.bfloat16)
    final_bias = noise(key_list[17], (D,), 0.5, 2.5, ((0, 16),))
    w_up = noise(key_list[18], (D, FF), D ** -0.5, 0.15625, ((0, 16),))
    w_down = noise(key_list[19], (FF, D), FF ** -0.5, 0.078125, ((0, 16),))
    cotangent = noise(key_list[20], (TOKENS, D), 1.0, 6.0, ((0, 32),))
    return dict(hidden=hidden, text_states=text_states, clip_index=clip_index, frame_offset=frame_offset, self_gain=self_gain, self_bias=self_bias, w_query=w_query, w_key=w_key, w_value=w_value, w_output=w_output, cross_gain=cross_gain, cross_bias=cross_bias, x_query=x_query, x_key=x_key, x_value=x_value, x_output=x_output, final_gain=final_gain, final_bias=final_bias, w_up=w_up, w_down=w_down, cotangent=cotangent)


@jax.custom_vjp
def low(v):
    return lax.optimization_barrier(v.astype(jnp.bfloat16)).astype(jnp.float32)

@jax.custom_vjp
def low_back(v):
    return v

def low_keep(v):
    return (low(v), None)

def low_pass(kept, grad):
    return (grad,)

def back_keep(v):
    return (v, None)

def back_low(kept, grad):
    return (low(grad),)
low.defvjp(low_keep, low_pass)
low_back.defvjp(back_keep, back_low)
EPSILON = 1e-05
NEGATIVE = -1e+30

def layer_norm(values, scale_vec, bias_vec):
    centre = values - lax.optimization_barrier(jnp.mean(values, axis=-1, keepdims=True))
    spread = lax.optimization_barrier(jnp.mean(centre * centre, axis=-1, keepdims=True))
    return centre * lax.rsqrt(spread + EPSILON) * scale_vec + bias_vec

def matmul(left, right):
    return jnp.dot(left, right, precision=lax.Precision.HIGHEST, preferred_element_type=jnp.float32)

def both_round(values):
    return low_back(low(values))

def self_attention(queries, keys_in, values_in, offsets):
    context = (NEIGHBORS + 1) * TOK_DEV
    padding = jnp.zeros((NEIGHBORS * TOK_DEV, D), jnp.float32)
    keys_all = jnp.concatenate([padding, keys_in], axis=0)
    values_all = jnp.concatenate([padding, values_in], axis=0)
    row_index = jnp.arange(TOK_DEV, dtype=jnp.int32)[:, None]
    col_index = jnp.arange(context, dtype=jnp.int32)[None, :]
    distance = row_index + NEIGHBORS * TOK_DEV - col_index
    key_scale = HD ** (-0.5)

    def block(index):
        start = (index * TOK_DEV).astype(jnp.int32)
        query_blk = lax.dynamic_slice_in_dim(queries, start, TOK_DEV, 0).reshape(TOK_DEV, HEADS, HD)
        key_blk = lax.dynamic_slice_in_dim(keys_all, start, context, 0).reshape(context, HEADS, HD)
        value_blk = lax.dynamic_slice_in_dim(values_all, start, context, 0).reshape(context, HEADS, HD)
        offset_blk = lax.dynamic_slice_in_dim(offsets, start, TOK_DEV, 0)
        allowed = (distance >= 0) & (distance <= offset_blk[:, None])
        scores = low_back(jnp.einsum('thd,khd->htk', query_blk, key_blk, precision=lax.Precision.HIGHEST) * key_scale)
        scores = jnp.where(allowed[None], scores, NEGATIVE)
        probs = jax.nn.softmax(scores, axis=2)
        mixed = jnp.einsum('htk,khd->thd', low(probs), value_blk, precision=lax.Precision.HIGHEST)
        return mixed.reshape(TOK_DEV, D)
    blocks = lax.map(jax.checkpoint(block), jnp.arange(TOKENS // TOK_DEV, dtype=jnp.int32))
    return blocks.reshape(TOKENS, D)

def cross_attention(queries, text_keys, text_values, clips):
    key_scale = HD ** (-0.5)
    slot = jnp.arange(2 * TEXT, dtype=jnp.int32) // TEXT

    def block(index):
        start = (index * TOK_DEV).astype(jnp.int32)
        query_blk = lax.dynamic_slice_in_dim(queries, start, TOK_DEV, 0).reshape(TOK_DEV, HEADS, HD)
        clip_blk = lax.dynamic_slice_in_dim(clips, start, TOK_DEV, 0)
        first = clip_blk[0]
        second = jnp.minimum(first + 1, NCLIPS - 1)
        key_blk = jnp.concatenate([lax.dynamic_index_in_dim(text_keys, first, 0, False), lax.dynamic_index_in_dim(text_keys, second, 0, False)], axis=0).reshape(2 * TEXT, HEADS, HD)
        value_blk = jnp.concatenate([lax.dynamic_index_in_dim(text_values, first, 0, False), lax.dynamic_index_in_dim(text_values, second, 0, False)], axis=0).reshape(2 * TEXT, HEADS, HD)
        slot_clip = jnp.where(slot == 0, first, second)
        open_slot = (slot == 0) | (second != first)
        allowed = (clip_blk[:, None] == slot_clip[None, :]) & open_slot[None, :]
        scores = low_back(jnp.einsum('thd,khd->htk', query_blk, key_blk, precision=lax.Precision.HIGHEST) * key_scale)
        scores = jnp.where(allowed[None], scores, NEGATIVE)
        probs = jax.nn.softmax(scores, axis=2)
        mixed = jnp.einsum('htk,khd->thd', low(probs), value_blk, precision=lax.Precision.HIGHEST)
        return mixed.reshape(TOK_DEV, D)
    blocks = lax.map(jax.checkpoint(block), jnp.arange(TOKENS // TOK_DEV, dtype=jnp.int32))
    return blocks.reshape(TOKENS, D)

def reference(hidden, text_states, clip_index, frame_offset, self_gain, self_bias, w_query, w_key, w_value, w_output, cross_gain, cross_bias, x_query, x_key, x_value, x_output, final_gain, final_bias, w_up, w_down, cotangent):
    floats = [arr.astype(jnp.float32) for arr in (hidden, text_states, self_gain, self_bias, w_query, w_key, w_value, w_output, cross_gain, cross_bias, x_query, x_key, x_value, x_output, final_gain, final_bias, w_up, w_down)]

    def forward(resid, texts_in, gain_one, bias_one, wq_in, wk_in, wv_in, wo_in, gain_two, bias_two, cq_in, ck_in, cv_in, co_in, gain_three, bias_three, up_in, down_in):
        normed_one = low(layer_norm(resid, gain_one, bias_one))
        queries = both_round(matmul(normed_one, wq_in))
        keys_in = both_round(matmul(normed_one, wk_in))
        values_in = both_round(matmul(normed_one, wv_in))
        attended = both_round(self_attention(queries, keys_in, values_in, frame_offset))
        after_self = resid + low_back(matmul(attended, wo_in))
        normed_two = low(layer_norm(after_self, gain_two, bias_two))
        cross_q = both_round(matmul(normed_two, cq_in))
        text_flat = texts_in.reshape(NCLIPS * TEXT, D)
        cross_k = both_round(matmul(text_flat, ck_in)).reshape(NCLIPS, TEXT, D)
        cross_v = both_round(matmul(text_flat, cv_in)).reshape(NCLIPS, TEXT, D)
        cross_mix = both_round(cross_attention(cross_q, cross_k, cross_v, clip_index))
        after_cross = after_self + low_back(matmul(cross_mix, co_in))
        normed_three = low(layer_norm(after_cross, gain_three, bias_three))
        pre_act = low_back(matmul(normed_three, up_in))
        activ = low(jax.nn.gelu(pre_act, approximate=False))
        return after_cross + low_back(matmul(activ, down_in))
    result, pull = jax.vjp(forward, *floats)
    grads = pull(cotangent.astype(jnp.float32))
    return (result.astype(jnp.bfloat16), grads[0].astype(jnp.bfloat16), grads[1], grads[2], grads[3], grads[4], grads[5], grads[6], grads[7], grads[8], grads[9], grads[10], grads[11], grads[12], grads[13], grads[14], grads[15], grads[16], grads[17])
```

```python
import functools

import jax
import jax.numpy as jnp
from jax import lax
from jax.experimental import pallas as pl
from jax.experimental.pallas import tpu as pltpu
from jax.sharding import PartitionSpec as P

HD = 64
CLIP_MAX = 1280
EPSILON = 1e-05
NEGATIVE = -1e30
BLOCK = 256
BOTH = ("rep", "shard")
LOW = jnp.bfloat16
WIDE = jnp.float32


def normalize(values):
    centre = values - jnp.mean(values, axis=-1, keepdims=True)
    spread = jnp.mean(centre * centre, axis=-1, keepdims=True)
    return centre * lax.rsqrt(spread + EPSILON)


def scaled_norm(values, scale_vec):
    return normalize(values) * scale_vec


def exact_gelu(values):
    return jax.nn.gelu(values, approximate=False)


def matmul(left, right):
    return jnp.dot(left, right, preferred_element_type=WIDE)


def left_t(left, right):
    return lax.dot_general(left, right, (((0,), (0,)), ((), ())), preferred_element_type=WIDE)


def right_t(left, right):
    return lax.dot_general(left, right, (((1,), (1,)), ((), ())), preferred_element_type=WIDE)


def norm_back(values, scale_vec, upstream):
    _, pull = jax.vjp(scaled_norm, values, scale_vec.astype(WIDE))
    grad_values, grad_scale = pull(upstream)
    return (grad_values, grad_scale, jnp.sum(upstream, axis=0))


def pick(array, index, axis):
    return lax.dynamic_index_in_dim(array, index, axis, False)


def axis_length(axis):
    return lax.axis_size(axis)


def swap(array, axis, pairing):
    length = axis_length(axis)
    pairs = [(i, pairing(i)) for i in range(length)]
    return lax.ppermute(array, axis, [(i, j) for i, j in pairs if 0 <= j < length])


def add_low(left, right):
    return (left.astype(WIDE) + right.astype(WIDE)).astype(LOW)


def gather_rows(array):
    return lax.all_gather(array, "shard", axis=0, tiled=True)


def joined(parts):
    return parts[0] if len(parts) == 1 else jnp.concatenate(parts, axis=-1)


def staged_total(grads):
    index = lax.axis_index("shard")
    core, side, level, rep = index % 2, (index // 2) % 2, index // 4, lax.axis_index("rep")
    rows = grads[0].shape[0] // 16
    parts = [grad.reshape(8, 2, rows, grad.shape[1]) for grad in grads]
    away = joined([pick(part, 1 - core, 1) for part in parts])
    held = joined([pick(part, core, 1) for part in parts])
    width = held.shape[-1]
    half = width // 2
    held = add_low(held, swap(away, "shard", lambda i: i ^ 1))
    held = held.reshape(4, 2, rows, width)
    first = held[..., :half]
    first = add_low(
        pick(first, side, 1),
        swap(pick(first, 1 - side, 1), "shard", lambda i: i ^ 2),
    ).reshape(4, 2, rows // 2, half)
    second = held[..., half:].reshape(4, 2, 2, rows // 2, width - half)
    second = add_low(
        pick(second, rep, 2),
        swap(pick(second, 1 - rep, 2), "rep", lambda i: i ^ 1),
    )
    first = add_low(pick(first, rep, 1), swap(pick(first, 1 - rep, 1), "rep", lambda i: i ^ 1))
    second = add_low(
        pick(second, side, 1),
        swap(pick(second, 1 - side, 1), "shard", lambda i: i ^ 2),
    )
    both = jnp.concatenate([first, second], axis=2)
    total = pick(both, level, 0).astype(WIDE)
    for step in range(1, 4):
        total = total + swap(
            pick(both, (level + step) % 4, 0), "shard", lambda i: (i + 4 * step) % 16
        ).astype(WIDE)
    own = total.astype(LOW)
    other = swap(own, "rep", lambda i: i ^ 1)
    low, high = jnp.where(rep == 0, own, other), jnp.where(rep == 0, other, own)
    return jnp.concatenate([low, high], axis=0).astype(WIDE)


def summed_rows(grads):
    grads = [grad.astype(LOW) for grad in grads]
    widths = [grad.shape[1] for grad in grads]
    if axis_length("shard") == 16 and axis_length("rep") == 2:
        whole = staged_total(grads)
    else:
        share = lax.psum_scatter(joined(grads), "shard", scatter_dimension=0, tiled=True)
        whole = lax.psum(share.astype(WIDE), "rep")
    out, start = [], 0
    for width in widths:
        out.append(whole[:, start : start + width])
        start += width
    return out


def summed_vectors(stack):
    if axis_length("shard") != 16 or axis_length("rep") != 2:
        return lax.psum(stack, BOTH)
    for bit in (1, 2, 4, 8):
        stack = stack + swap(stack, "shard", lambda i: i ^ bit)
    return stack + swap(stack, "rep", lambda i: i ^ 1)


def head_lanes(which):
    lane = lax.broadcasted_iota(jnp.int32, (BLOCK, 2 * HD), 1)
    return lane < HD if which == 0 else lane >= HD


def open_pairs(offsets, step, reach):
    base = (reach - step) * BLOCK
    keys = lax.broadcasted_iota(jnp.int32, (BLOCK, BLOCK), 0)
    column = lax.broadcasted_iota(jnp.int32, (1, BLOCK), 1)
    allowed = keys >= (column - offsets) + base
    if base == 0:
        allowed = allowed & (keys <= lax.broadcasted_iota(jnp.int32, (BLOCK, BLOCK), 1))
    return allowed


def attend_kernel(reach, offset_ref, query_ref, window_ref, out_ref, log_ref, held):
    start = pl.program_id(1) * BLOCK
    offsets = offset_ref[...]
    scaled = query_ref[...] * jnp.asarray(HD**-0.5, LOW)
    mixed = []
    for head in range(2):
        query = jnp.where(head_lanes(head), scaled, jnp.zeros_like(scaled))
        peak = jnp.full((1, BLOCK), NEGATIVE, WIDE)
        for step in range(reach + 1):
            rows = pl.ds(pl.multiple_of(start + step * BLOCK, BLOCK), BLOCK)
            scores = right_t(window_ref[0, rows, :], query)
            scores = jnp.where(open_pairs(offsets, step, reach), scores, NEGATIVE)
            held[head, step] = scores
            peak = jnp.maximum(peak, jnp.max(scores, axis=0, keepdims=True))
        total = jnp.zeros((1, BLOCK), WIDE)
        blend = jnp.zeros((2 * HD, BLOCK), WIDE)
        for step in range(reach + 1):
            rows = pl.ds(pl.multiple_of(start + step * BLOCK, BLOCK), BLOCK)
            expo = jnp.exp(held[head, step] - peak)
            total = total + jnp.sum(expo, axis=0, keepdims=True)
            blend = blend + left_t(window_ref[1, rows, :], expo.astype(LOW))
        mixed.append((blend / total)[head * HD : (head + 1) * HD])
        log_ref[0, pl.ds(head, 1), :] = peak + jnp.log(total)
    out_ref[...] = jnp.concatenate(mixed, axis=0).T.astype(LOW)


def attend(offsets, queries, window, reach):
    rows, width = queries.shape
    pairs, blocks, context = width // (2 * HD), rows // BLOCK, window.shape[1]
    work = pairs * 2 * rows * (reach + 1) * BLOCK
    return pl.pallas_call(
        functools.partial(attend_kernel, reach),
        grid=(pairs, blocks),
        in_specs=[
            pl.BlockSpec((1, BLOCK), lambda p, b: (0, b)),
            pl.BlockSpec((BLOCK, 2 * HD), lambda p, b: (b, p)),
            pl.BlockSpec((2, context, 2 * HD), lambda p, b: (0, 0, p)),
        ],
        out_specs=[
            pl.BlockSpec((BLOCK, 2 * HD), lambda p, b: (b, p)),
            pl.BlockSpec((1, 2, BLOCK), lambda p, b: (p, 0, b)),
        ],
        out_shape=[
            jax.ShapeDtypeStruct((rows, width), LOW),
            jax.ShapeDtypeStruct((pairs, 2, rows), WIDE),
        ],
        scratch_shapes=[pltpu.VMEM((2, reach + 1, BLOCK, BLOCK), WIDE)],
        cost_estimate=pl.CostEstimate(
            flops=16 * HD * work, transcendentals=work, bytes_accessed=8 * rows * width
        ),
        name="attend_forward",
    )(offsets, queries, window)


def attend_back_kernel(
    reach,
    offset_ref,
    query_ref,
    window_ref,
    out_ref,
    log_ref,
    grad_ref,
    grad_query_ref,
    grad_window_ref,
    grad_keys,
    grad_values,
):
    block = pl.program_id(1)
    start = block * BLOCK

    @pl.when(block == 0)
    def _():
        grad_keys[...] = jnp.zeros_like(grad_keys)
        grad_values[...] = jnp.zeros_like(grad_values)

    offsets = offset_ref[...]
    scaled = query_ref[...] * jnp.asarray(HD**-0.5, LOW)
    grads = grad_ref[...]
    inner = (grads.astype(WIDE) * out_ref[...].astype(WIDE)).T
    query, grad, inners, logs = [], [], [], []
    for head in range(2):
        lanes = head_lanes(head)
        query.append(jnp.where(lanes, scaled, jnp.zeros_like(scaled)))
        grad.append(jnp.where(lanes, grads, jnp.zeros_like(grads)))
        inners.append(jnp.sum(inner[head * HD : (head + 1) * HD], axis=0, keepdims=True))
        logs.append(log_ref[0, pl.ds(head, 1), :])
    back = [jnp.zeros((2 * HD, BLOCK), WIDE) for _ in range(2)]
    for step in range(reach + 1):
        rows = pl.ds(pl.multiple_of(start + step * BLOCK, BLOCK), BLOCK)
        key, value = window_ref[0, rows, :], window_ref[1, rows, :]
        allowed = open_pairs(offsets, step, reach)
        to_key = jnp.zeros((BLOCK, 2 * HD), WIDE)
        to_value = jnp.zeros((BLOCK, 2 * HD), WIDE)
        for head in range(2):
            scores = jnp.where(allowed, right_t(key, query[head]), NEGATIVE)
            probs = jnp.exp(scores - logs[head])
            to_value = to_value + matmul(probs.astype(LOW), grad[head])
            grad_probs = right_t(value, grad[head])
            grad_scores = (probs * (grad_probs - inners[head])).astype(LOW)
            to_key = to_key + matmul(grad_scores, query[head])
            back[head] = back[head] + left_t(key, grad_scores)
        grad_keys[rows, :] += to_key
        grad_values[rows, :] += to_value
    back = jnp.concatenate([back[0][:HD], back[1][HD:]], axis=0) * (HD**-0.5)
    grad_query_ref[...] = back.T.astype(LOW)

    @pl.when(block == pl.num_programs(1) - 1)
    def _():
        grad_window_ref[0] = grad_keys[...].astype(LOW)
        grad_window_ref[1] = grad_values[...].astype(LOW)


def attend_back(offsets, queries, window, out, logs, grads, reach):
    rows, width = queries.shape
    pairs, blocks, context = width // (2 * HD), rows // BLOCK, window.shape[1]
    work = pairs * 2 * rows * (reach + 1) * BLOCK
    row_block = pl.BlockSpec((BLOCK, 2 * HD), lambda p, b: (b, p))
    window_block = pl.BlockSpec((2, context, 2 * HD), lambda p, b: (0, 0, p))
    return pl.pallas_call(
        functools.partial(attend_back_kernel, reach),
        grid=(pairs, blocks),
        in_specs=[
            pl.BlockSpec((1, BLOCK), lambda p, b: (0, b)),
            row_block,
            window_block,
            row_block,
            pl.BlockSpec((1, 2, BLOCK), lambda p, b: (p, 0, b)),
            row_block,
        ],
        out_specs=[row_block, window_block],
        out_shape=[
            jax.ShapeDtypeStruct((rows, width), LOW),
            jax.ShapeDtypeStruct(window.shape, LOW),
        ],
        scratch_shapes=[
            pltpu.VMEM((context, 2 * HD), WIDE),
            pltpu.VMEM((context, 2 * HD), WIDE),
        ],
        cost_estimate=pl.CostEstimate(
            flops=40 * HD * work, transcendentals=work, bytes_accessed=16 * rows * width
        ),
        name="attend_backward",
    )(offsets, queries, window, out, logs, grads)


def core_pair(own, got, core, axis):
    return jnp.where(
        core == 0,
        jnp.concatenate([own, got], axis=axis),
        jnp.concatenate([got, own], axis=axis),
    )


def on_device(
    hidden,
    text_states,
    clip_index,
    frame_offset,
    self_gain,
    self_bias,
    w_query,
    w_key,
    w_value,
    w_output,
    cross_gain,
    cross_bias,
    x_query,
    x_key,
    x_value,
    x_output,
    final_gain,
    final_bias,
    w_up,
    w_down,
    cotangent,
):
    tok_rows, model_width = hidden.shape
    head_count = model_width // HD
    half_width = model_width // 2
    reach = (CLIP_MAX - 2) // tok_rows + 1
    key_scale = HD ** (-0.5)
    clip_total = text_states.shape[0]
    text_rows = text_states.shape[1]
    shard_count, rep_count = axis_length("shard"), axis_length("rep")
    device_count = shard_count * rep_count
    place = lax.axis_index("rep") * shard_count + lax.axis_index("shard")
    core, side = place % 2, (place // 2) % 2

    params = jnp.stack(
        [self_gain, self_bias, cross_gain, cross_bias, final_gain, final_bias], axis=1
    )
    params = jnp.pad(params, ((0, 0), (0, 128 - params.shape[1])))
    split = [w[:, h : h + half_width] for h in (0, half_width) for w in (w_query, w_key, w_value)]
    first_group = gather_rows(jnp.concatenate(split + [params], axis=1))
    full_qkv = first_group[:, : 3 * model_width]
    gain_one, bias_one, gain_two, bias_two, gain_three, bias_three = (
        first_group[:, 3 * model_width + i].astype(WIDE) for i in range(6)
    )
    second_group = gather_rows(
        jnp.concatenate([w_output, x_query, x_key, x_value, x_output], axis=1)
    )
    full_output, full_xquery, full_xkey, full_xvalue, full_xoutput = (
        second_group[:, i * model_width : (i + 1) * model_width] for i in range(5)
    )
    full_up = gather_rows(w_up)
    full_down = gather_rows(w_down)

    offsets = core_pair(frame_offset, swap(frame_offset, BOTH, lambda i: i ^ 1), core, 0)[None, :]
    resid = hidden.astype(WIDE)
    normed_one = (scaled_norm(resid, gain_one) + bias_one).astype(LOW)
    projected = matmul(normed_one, full_qkv)
    projected = projected.astype(LOW).reshape(tok_rows, 2, 3, half_width)
    projected = jnp.transpose(projected, (1, 2, 0, 3))
    got = swap(pick(projected, 1 - core, 0), BOTH, lambda i: i ^ 1)
    chip_qkv = core_pair(pick(projected, core, 0), got, core, 1)
    queries, own_unit = chip_qkv[0], chip_qkv[1:]
    below = swap(own_unit, BOTH, lambda i: i + 4)
    far = swap(own_unit[:, tok_rows:], BOTH, lambda i: i + 8 if i % 4 >= 2 else -1)
    message = jnp.concatenate(
        [
            jnp.where(side == 0, own_unit, below),
            jnp.where(side == 0, below[:, tok_rows:], far),
        ],
        axis=1,
    )
    across = swap(message, BOTH, lambda i: i ^ 2)
    chip_rows = 2 * tok_rows
    window = jnp.concatenate(
        [across[:, chip_rows:], below, across[:, :chip_rows], own_unit], axis=1
    )
    chip_mixed, logs = attend(offsets, queries, window, reach)

    def to_tokens(chip_rows_array):
        mine = lax.dynamic_slice_in_dim(chip_rows_array, core * tok_rows, tok_rows, 0)
        away = lax.dynamic_slice_in_dim(chip_rows_array, (1 - core) * tok_rows, tok_rows, 0)
        return core_pair(mine, swap(away, BOTH, lambda i: i ^ 1), core, 1)

    attended = to_tokens(chip_mixed)
    after_self = resid + matmul(attended, full_output)
    normed_two = (scaled_norm(after_self, gain_two) + bias_two).astype(LOW)
    cross_q = matmul(normed_two, full_xquery).astype(LOW)
    first = clip_index[0]
    second = jnp.minimum(first + 1, clip_total - 1)
    chosen = jnp.concatenate(
        [
            lax.dynamic_index_in_dim(text_states, first, 0, False),
            lax.dynamic_index_in_dim(text_states, second, 0, False),
        ],
        axis=0,
    )
    cross_k = matmul(chosen, full_xkey).astype(LOW)
    cross_v = matmul(chosen, full_xvalue).astype(LOW)
    slot = jnp.arange(2 * text_rows, dtype=jnp.int32) // text_rows
    slot_clip = jnp.where(slot == 0, first, second)
    open_slot = (slot == 0) | (second != first)
    cross_mask = (clip_index[:, None] == slot_clip[None, :]) & open_slot[None, :]
    cq_heads = cross_q.reshape(tok_rows, head_count, HD)
    ck_heads = cross_k.reshape(2 * text_rows, head_count, HD)
    cv_heads = cross_v.reshape(2 * text_rows, head_count, HD)
    cross_scores = (
        jnp.einsum("thd,khd->htk", cq_heads, ck_heads, preferred_element_type=WIDE) * key_scale
    )
    cross_scores = jnp.where(cross_mask[None], cross_scores, NEGATIVE)
    cross_probs = jax.nn.softmax(cross_scores, axis=2)
    cross_low = cross_probs.astype(LOW)
    cross_mix = (
        jnp.einsum("htk,khd->thd", cross_low, cv_heads, preferred_element_type=WIDE)
        .reshape(tok_rows, model_width)
        .astype(LOW)
    )
    after_cross = after_self + matmul(cross_mix, full_xoutput)
    normed_three = (scaled_norm(after_cross, gain_three) + bias_three).astype(LOW)
    pre_act = matmul(normed_three, full_up)
    activ = exact_gelu(pre_act).astype(LOW)
    grad_down = left_t(activ, cotangent)
    (fin_down,) = summed_rows([grad_down])
    block_out = (after_cross + matmul(activ, full_down)).astype(LOW)
    grad_act = right_t(cotangent, full_down)
    _, gelu_pull = jax.vjp(exact_gelu, pre_act)
    grad_pre = gelu_pull(grad_act)[0].astype(LOW)
    grad_up = left_t(normed_three, grad_pre)
    (fin_up,) = summed_rows([grad_up])
    grad_norm_three = right_t(grad_pre, full_up)
    norm_three_part, grad_gain_three, grad_bias_three = norm_back(
        after_cross, gain_three, grad_norm_three
    )
    grad_cross_res = cotangent.astype(WIDE) + norm_three_part
    branch_two = grad_cross_res.astype(LOW)
    grad_xoutput = left_t(cross_mix, branch_two)
    grad_cmix = right_t(branch_two, full_xoutput).astype(LOW)
    grad_cmix = grad_cmix.reshape(tok_rows, head_count, HD)
    grad_cprob = jnp.einsum("thd,khd->htk", grad_cmix, cv_heads, preferred_element_type=WIDE)
    cross_inner = jnp.sum(cross_probs * grad_cprob, axis=2, keepdims=True)
    grad_cscore = (cross_probs * (grad_cprob - cross_inner)).astype(LOW)
    grad_cq = (
        (jnp.einsum("htk,khd->thd", grad_cscore, ck_heads, preferred_element_type=WIDE) * key_scale)
        .reshape(tok_rows, model_width)
        .astype(LOW)
    )
    grad_ck = (
        jnp.einsum("htk,thd->khd", grad_cscore, cq_heads, preferred_element_type=WIDE) * key_scale
    ).reshape(2 * text_rows, model_width)
    grad_cv = jnp.einsum(
        "htk,thd->khd", cross_low, grad_cmix, preferred_element_type=WIDE
    ).reshape(2 * text_rows, model_width)
    grad_xquery = left_t(normed_two, grad_cq)
    grad_norm_two = right_t(grad_cq, full_xquery)
    norm_two_part, grad_gain_two, grad_bias_two = norm_back(after_self, gain_two, grad_norm_two)
    grad_self_res = grad_cross_res + norm_two_part
    branch_one = grad_self_res.astype(LOW)
    grad_output = left_t(attended, branch_one)
    fin_xoutput, fin_xquery, fin_output = summed_rows([grad_xoutput, grad_xquery, grad_output])

    slots = jnp.arange(clip_total, dtype=jnp.int32)
    in_first = (slots == first).astype(WIDE)[None, :, None, None]
    in_second = (slots == second).astype(WIDE)[None, :, None, None]
    pair = jnp.stack([grad_ck, grad_cv]).reshape(2, 2, text_rows, model_width)
    sums = (pair[:, None, 0] * in_first + pair[:, None, 1] * in_second).astype(LOW)
    sums = sums.reshape(2 * clip_total * text_rows, model_width)
    text_total = sums.shape[0]
    padded = -(-text_total // (16 * device_count)) * 16 * device_count
    sums = jnp.pad(sums, ((0, padded - text_total), (0, 0)))
    share = lax.psum_scatter(sums, BOTH, scatter_dimension=0, tiled=True)
    sums = lax.all_gather(share, BOTH, axis=0, tiled=True)
    flat_rows = clip_total * text_rows
    key_round, value_round = sums[:flat_rows], sums[flat_rows:text_total]
    shard_rows = x_key.shape[0]
    col_start = lax.axis_index("shard") * shard_rows
    text_flat = text_states.reshape(flat_rows, model_width)
    text_slice = lax.dynamic_slice_in_dim(text_flat, col_start, shard_rows, 1)
    grad_xkey = left_t(text_slice, key_round)
    grad_xvalue = left_t(text_slice, value_round)
    grad_text = right_t(key_round, full_xkey) + right_t(value_round, full_xvalue)
    grad_text = grad_text.reshape(clip_total, text_rows, model_width)

    grad_attended = right_t(branch_one, full_output).astype(LOW)
    halves = jnp.transpose(grad_attended.reshape(tok_rows, 2, half_width), (1, 0, 2))
    chip_grad = core_pair(
        pick(halves, core, 0),
        swap(pick(halves, 1 - core, 0), BOTH, lambda i: i ^ 1),
        core,
        0,
    )
    chip_dq, grad_window = attend_back(offsets, queries, window, chip_mixed, logs, chip_grad, reach)
    far_part = grad_window[:, :tok_rows]
    below_part = grad_window[:, tok_rows : tok_rows + chip_rows]
    across_part = grad_window[:, tok_rows + chip_rows : tok_rows + 2 * chip_rows]
    own_part = grad_window[:, tok_rows + 2 * chip_rows :]
    back = swap(jnp.concatenate([across_part, far_part], axis=1), BOTH, lambda i: i ^ 2)
    back_unit, back_half = back[:, :chip_rows], back[:, chip_rows:]
    nothing = jnp.zeros_like(back_half)
    low_half = jnp.concatenate([nothing, back_half], axis=1)
    to_below = add_low(below_part, jnp.where(side == 0, low_half, back_unit))
    own_sum = own_part.astype(WIDE) + jnp.where(side == 0, back_unit, jnp.zeros_like(back_unit))
    own_sum = own_sum + swap(to_below, BOTH, lambda i: i - 4).astype(WIDE)
    from_far = swap(back_half, BOTH, lambda i: i - 8 if i % 4 >= 2 else -1)
    own_sum = own_sum + jnp.concatenate([nothing, from_far], axis=1).astype(WIDE)
    chip_grads = jnp.concatenate([chip_dq[None], own_sum.astype(LOW)], axis=0)
    mine = lax.dynamic_slice_in_dim(chip_grads, core * tok_rows, tok_rows, 1)
    away = lax.dynamic_slice_in_dim(chip_grads, (1 - core) * tok_rows, tok_rows, 1)
    got = swap(away, BOTH, lambda i: i ^ 1)
    pieces = core_pair(mine, got, core, 0)
    grad_qkv = jnp.concatenate([pieces[i] for i in range(6)], axis=1)
    grad_weights = left_t(normed_one, grad_qkv)
    (fin_qkv,) = summed_rows([grad_weights])
    grad_norm_one = right_t(grad_qkv, full_qkv)
    norm_one_part, grad_gain_one, grad_bias_one = norm_back(resid, gain_one, grad_norm_one)
    grad_hidden = (grad_self_res + norm_one_part).astype(LOW)
    fin_query, fin_key, fin_value = (
        jnp.concatenate(
            [
                fin_qkv[:, i * half_width : (i + 1) * half_width],
                fin_qkv[:, (i + 3) * half_width : (i + 4) * half_width],
            ],
            axis=1,
        )
        for i in range(3)
    )
    vectors = summed_vectors(
        jnp.stack(
            [
                grad_gain_one,
                grad_bias_one,
                grad_gain_two,
                grad_bias_two,
                grad_gain_three,
                grad_bias_three,
            ]
        ),
    )
    fin_gain_one, fin_bias_one, fin_gain_two, fin_bias_two, fin_gain_three, fin_bias_three = (
        lax.dynamic_slice_in_dim(vectors, col_start, shard_rows, 1)
    )
    return (
        block_out,
        grad_hidden,
        grad_text,
        fin_gain_one,
        fin_bias_one,
        fin_query,
        fin_key,
        fin_value,
        fin_output,
        fin_gain_two,
        fin_bias_two,
        fin_xquery,
        grad_xkey,
        grad_xvalue,
        fin_xoutput,
        fin_gain_three,
        fin_bias_three,
        fin_up,
        fin_down,
    )


def solution(mesh):
    rows, vector, tokens = P("shard", None), P("shard"), P(BOTH, None)
    placed = (
        (tokens, P(), P(BOTH), P(BOTH))
        + (vector, vector, rows, rows, rows, rows)
        + (vector, vector, rows, rows, rows, rows)
        + (vector, vector, rows, rows, tokens)
    )
    return jax.shard_map(
        on_device,
        mesh=mesh,
        in_specs=placed,
        out_specs=(
            (tokens, tokens, P())
            + (vector, vector, rows, rows, rows, rows)
            + (vector, vector, rows, rows, rows, rows)
            + (vector, vector, rows, rows)
        ),
        check_vma=False,
    )
```

```python
import functools

import jax
import jax.numpy as jnp
from jax import lax
from jax.experimental import pallas as pl
from jax.experimental.pallas import tpu as pltpu
from jax.sharding import PartitionSpec as P


HD = 64
CLIP_MAX = 1280
EPSILON = 1e-05
NEGATIVE = -1e30
BLOCK = 256
BOTH = ("rep", "shard")
LOW = jnp.bfloat16
WIDE = jnp.float32


def normalize(values):
    centre = values - jnp.mean(values, axis=-1, keepdims=True)
    spread = jnp.mean(centre * centre, axis=-1, keepdims=True)
    return centre * lax.rsqrt(spread + EPSILON)


def scaled_norm(values, scale_vec):
    return normalize(values) * scale_vec


def exact_gelu(values):
    return jax.nn.gelu(values, approximate=False)


def matmul(left, right):
    return jnp.dot(left, right, preferred_element_type=WIDE)


def left_t(left, right):
    return lax.dot_general(left, right, (((0,), (0,)), ((), ())), preferred_element_type=WIDE)


def right_t(left, right):
    return lax.dot_general(left, right, (((1,), (1,)), ((), ())), preferred_element_type=WIDE)


def norm_back(values, scale_vec, upstream):
    _, pull = jax.vjp(scaled_norm, values, scale_vec.astype(WIDE))
    grad_values, grad_scale = pull(upstream)
    return (grad_values, grad_scale, jnp.sum(upstream, axis=0))


def pick(array, index, axis):
    return lax.dynamic_index_in_dim(array, index, axis, False)


def axis_length(axis):
    return lax.axis_size(axis)


def swap(array, axis, pairing):
    length = axis_length(axis)
    pairs = [(i, pairing(i)) for i in range(length)]
    return lax.ppermute(array, axis, [(i, j) for i, j in pairs if 0 <= j < length])


def add_low(left, right):
    return (left.astype(WIDE) + right.astype(WIDE)).astype(LOW)


def gather_rows(array):
    return lax.all_gather(array, "shard", axis=0, tiled=True)


def joined(parts):
    return parts[0] if len(parts) == 1 else jnp.concatenate(parts, axis=-1)


def positions(grads):
    index, rep = lax.axis_index("shard"), lax.axis_index("rep")
    grads, index, rep = lax.optimization_barrier((grads, index, rep))
    return grads, index % 2, (index // 2) % 2, index // 4, rep


def across_cores(grads, core):
    rows = grads[0].shape[0] // 16
    parts = [grad.reshape(8, 2, rows, grad.shape[1]) for grad in grads]
    away = joined([pick(part, 1 - core, 1) for part in parts])
    held = joined([pick(part, core, 1) for part in parts])
    return add_low(held, swap(away, "shard", lambda i: i ^ 1))


def down_levels(both, level):
    total = pick(both, level, 0).astype(WIDE)
    for step in range(1, 4):
        total = total + swap(
            pick(both, (level + step) % 4, 0), "shard", lambda i: (i + 4 * step) % 16
        ).astype(WIDE)
    return total.astype(LOW)


def box_total(held, side, level, rep):
    rows, width = held.shape[-2:]
    held = held.reshape(4, 2, rows, width)
    half = width // 2
    first = held[..., :half]
    second = held[..., half:].reshape(4, 2, 2, rows // 2, width - half)
    second = add_low(
        pick(second, rep, 2),
        swap(pick(second, 1 - rep, 2), "rep", lambda i: i ^ 1),
    )
    first = add_low(
        pick(first, side, 1),
        swap(pick(first, 1 - side, 1), "shard", lambda i: i ^ 2),
    ).reshape(4, 2, rows // 2, half)
    first = add_low(pick(first, rep, 1), swap(pick(first, 1 - rep, 1), "rep", lambda i: i ^ 1))
    second = add_low(
        pick(second, side, 1),
        swap(pick(second, 1 - side, 1), "shard", lambda i: i ^ 2),
    )
    own = down_levels(jnp.concatenate([first, second], axis=2), level)
    other = swap(own, "rep", lambda i: i ^ 1)
    low, high = jnp.where(rep == 0, own, other), jnp.where(rep == 0, other, own)
    return jnp.concatenate([low, high], axis=0)


def plane_total(grads):
    if axis_length("shard") != 16:
        return lax.psum_scatter(joined(grads), "shard", scatter_dimension=0, tiled=True)
    grads, core, side, level, _ = positions(grads)
    held = across_cores(grads, core)
    held = held.reshape(4, 2, *held.shape[1:])
    held = add_low(
        pick(held, side, 1),
        swap(pick(held, 1 - side, 1), "shard", lambda i: i ^ 2),
    )
    return down_levels(held, level)


def rep_pair(own):
    other = swap(own, "rep", lambda i: i ^ 1)
    rep = lax.axis_index("rep")
    return jnp.where(rep == 0, own, other), jnp.where(rep == 0, other, own)


def summed_rows(grads):
    grads = [grad.astype(LOW) for grad in grads]
    widths = [grad.shape[1] for grad in grads]
    if axis_length("shard") == 16 and axis_length("rep") == 2:
        grads, core, side, level, rep = positions(grads)
        whole = box_total(across_cores(grads, core), side, level, rep)
    else:
        share = lax.psum_scatter(joined(grads), "shard", scatter_dimension=0, tiled=True)
        whole = lax.psum(share.astype(WIDE), "rep")
    whole = whole.astype(WIDE)
    out, start = [], 0
    for width in widths:
        out.append(whole[:, start : start + width])
        start += width
    return out


def summed_halves(grads):
    width = sum(grad.shape[1] for grad in grads)
    grad = joined([grad.astype(LOW) for grad in grads])
    if axis_length("shard") == 16 and axis_length("rep") == 2:
        grad, core, side, level, rep = positions(grad)
        whole = box_total(grad.reshape(8, -1, width), side, level, rep)
        rows = whole.shape[0] // 2
        parts = whole.reshape(2, rows, width)
        got = swap(pick(parts, 1 - core, 0), "shard", lambda i: i ^ 1)
        return core_pair(pick(parts, core, 0), got, core, 1).astype(WIDE)
    core = lax.axis_index("shard") % 2
    grad = core_pair(grad, jnp.zeros_like(grad), core, 1)
    share = lax.psum_scatter(grad, "shard", scatter_dimension=0, tiled=True)
    return lax.psum(share.astype(WIDE), "rep")


def summed_vectors(stack):
    if axis_length("shard") != 16 or axis_length("rep") != 2:
        return lax.psum(stack, BOTH)
    for bit in (1, 2, 4, 8):
        stack = stack + swap(stack, "shard", lambda i: i ^ bit)
    return stack + swap(stack, "rep", lambda i: i ^ 1)


def head_lanes(which):
    lane = lax.broadcasted_iota(jnp.int32, (BLOCK, 2 * HD), 1)
    return lane < HD if which == 0 else lane >= HD


def open_pairs(offsets, step, reach):
    base = (reach - step) * BLOCK
    keys = lax.broadcasted_iota(jnp.int32, (BLOCK, BLOCK), 0)
    column = lax.broadcasted_iota(jnp.int32, (1, BLOCK), 1)
    allowed = keys >= (column - offsets) + base
    if base == 0:
        allowed = allowed & (keys <= lax.broadcasted_iota(jnp.int32, (BLOCK, BLOCK), 1))
    return allowed


def attend_kernel(reach, offset_ref, query_ref, window_ref, out_ref, log_ref, held):
    start = pl.program_id(1) * BLOCK
    offsets = offset_ref[...]
    scaled = query_ref[...] * jnp.asarray(HD**-0.5, LOW)
    mixed = []
    for head in range(2):
        query = jnp.where(head_lanes(head), scaled, jnp.zeros_like(scaled))
        peak = jnp.full((1, BLOCK), NEGATIVE, WIDE)
        for step in range(reach + 1):
            rows = pl.ds(pl.multiple_of(start + step * BLOCK, BLOCK), BLOCK)
            scores = right_t(window_ref[0, rows, :], query)
            scores = jnp.where(open_pairs(offsets, step, reach), scores, NEGATIVE)
            held[head, step] = scores
            peak = jnp.maximum(peak, jnp.max(scores, axis=0, keepdims=True))
        total = jnp.zeros((1, BLOCK), WIDE)
        blend = jnp.zeros((2 * HD, BLOCK), WIDE)
        for step in range(reach + 1):
            rows = pl.ds(pl.multiple_of(start + step * BLOCK, BLOCK), BLOCK)
            expo = jnp.exp(held[head, step] - peak)
            total = total + jnp.sum(expo, axis=0, keepdims=True)
            blend = blend + left_t(window_ref[1, rows, :], expo.astype(LOW))
        mixed.append((blend / total)[head * HD : (head + 1) * HD])
        log_ref[0, pl.ds(head, 1), :] = peak + jnp.log(total)
    out_ref[...] = jnp.concatenate(mixed, axis=0).T.astype(LOW)


def attend(offsets, queries, window, reach):
    rows, width = queries.shape
    pairs, blocks, context = width // (2 * HD), rows // BLOCK, window.shape[1]
    work = pairs * 2 * rows * (reach + 1) * BLOCK
    return pl.pallas_call(
        functools.partial(attend_kernel, reach),
        grid=(pairs, blocks),
        in_specs=[
            pl.BlockSpec((1, BLOCK), lambda p, b: (0, b)),
            pl.BlockSpec((BLOCK, 2 * HD), lambda p, b: (b, p)),
            pl.BlockSpec((2, context, 2 * HD), lambda p, b: (0, 0, p)),
        ],
        out_specs=[
            pl.BlockSpec((BLOCK, 2 * HD), lambda p, b: (b, p)),
            pl.BlockSpec((1, 2, BLOCK), lambda p, b: (p, 0, b)),
        ],
        out_shape=[
            jax.ShapeDtypeStruct((rows, width), LOW),
            jax.ShapeDtypeStruct((pairs, 2, rows), WIDE),
        ],
        scratch_shapes=[pltpu.VMEM((2, reach + 1, BLOCK, BLOCK), WIDE)],
        cost_estimate=pl.CostEstimate(
            flops=16 * HD * work, transcendentals=work, bytes_accessed=8 * rows * width
        ),
        name="attend_forward",
    )(offsets, queries, window)


def attend_back_kernel(
    reach,
    offset_ref,
    query_ref,
    window_ref,
    out_ref,
    log_ref,
    grad_ref,
    grad_query_ref,
    grad_window_ref,
    grad_keys,
    grad_values,
):
    block = pl.program_id(1)
    start = block * BLOCK

    @pl.when(block == 0)
    def _():
        grad_keys[...] = jnp.zeros_like(grad_keys)
        grad_values[...] = jnp.zeros_like(grad_values)

    offsets = offset_ref[...]
    scaled = query_ref[...] * jnp.asarray(HD**-0.5, LOW)
    grads = grad_ref[...]
    inner = (grads.astype(WIDE) * out_ref[...].astype(WIDE)).T
    query, grad, inners, logs = [], [], [], []
    for head in range(2):
        lanes = head_lanes(head)
        query.append(jnp.where(lanes, scaled, jnp.zeros_like(scaled)))
        grad.append(jnp.where(lanes, grads, jnp.zeros_like(grads)))
        inners.append(jnp.sum(inner[head * HD : (head + 1) * HD], axis=0, keepdims=True))
        logs.append(log_ref[0, pl.ds(head, 1), :])
    back = [jnp.zeros((2 * HD, BLOCK), WIDE) for _ in range(2)]
    for step in range(reach + 1):
        rows = pl.ds(pl.multiple_of(start + step * BLOCK, BLOCK), BLOCK)
        key, value = window_ref[0, rows, :], window_ref[1, rows, :]
        allowed = open_pairs(offsets, step, reach)
        to_key = jnp.zeros((BLOCK, 2 * HD), WIDE)
        to_value = jnp.zeros((BLOCK, 2 * HD), WIDE)
        for head in range(2):
            scores = jnp.where(allowed, right_t(key, query[head]), NEGATIVE)
            probs = jnp.exp(scores - logs[head])
            to_value = to_value + matmul(probs.astype(LOW), grad[head])
            grad_probs = right_t(value, grad[head])
            grad_scores = (probs * (grad_probs - inners[head])).astype(LOW)
            to_key = to_key + matmul(grad_scores, query[head])
            back[head] = back[head] + left_t(key, grad_scores)
        grad_keys[rows, :] += to_key
        grad_values[rows, :] += to_value
    back = jnp.concatenate([back[0][:HD], back[1][HD:]], axis=0) * (HD**-0.5)
    grad_query_ref[...] = back.T.astype(LOW)

    @pl.when(block == pl.num_programs(1) - 1)
    def _():
        grad_window_ref[0] = grad_keys[...].astype(LOW)
        grad_window_ref[1] = grad_values[...].astype(LOW)


def attend_back(offsets, queries, window, out, logs, grads, reach, begin, pairs):
    rows = queries.shape[0]
    width = pairs * 2 * HD
    blocks, context = rows // BLOCK, window.shape[1]
    work = pairs * 2 * rows * (reach + 1) * BLOCK
    row_block = pl.BlockSpec((BLOCK, 2 * HD), lambda p, b: (b, p + begin))
    window_block = pl.BlockSpec((2, context, 2 * HD), lambda p, b: (0, 0, p + begin))
    return pl.pallas_call(
        functools.partial(attend_back_kernel, reach),
        grid=(pairs, blocks),
        in_specs=[
            pl.BlockSpec((1, BLOCK), lambda p, b: (0, b)),
            row_block,
            window_block,
            row_block,
            pl.BlockSpec((1, 2, BLOCK), lambda p, b: (p + begin, 0, b)),
            row_block,
        ],
        out_specs=[
            pl.BlockSpec((BLOCK, 2 * HD), lambda p, b: (b, p)),
            pl.BlockSpec((2, context, 2 * HD), lambda p, b: (0, 0, p)),
        ],
        out_shape=[
            jax.ShapeDtypeStruct((rows, width), LOW),
            jax.ShapeDtypeStruct((2, context, width), LOW),
        ],
        scratch_shapes=[
            pltpu.VMEM((context, 2 * HD), WIDE),
            pltpu.VMEM((context, 2 * HD), WIDE),
        ],
        cost_estimate=pl.CostEstimate(
            flops=40 * HD * work, transcendentals=work, bytes_accessed=16 * rows * width
        ),
        name="attend_backward",
    )(offsets, queries, window, out, logs, grads)


def core_pair(own, got, core, axis):
    return jnp.where(
        core == 0,
        jnp.concatenate([own, got], axis=axis),
        jnp.concatenate([got, own], axis=axis),
    )


def on_device(
    hidden,
    text_states,
    clip_index,
    frame_offset,
    self_gain,
    self_bias,
    w_query,
    w_key,
    w_value,
    w_output,
    cross_gain,
    cross_bias,
    x_query,
    x_key,
    x_value,
    x_output,
    final_gain,
    final_bias,
    w_up,
    w_down,
    cotangent,
):
    tok_rows, model_width = hidden.shape
    head_count = model_width // HD
    half_width = model_width // 2
    reach = (CLIP_MAX - 2) // tok_rows + 1
    key_scale = HD ** (-0.5)
    clip_total = text_states.shape[0]
    text_rows = text_states.shape[1]
    shard_count, rep_count = axis_length("shard"), axis_length("rep")
    device_count = shard_count * rep_count
    place = lax.axis_index("rep") * shard_count + lax.axis_index("shard")
    core, side = place % 2, (place // 2) % 2

    params = jnp.stack(
        [self_gain, self_bias, cross_gain, cross_bias, final_gain, final_bias], axis=1
    )
    params = jnp.pad(params, ((0, 0), (0, 128 - params.shape[1])))
    split = [w[:, h : h + half_width] for h in (0, half_width) for w in (w_query, w_key, w_value)]
    first_group = gather_rows(jnp.concatenate(split + [w_output, params], axis=1))
    full_output = first_group[:, 3 * model_width : 4 * model_width]
    gain_one, bias_one, gain_two, bias_two, gain_three, bias_three = (
        first_group[:, 4 * model_width + i].astype(WIDE) for i in range(6)
    )
    full_part = lax.dynamic_slice_in_dim(
        first_group, core * (3 * half_width), 3 * half_width, 1
    )
    second_group = gather_rows(jnp.concatenate([x_query, x_key, x_value, x_output], axis=1))
    full_xquery, full_xkey, full_xvalue, full_xoutput = (
        second_group[:, i * model_width : (i + 1) * model_width] for i in range(4)
    )
    rep_index = lax.axis_index("rep")
    down_rows = w_down.shape[0]
    chunk = down_rows // 4
    some_up = pick(w_up.reshape(w_up.shape[0], shard_count, 2, 2, chunk), rep_index, 2)
    some_up = jnp.transpose(some_up, (0, 2, 1, 3)).reshape(w_up.shape[0], -1)
    some_down = pick(w_down.reshape(2, 2, chunk, model_width), rep_index, 0)
    hidden_half = some_up.shape[1]
    third_group = gather_rows(jnp.concatenate([some_up, some_down[0], some_down[1]], axis=1))
    half_up = third_group[:, :hidden_half]
    half_down = [
        third_group[:, hidden_half + i * model_width : hidden_half + (i + 1) * model_width]
        for i in range(2)
    ]
    upstream = jnp.concatenate([cotangent, swap(cotangent, "rep", lambda i: i ^ 1)], axis=0)

    offsets = core_pair(frame_offset, swap(frame_offset, BOTH, lambda i: i ^ 1), core, 0)[None, :]
    resid = hidden.astype(WIDE)
    below = swap(hidden, BOTH, lambda i: i + 4)
    far = swap(hidden, BOTH, lambda i: i + 8 if i % 4 == 3 else -1)
    across = swap(jnp.where(side == 0, hidden, below), BOTH, lambda i: i ^ 2)
    third = swap(jnp.where(side == 0, below, far), BOTH, lambda i: i ^ 2 if i % 2 == 1 else -1)
    shards = jnp.stack([below, across, hidden, third])
    partner = swap(shards, BOTH, lambda i: i ^ 1)
    paired = core_pair(shards[:3], partner[:3], core, 1)
    around = jnp.concatenate(
        [jnp.where(core == 1, third, partner[3]), paired[0], paired[1], paired[2]], axis=0
    )
    chip_rows = 2 * tok_rows
    halo_rows = tok_rows + 2 * chip_rows
    around = around.astype(WIDE)
    normed_around = (scaled_norm(around, gain_one) + bias_one).astype(LOW)
    normed_chip = normed_around[halo_rows:]
    queries = matmul(normed_chip, full_part[:, :half_width]).astype(LOW)
    window = jnp.stack(
        [
            matmul(normed_around, full_part[:, half_width : 2 * half_width]).astype(LOW),
            matmul(normed_around, full_part[:, 2 * half_width :]).astype(LOW),
        ]
    )
    chip_mixed, logs = attend(offsets, queries, window, reach)

    def to_tokens(chip_rows_array):
        mine = lax.dynamic_slice_in_dim(chip_rows_array, core * tok_rows, tok_rows, 0)
        away = lax.dynamic_slice_in_dim(chip_rows_array, (1 - core) * tok_rows, tok_rows, 0)
        return core_pair(mine, swap(away, BOTH, lambda i: i ^ 1), core, 1)

    attended = to_tokens(chip_mixed)
    after_self = resid + matmul(attended, full_output)
    normed_two = (scaled_norm(after_self, gain_two) + bias_two).astype(LOW)
    cross_q = matmul(normed_two, full_xquery).astype(LOW)
    first = clip_index[0]
    second = jnp.minimum(first + 1, clip_total - 1)
    chosen = jnp.concatenate(
        [
            lax.dynamic_index_in_dim(text_states, first, 0, False),
            lax.dynamic_index_in_dim(text_states, second, 0, False),
        ],
        axis=0,
    )
    cross_k = matmul(chosen, full_xkey).astype(LOW)
    cross_v = matmul(chosen, full_xvalue).astype(LOW)
    slot = jnp.arange(2 * text_rows, dtype=jnp.int32) // text_rows
    slot_clip = jnp.where(slot == 0, first, second)
    open_slot = (slot == 0) | (second != first)
    cross_mask = (clip_index[:, None] == slot_clip[None, :]) & open_slot[None, :]
    cq_heads = cross_q.reshape(tok_rows, head_count, HD)
    ck_heads = cross_k.reshape(2 * text_rows, head_count, HD)
    cv_heads = cross_v.reshape(2 * text_rows, head_count, HD)
    cross_scores = (
        jnp.einsum("thd,khd->htk", cq_heads, ck_heads, preferred_element_type=WIDE) * key_scale
    )
    cross_scores = jnp.where(cross_mask[None], cross_scores, NEGATIVE)
    cross_probs = jax.nn.softmax(cross_scores, axis=2)
    cross_low = cross_probs.astype(LOW)
    cross_mix = (
        jnp.einsum("htk,khd->thd", cross_low, cv_heads, preferred_element_type=WIDE)
        .reshape(tok_rows, model_width)
        .astype(LOW)
    )
    after_cross = after_self + matmul(cross_mix, full_xoutput)
    normed_three = (scaled_norm(after_cross, gain_three) + bias_three).astype(LOW)
    both_three = jnp.concatenate([normed_three, swap(normed_three, "rep", lambda i: i ^ 1)], axis=0)
    pre_act = matmul(both_three, half_up)
    activ, gelu_pull = jax.vjp(exact_gelu, pre_act)
    activ = activ.astype(LOW)
    slope = gelu_pull(jnp.ones_like(pre_act))[0]
    activ, slope = lax.optimization_barrier((activ, slope))
    grad_act = [right_t(upstream, part) for part in half_down]
    grad_pre = (slope * jnp.concatenate(grad_act, axis=1)).astype(LOW)
    grad_both = right_t(grad_pre, half_up)
    grad_norm_three = grad_both[:tok_rows] + swap(
        grad_both[tok_rows:].astype(LOW), "rep", lambda i: i ^ 1
    ).astype(WIDE)
    quarter = hidden_half // 2
    grad_down = [
        left_t(activ[:, i * quarter : (i + 1) * quarter], upstream).astype(LOW)
        for i in range(2)
    ]
    grad_up = left_t(both_three, grad_pre).astype(LOW)
    down_halves = rep_pair(plane_total(grad_down))
    fin_down = jnp.concatenate(
        [half[:, i * model_width : (i + 1) * model_width] for half in down_halves for i in range(2)],
        axis=0,
    ).astype(WIDE)
    up_halves = rep_pair(plane_total([grad_up]))
    fin_up = jnp.stack(
        [half.reshape(w_up.shape[0], 2, shard_count, chunk) for half in up_halves], axis=1
    )
    fin_up = jnp.transpose(fin_up, (0, 3, 1, 2, 4)).reshape(w_up.shape).astype(WIDE)
    mixed_both = matmul(activ[:, :quarter], half_down[0]) + matmul(activ[:, quarter:], half_down[1])
    block_out = (
        after_cross
        + mixed_both[:tok_rows]
        + swap(mixed_both[tok_rows:].astype(LOW), "rep", lambda i: i ^ 1).astype(WIDE)
    ).astype(LOW)
    norm_three_part, grad_gain_three, grad_bias_three = norm_back(
        after_cross, gain_three, grad_norm_three
    )
    grad_cross_res = cotangent.astype(WIDE) + norm_three_part
    branch_two = grad_cross_res.astype(LOW)
    grad_xoutput = left_t(cross_mix, branch_two)
    grad_cmix = right_t(branch_two, full_xoutput).astype(LOW)
    grad_cmix = grad_cmix.reshape(tok_rows, head_count, HD)
    grad_cprob = jnp.einsum("thd,khd->htk", grad_cmix, cv_heads, preferred_element_type=WIDE)
    cross_inner = jnp.sum(cross_probs * grad_cprob, axis=2, keepdims=True)
    grad_cscore = (cross_probs * (grad_cprob - cross_inner)).astype(LOW)
    grad_cq = (
        (jnp.einsum("htk,khd->thd", grad_cscore, ck_heads, preferred_element_type=WIDE) * key_scale)
        .reshape(tok_rows, model_width)
        .astype(LOW)
    )
    grad_ck = (
        jnp.einsum("htk,thd->khd", grad_cscore, cq_heads, preferred_element_type=WIDE) * key_scale
    ).reshape(2 * text_rows, model_width)
    grad_cv = jnp.einsum(
        "htk,thd->khd", cross_low, grad_cmix, preferred_element_type=WIDE
    ).reshape(2 * text_rows, model_width)
    grad_xquery = left_t(normed_two, grad_cq)
    grad_norm_two = right_t(grad_cq, full_xquery)
    norm_two_part, grad_gain_two, grad_bias_two = norm_back(after_self, gain_two, grad_norm_two)
    grad_self_res = grad_cross_res + norm_two_part
    branch_one = grad_self_res.astype(LOW)
    grad_output = left_t(attended, branch_one)
    fin_xoutput, fin_xquery, fin_output = summed_rows([grad_xoutput, grad_xquery, grad_output])

    slots = jnp.arange(clip_total, dtype=jnp.int32)
    in_first = (slots == first).astype(WIDE)[None, :, None, None]
    in_second = (slots == second).astype(WIDE)[None, :, None, None]
    pair = jnp.stack([grad_ck, grad_cv]).reshape(2, 2, text_rows, model_width)
    sums = (pair[:, None, 0] * in_first + pair[:, None, 1] * in_second).astype(LOW)
    sums = sums.reshape(2 * clip_total * text_rows, model_width)
    text_total = sums.shape[0]
    padded = -(-text_total // (16 * device_count)) * 16 * device_count
    sums = jnp.pad(sums, ((0, padded - text_total), (0, 0)))
    share = lax.psum_scatter(sums, BOTH, scatter_dimension=0, tiled=True)
    sums = lax.all_gather(share, BOTH, axis=0, tiled=True)
    flat_rows = clip_total * text_rows
    key_round, value_round = sums[:flat_rows], sums[flat_rows:text_total]
    shard_rows = x_key.shape[0]
    col_start = lax.axis_index("shard") * shard_rows
    text_flat = text_states.reshape(flat_rows, model_width)
    text_slice = lax.dynamic_slice_in_dim(text_flat, col_start, shard_rows, 1)
    grad_xkey = left_t(text_slice, key_round)
    grad_xvalue = left_t(text_slice, value_round)
    grad_text = right_t(key_round, full_xkey) + right_t(value_round, full_xvalue)
    grad_text = grad_text.reshape(clip_total, text_rows, model_width)

    grad_attended = right_t(branch_one, full_output).astype(LOW)
    halves = jnp.transpose(grad_attended.reshape(tok_rows, 2, half_width), (1, 0, 2))
    chip_grad = core_pair(
        pick(halves, core, 0),
        swap(pick(halves, 1 - core, 0), BOTH, lambda i: i ^ 1),
        core,
        0,
    )
    pairs = head_count // 4
    calls = 2 if pairs % 2 == 0 else 1
    backs = []
    for call in range(calls):
        backs.append(
            attend_back(
                offsets,
                queries,
                window,
                chip_mixed,
                logs,
                chip_grad,
                reach,
                call * pairs // calls,
                pairs // calls,
            )
        )
    chip_dq = jnp.concatenate([part[0] for part in backs], axis=1)
    grad_window = jnp.concatenate([part[1] for part in backs], axis=2)
    grad_weights = [
        left_t(normed_chip, chip_dq),
        left_t(normed_around, grad_window[0]),
        left_t(normed_around, grad_window[1]),
    ]
    fin_qkv = summed_halves(grad_weights)
    fin_query, fin_key, fin_value = (
        jnp.concatenate(
            [
                fin_qkv[:, i * half_width : (i + 1) * half_width],
                fin_qkv[:, (i + 3) * half_width : (i + 4) * half_width],
            ],
            axis=1,
        )
        for i in range(3)
    )
    grad_around = right_t(grad_window[0], full_part[:, half_width : 2 * half_width]) + right_t(
        grad_window[1], full_part[:, 2 * half_width :]
    )
    grad_chip = grad_around[halo_rows:] + right_t(chip_dq, full_part[:, :half_width])
    grad_halo = grad_around[:halo_rows].astype(LOW)
    units = jnp.concatenate([grad_halo[tok_rows:], grad_chip.astype(LOW)], axis=0)
    units = units.reshape(3, 2, tok_rows, model_width)
    sent = jnp.concatenate([pick(units, 1 - core, 1), grad_halo[None, :tok_rows]], axis=0)
    partner = swap(sent, BOTH, lambda i: i ^ 1)
    sums = add_low(pick(units, core, 1), partner[:3])
    low_sum = add_low(grad_halo[:tok_rows], partner[3])
    back = swap(sums[1], BOTH, lambda i: i ^ 2).astype(WIDE)
    back_half = swap(low_sum, BOTH, lambda i: i ^ 2 if i % 2 == 1 else -1)
    to_below = (
        sums[0].astype(WIDE) + jnp.where(side == 0, back_half.astype(WIDE), back)
    ).astype(LOW)
    grad_norm_one = (
        sums[2].astype(WIDE)
        + jnp.where(side == 0, back, 0.0)
        + swap(to_below, BOTH, lambda i: i - 4).astype(WIDE)
        + swap(back_half, BOTH, lambda i: i - 8 if i % 4 == 3 else -1).astype(WIDE)
    )
    norm_one_part, grad_gain_one, grad_bias_one = norm_back(resid, gain_one, grad_norm_one)
    grad_hidden = (grad_self_res + norm_one_part).astype(LOW)
    vectors = summed_vectors(
        jnp.stack(
            [
                grad_gain_one,
                grad_bias_one,
                grad_gain_two,
                grad_bias_two,
                grad_gain_three,
                grad_bias_three,
            ]
        ),
    )
    fin_gain_one, fin_bias_one, fin_gain_two, fin_bias_two, fin_gain_three, fin_bias_three = (
        lax.dynamic_slice_in_dim(vectors, col_start, shard_rows, 1)
    )
    return (
        block_out,
        grad_hidden,
        grad_text,
        fin_gain_one,
        fin_bias_one,
        fin_query,
        fin_key,
        fin_value,
        fin_output,
        fin_gain_two,
        fin_bias_two,
        fin_xquery,
        grad_xkey,
        grad_xvalue,
        fin_xoutput,
        fin_gain_three,
        fin_bias_three,
        fin_up,
        fin_down,
    )


def solution(mesh):
    rows, vector, tokens = P("shard", None), P("shard"), P(BOTH, None)
    placed = (
        (tokens, P(), P(BOTH), P(BOTH))
        + (vector, vector, rows, rows, rows, rows)
        + (vector, vector, rows, rows, rows, rows)
        + (vector, vector, rows, rows, tokens)
    )
    return jax.shard_map(
        on_device,
        mesh=mesh,
        in_specs=placed,
        out_specs=(
            (tokens, tokens, P())
            + (vector, vector, rows, rows, rows, rows)
            + (vector, vector, rows, rows, rows, rows)
            + (vector, vector, rows, rows)
        ),
        check_vma=False,
    )
```

```python
import functools

import jax
import jax.numpy as jnp
from jax import lax
from jax.experimental import pallas as pl
from jax.experimental.pallas import tpu as pltpu
from jax.sharding import PartitionSpec as P


HD = 64
CLIP_MAX = 1280
EPSILON = 1e-05
NEGATIVE = -1e30
BLOCK = 256
BOTH = ("rep", "shard")
LOW = jnp.bfloat16
WIDE = jnp.float32


def normalize(values):
    centre = values - jnp.mean(values, axis=-1, keepdims=True)
    spread = jnp.mean(centre * centre, axis=-1, keepdims=True)
    return centre * lax.rsqrt(spread + EPSILON)


def scaled_norm(values, scale_vec):
    return normalize(values) * scale_vec


def exact_gelu(values):
    return jax.nn.gelu(values, approximate=False)


def matmul(left, right):
    return jnp.dot(left, right, preferred_element_type=WIDE)


def left_t(left, right):
    return lax.dot_general(left, right, (((0,), (0,)), ((), ())), preferred_element_type=WIDE)


def right_t(left, right):
    return lax.dot_general(left, right, (((1,), (1,)), ((), ())), preferred_element_type=WIDE)


def norm_back(values, scale_vec, upstream):
    _, pull = jax.vjp(scaled_norm, values, scale_vec.astype(WIDE))
    grad_values, grad_scale = pull(upstream)
    return (grad_values, grad_scale, jnp.sum(upstream, axis=0))


def pick(array, index, axis):
    return lax.dynamic_index_in_dim(array, index, axis, False)


def axis_length(axis):
    return lax.axis_size(axis)


def swap(array, axis, pairing):
    length = axis_length(axis)
    pairs = [(i, pairing(i)) for i in range(length)]
    return lax.ppermute(array, axis, [(i, j) for i, j in pairs if 0 <= j < length])


def add_low(left, right):
    return (left.astype(WIDE) + right.astype(WIDE)).astype(LOW)


def gather_rows(array):
    return lax.all_gather(array, "shard", axis=0, tiled=True)


def joined(parts):
    return parts[0] if len(parts) == 1 else jnp.concatenate(parts, axis=-1)


def positions(grads):
    index, rep = lax.axis_index("shard"), lax.axis_index("rep")
    grads, index, rep = lax.optimization_barrier((grads, index, rep))
    return grads, index % 2, (index // 2) % 2, index // 4, rep


def across_cores(grads, core):
    rows = grads[0].shape[0] // 16
    parts = [grad.reshape(8, 2, rows, grad.shape[1]) for grad in grads]
    away = joined([pick(part, 1 - core, 1) for part in parts])
    held = joined([pick(part, core, 1) for part in parts])
    return add_low(held, swap(away, "shard", lambda i: i ^ 1))


def down_levels(both, level):
    axis = both.ndim - 3
    total = pick(both, level, axis).astype(WIDE)
    for step in range(1, 4):
        total = total + swap(
            pick(both, (level + step) % 4, axis), "shard", lambda i: (i + 4 * step) % 16
        ).astype(WIDE)
    return total.astype(LOW)


def box_total(firsts, seconds, side, level, rep):
    rows = firsts[0].shape[-2]
    firsts = [part.reshape(4, 2, *part.shape[-2:]) for part in firsts]
    seconds = [part.reshape(4, 2, 2, rows // 2, part.shape[-1]) for part in seconds]
    second = add_low(
        joined([pick(part, rep, 2) for part in seconds]),
        swap(joined([pick(part, 1 - rep, 2) for part in seconds]), "rep", lambda i: i ^ 1),
    )
    first = add_low(
        joined([pick(part, side, 1) for part in firsts]),
        swap(joined([pick(part, 1 - side, 1) for part in firsts]), "shard", lambda i: i ^ 2),
    )
    first = first.reshape(4, 2, rows // 2, first.shape[-1])
    first = add_low(pick(first, rep, 1), swap(pick(first, 1 - rep, 1), "rep", lambda i: i ^ 1))
    second = add_low(
        pick(second, side, 1),
        swap(pick(second, 1 - side, 1), "shard", lambda i: i ^ 2),
    )
    own = down_levels(jnp.concatenate([first, second], axis=2), level)
    other = swap(own, "rep", lambda i: i ^ 1)
    low, high = jnp.where(rep == 0, own, other), jnp.where(rep == 0, other, own)
    return jnp.concatenate([low, high], axis=0)


def plane_total(grad):
    if axis_length("shard") != 16:
        return lax.psum_scatter(grad, "shard", scatter_dimension=1, tiled=True)
    grad, core, side, level, _ = positions(grad)
    count, rows, width = grad.shape[0], grad.shape[1] // 16, grad.shape[2]
    parts = grad.reshape(count, 8, 2, rows, width)
    held = add_low(
        pick(parts, core, 2),
        swap(pick(parts, 1 - core, 2), "shard", lambda i: i ^ 1),
    ).reshape(count, 4, 2, rows, width)
    held = add_low(
        pick(held, side, 2),
        swap(pick(held, 1 - side, 2), "shard", lambda i: i ^ 2),
    )
    return down_levels(held, level)


def rep_pair(own):
    other = swap(own, "rep", lambda i: i ^ 1)
    rep = lax.axis_index("rep")
    return jnp.where(rep == 0, own, other), jnp.where(rep == 0, other, own)


def summed_rows(grads):
    grads = [grad.astype(LOW) for grad in grads]
    widths = [grad.shape[1] for grad in grads]
    if axis_length("shard") == 16 and axis_length("rep") == 2:
        grads, core, side, level, rep = positions(grads)
        held = across_cores(grads, core)
        half = held.shape[-1] // 2
        whole = box_total([held[..., :half]], [held[..., half:]], side, level, rep)
    else:
        share = lax.psum_scatter(joined(grads), "shard", scatter_dimension=0, tiled=True)
        whole = lax.psum(share.astype(WIDE), "rep")
    whole = whole.astype(WIDE)
    out, start = [], 0
    for width in widths:
        out.append(whole[:, start : start + width])
        start += width
    return out


def summed_halves(wide, narrow):
    wide, narrow = wide.astype(LOW), narrow.astype(LOW)
    width = wide.shape[1] + narrow.shape[1]
    if axis_length("shard") == 16 and axis_length("rep") == 2:
        (wide, narrow), core, side, level, rep = positions((wide, narrow))
        wide, narrow = (part.reshape(8, -1, part.shape[1]) for part in (wide, narrow))
        half = width // 2
        whole = box_total([wide[..., :half]], [wide[..., half:], narrow], side, level, rep)
        parts = whole.reshape(2, -1, width)
        got = swap(pick(parts, 1 - core, 0), "shard", lambda i: i ^ 1)
        return core_pair(pick(parts, core, 0), got, core, 1).astype(WIDE)
    core = lax.axis_index("shard") % 2
    grad = joined([wide, narrow])
    grad = core_pair(grad, jnp.zeros_like(grad), core, 1)
    share = lax.psum_scatter(grad, "shard", scatter_dimension=0, tiled=True)
    return lax.psum(share.astype(WIDE), "rep")


def summed_vectors(stack):
    return jnp.sum(lax.all_gather(stack, BOTH), axis=0)


def head_lanes(which):
    lane = lax.broadcasted_iota(jnp.int32, (BLOCK, 2 * HD), 1)
    return lane < HD if which == 0 else lane >= HD


def open_pairs(offsets, step, reach):
    base = (reach - step) * BLOCK
    keys = lax.broadcasted_iota(jnp.int32, (BLOCK, BLOCK), 0)
    column = lax.broadcasted_iota(jnp.int32, (1, BLOCK), 1)
    allowed = keys >= (column - offsets) + base
    if base == 0:
        allowed = allowed & (keys <= lax.broadcasted_iota(jnp.int32, (BLOCK, BLOCK), 1))
    return allowed


def attend_kernel(reach, offset_ref, query_ref, window_ref, out_ref, log_ref, held):
    start = pl.program_id(1) * BLOCK
    offsets = offset_ref[...]
    scaled = query_ref[...] * jnp.asarray(HD**-0.5, LOW)
    mixed = []
    for head in range(2):
        query = jnp.where(head_lanes(head), scaled, jnp.zeros_like(scaled))
        peak = jnp.full((1, BLOCK), NEGATIVE, WIDE)
        for step in range(reach + 1):
            rows = pl.ds(pl.multiple_of(start + step * BLOCK, BLOCK), BLOCK)
            scores = right_t(window_ref[rows, : 2 * HD], query)
            scores = jnp.where(open_pairs(offsets, step, reach), scores, NEGATIVE)
            held[head, step] = scores
            peak = jnp.maximum(peak, jnp.max(scores, axis=0, keepdims=True))
        total = jnp.zeros((1, BLOCK), WIDE)
        blend = jnp.zeros((2 * HD, BLOCK), WIDE)
        for step in range(reach + 1):
            rows = pl.ds(pl.multiple_of(start + step * BLOCK, BLOCK), BLOCK)
            expo = jnp.exp(held[head, step] - peak)
            total = total + jnp.sum(expo, axis=0, keepdims=True)
            blend = blend + left_t(window_ref[rows, 2 * HD :], expo.astype(LOW))
        mixed.append((blend / total)[head * HD : (head + 1) * HD])
        log_ref[0, pl.ds(head, 1), :] = peak + jnp.log(total)
    out_ref[...] = jnp.concatenate(mixed, axis=0).T.astype(LOW)


def attend(offsets, queries, window, reach):
    rows, width = queries.shape
    pairs, blocks, context = width // (2 * HD), rows // BLOCK, window.shape[0]
    work = pairs * 2 * rows * (reach + 1) * BLOCK
    return pl.pallas_call(
        functools.partial(attend_kernel, reach),
        grid=(pairs, blocks),
        in_specs=[
            pl.BlockSpec((1, BLOCK), lambda p, b: (0, b)),
            pl.BlockSpec((BLOCK, 2 * HD), lambda p, b: (b, p)),
            pl.BlockSpec((context, 4 * HD), lambda p, b: (0, p)),
        ],
        out_specs=[
            pl.BlockSpec((BLOCK, 2 * HD), lambda p, b: (b, p)),
            pl.BlockSpec((1, 2, BLOCK), lambda p, b: (p, 0, b)),
        ],
        out_shape=[
            jax.ShapeDtypeStruct((rows, width), LOW),
            jax.ShapeDtypeStruct((pairs, 2, rows), WIDE),
        ],
        scratch_shapes=[pltpu.VMEM((2, reach + 1, BLOCK, BLOCK), WIDE)],
        cost_estimate=pl.CostEstimate(
            flops=16 * HD * work, transcendentals=work, bytes_accessed=8 * rows * width
        ),
        name="attend_forward",
    )(offsets, queries, window)


def attend_back_kernel(
    reach,
    offset_ref,
    query_ref,
    window_ref,
    out_ref,
    log_ref,
    grad_ref,
    *rest,
):
    grad_query_ref, grad_window_ref, grad_keys, grad_values = rest[-4:]
    block = pl.program_id(1)
    start = block * BLOCK

    @pl.when(block == 0)
    def _():
        grad_keys[...] = jnp.zeros_like(grad_keys)
        grad_values[...] = jnp.zeros_like(grad_values)

    offsets = offset_ref[...]
    scaled = query_ref[...] * jnp.asarray(HD**-0.5, LOW)
    grads = grad_ref[...]
    inner = (grads.astype(WIDE) * out_ref[...].astype(WIDE)).T
    query, grad, inners, logs = [], [], [], []
    for head in range(2):
        lanes = head_lanes(head)
        query.append(jnp.where(lanes, scaled, jnp.zeros_like(scaled)))
        grad.append(jnp.where(lanes, grads, jnp.zeros_like(grads)))
        inners.append(jnp.sum(inner[head * HD : (head + 1) * HD], axis=0, keepdims=True))
        logs.append(log_ref[0, pl.ds(head, 1), :])
    back = [jnp.zeros((2 * HD, BLOCK), WIDE) for _ in range(2)]
    for step in range(reach + 1):
        rows = pl.ds(pl.multiple_of(start + step * BLOCK, BLOCK), BLOCK)
        key, value = window_ref[rows, : 2 * HD], window_ref[rows, 2 * HD :]
        allowed = open_pairs(offsets, step, reach)
        to_key = jnp.zeros((BLOCK, 2 * HD), WIDE)
        to_value = jnp.zeros((BLOCK, 2 * HD), WIDE)
        for head in range(2):
            scores = jnp.where(allowed, right_t(key, query[head]), NEGATIVE)
            probs = jnp.exp(scores - logs[head])
            to_value = to_value + matmul(probs.astype(LOW), grad[head])
            grad_probs = right_t(value, grad[head])
            grad_scores = (probs * (grad_probs - inners[head])).astype(LOW)
            to_key = to_key + matmul(grad_scores, query[head])
            back[head] = back[head] + left_t(key, grad_scores)
        grad_keys[rows, :] += to_key
        grad_values[rows, :] += to_value
    back = jnp.concatenate([back[0][:HD], back[1][HD:]], axis=0) * (HD**-0.5)
    grad_query_ref[...] = back.T.astype(LOW)

    @pl.when(block == pl.num_programs(1) - 1)
    def _():
        grad_window_ref[:, : 2 * HD] = grad_keys[...].astype(LOW)
        grad_window_ref[:, 2 * HD :] = grad_values[...].astype(LOW)


def attend_back(offsets, queries, window, out, logs, grads, reach, begin, pairs, filled):
    rows, width = queries.shape
    blocks, context = rows // BLOCK, window.shape[0]
    work = pairs * 2 * rows * (reach + 1) * BLOCK
    row_block = pl.BlockSpec((BLOCK, 2 * HD), lambda p, b: (b, p + begin))
    window_block = pl.BlockSpec((context, 4 * HD), lambda p, b: (0, p + begin))
    return pl.pallas_call(
        functools.partial(attend_back_kernel, reach),
        grid=(pairs, blocks),
        in_specs=[
            pl.BlockSpec((1, BLOCK), lambda p, b: (0, b)),
            row_block,
            window_block,
            row_block,
            pl.BlockSpec((1, 2, BLOCK), lambda p, b: (p + begin, 0, b)),
            row_block,
        ]
        + [pl.BlockSpec(memory_space=pl.ANY)] * len(filled),
        out_specs=[row_block, window_block],
        out_shape=[
            jax.ShapeDtypeStruct((rows, width), LOW),
            jax.ShapeDtypeStruct(window.shape, LOW),
        ],
        input_output_aliases={6 + i: i for i in range(len(filled))},
        scratch_shapes=[
            pltpu.VMEM((context, 2 * HD), WIDE),
            pltpu.VMEM((context, 2 * HD), WIDE),
        ],
        cost_estimate=pl.CostEstimate(
            flops=40 * HD * work, transcendentals=work, bytes_accessed=16 * rows * width
        ),
        name="attend_backward",
    )(offsets, queries, window, out, logs, grads, *filled)


def core_pair(own, got, core, axis):
    return jnp.where(
        core == 0,
        jnp.concatenate([own, got], axis=axis),
        jnp.concatenate([got, own], axis=axis),
    )


def on_device(
    hidden,
    text_states,
    clip_index,
    frame_offset,
    self_gain,
    self_bias,
    w_query,
    w_key,
    w_value,
    w_output,
    cross_gain,
    cross_bias,
    x_query,
    x_key,
    x_value,
    x_output,
    final_gain,
    final_bias,
    w_up,
    w_down,
    cotangent,
):
    tok_rows, model_width = hidden.shape
    head_count = model_width // HD
    half_width = model_width // 2
    reach = (CLIP_MAX - 2) // tok_rows + 1
    key_scale = HD ** (-0.5)
    clip_total = text_states.shape[0]
    text_rows = text_states.shape[1]
    shard_count = axis_length("shard")
    shard_rows = x_key.shape[0]
    place = lax.axis_index("rep") * shard_count + lax.axis_index("shard")
    core, side = place % 2, (place // 2) % 2

    params = jnp.stack(
        [self_gain, self_bias, cross_gain, cross_bias, final_gain, final_bias], axis=1
    )
    params = jnp.pad(params, ((0, 0), (0, 128 - params.shape[1])))
    pairs = head_count // 4
    pair_split = (shard_rows, 2, pairs, 1, 2 * HD)
    key_value = jnp.concatenate([w_key.reshape(pair_split), w_value.reshape(pair_split)], axis=3)
    key_value = key_value.reshape(shard_rows, 2, model_width)
    first_group = gather_rows(
        jnp.concatenate(
            [
                part
                for h in range(2)
                for part in (w_query[:, h * half_width : (h + 1) * half_width], key_value[:, h])
            ]
            + [w_output, params],
            axis=1,
        ),
    )
    full_output = first_group[:, 3 * model_width : 4 * model_width]
    gain_one, bias_one, gain_two, bias_two, gain_three, bias_three = (
        first_group[:, 4 * model_width + i].astype(WIDE) for i in range(6)
    )
    part_query, part_pair = (
        lax.dynamic_slice_in_dim(first_group, core * (3 * half_width) + begin, width, 1)
        for begin, width in ((0, half_width), (half_width, model_width))
    )
    second_group = gather_rows(jnp.concatenate([x_query, x_key, x_value, x_output], axis=1))
    full_xquery, full_xkey, full_xvalue, full_xoutput = (
        second_group[:, i * model_width : (i + 1) * model_width] for i in range(4)
    )
    rep_index = lax.axis_index("rep")
    down_rows = w_down.shape[0]
    chunk = down_rows // 4
    some_up = pick(w_up.reshape(w_up.shape[0], shard_count, 2, 2, chunk), rep_index, 2)
    some_up = jnp.transpose(some_up, (0, 2, 1, 3)).reshape(w_up.shape[0], -1)
    some_down = pick(w_down.reshape(2, 2, chunk, model_width), rep_index, 0)
    hidden_half = some_up.shape[1]
    third_group = gather_rows(jnp.concatenate([some_up, some_down[0], some_down[1]], axis=1))
    half_up = third_group[:, :hidden_half]
    half_down = [
        third_group[:, hidden_half + i * model_width : hidden_half + (i + 1) * model_width]
        for i in range(2)
    ]
    upstream = jnp.concatenate([cotangent, swap(cotangent, "rep", lambda i: i ^ 1)], axis=0)

    offsets = core_pair(frame_offset, swap(frame_offset, BOTH, lambda i: i ^ 1), core, 0)[None, :]
    resid = hidden.astype(WIDE)
    below = swap(hidden, BOTH, lambda i: i + 4)
    far = swap(hidden, BOTH, lambda i: i + 8 if i % 4 == 3 else -1)
    across = swap(jnp.where(side == 0, hidden, below), BOTH, lambda i: i ^ 2)
    third = swap(jnp.where(side == 0, below, far), BOTH, lambda i: i ^ 2 if i % 2 == 1 else -1)
    shards = jnp.stack([below, across, hidden, third])
    partner = swap(shards, BOTH, lambda i: i ^ 1)
    paired = core_pair(shards[:3], partner[:3], core, 1)
    around = jnp.concatenate(
        [jnp.where(core == 1, third, partner[3]), paired[0], paired[1], paired[2]], axis=0
    )
    chip_rows = 2 * tok_rows
    halo_rows = tok_rows + 2 * chip_rows
    normed_plain = normalize(around.astype(WIDE))
    normed_around = (normed_plain * gain_one + bias_one).astype(LOW)
    normed_chip = normed_around[halo_rows:]
    window = matmul(normed_around, part_pair).astype(LOW)
    queries = matmul(normed_chip, part_query).astype(LOW)
    chip_mixed, logs = attend(offsets, queries, window, reach)

    def to_tokens(chip_rows_array):
        mine = lax.dynamic_slice_in_dim(chip_rows_array, core * tok_rows, tok_rows, 0)
        away = lax.dynamic_slice_in_dim(chip_rows_array, (1 - core) * tok_rows, tok_rows, 0)
        return core_pair(mine, swap(away, BOTH, lambda i: i ^ 1), core, 1)

    attended = to_tokens(chip_mixed)
    after_self = resid + matmul(attended, full_output)
    normed_two = (scaled_norm(after_self, gain_two) + bias_two).astype(LOW)
    cross_q = matmul(normed_two, full_xquery).astype(LOW)
    first = clip_index[0]
    second = jnp.minimum(first + 1, clip_total - 1)
    chosen = jnp.concatenate(
        [
            lax.dynamic_index_in_dim(text_states, first, 0, False),
            lax.dynamic_index_in_dim(text_states, second, 0, False),
        ],
        axis=0,
    )
    cross_k = matmul(chosen, full_xkey).astype(LOW)
    cross_v = matmul(chosen, full_xvalue).astype(LOW)
    slot = jnp.arange(2 * text_rows, dtype=jnp.int32) // text_rows
    slot_clip = jnp.where(slot == 0, first, second)
    open_slot = (slot == 0) | (second != first)
    cross_mask = (clip_index[:, None] == slot_clip[None, :]) & open_slot[None, :]
    cq_heads = cross_q.reshape(tok_rows, head_count, HD)
    ck_heads = cross_k.reshape(2 * text_rows, head_count, HD)
    cv_heads = cross_v.reshape(2 * text_rows, head_count, HD)
    cross_scores = (
        jnp.einsum("thd,khd->htk", cq_heads, ck_heads, preferred_element_type=WIDE) * key_scale
    )
    cross_scores = jnp.where(cross_mask[None], cross_scores, NEGATIVE)
    cross_probs = jax.nn.softmax(cross_scores, axis=2)
    cross_low = cross_probs.astype(LOW)
    cross_mix = (
        jnp.einsum("htk,khd->thd", cross_low, cv_heads, preferred_element_type=WIDE)
        .reshape(tok_rows, model_width)
        .astype(LOW)
    )
    after_cross = after_self + matmul(cross_mix, full_xoutput)
    normed_three = (scaled_norm(after_cross, gain_three) + bias_three).astype(LOW)
    both_three = jnp.concatenate([normed_three, swap(normed_three, "rep", lambda i: i ^ 1)], axis=0)
    quarter = hidden_half // 2
    activ, slope, grad_pre = [], [], []
    for i in range(2):
        pre_act = matmul(both_three, half_up[:, i * quarter : (i + 1) * quarter])
        shaped, gelu_pull = jax.vjp(exact_gelu, pre_act)
        shaped, steep = shaped.astype(LOW), gelu_pull(jnp.ones_like(pre_act))[0]
        shaped, steep = lax.optimization_barrier((shaped, steep))
        activ.append(shaped)
        slope.append(steep)
    for i in range(2):
        grad_pre.append((slope[i] * right_t(upstream, half_down[i])).astype(LOW))
    activ, grad_pre = jnp.concatenate(activ, axis=1), jnp.concatenate(grad_pre, axis=1)
    grad_both = right_t(grad_pre, half_up)
    grad_norm_three = grad_both[:tok_rows] + swap(
        grad_both[tok_rows:].astype(LOW), "rep", lambda i: i ^ 1
    ).astype(WIDE)
    grad_down = left_t(activ, upstream).astype(LOW).reshape(2, -1, model_width)
    grad_up = left_t(both_three, grad_pre).astype(LOW)
    own_down = plane_total(grad_down)
    own_up = plane_total(grad_up[None])
    norm_three_part, grad_gain_three, grad_bias_three = norm_back(
        after_cross, gain_three, grad_norm_three
    )
    grad_cross_res = cotangent.astype(WIDE) + norm_three_part
    branch_two = grad_cross_res.astype(LOW)
    grad_xoutput = left_t(cross_mix, branch_two)
    grad_cmix = right_t(branch_two, full_xoutput).astype(LOW)
    grad_cmix = grad_cmix.reshape(tok_rows, head_count, HD)
    grad_cprob = jnp.einsum("thd,khd->htk", grad_cmix, cv_heads, preferred_element_type=WIDE)
    cross_inner = jnp.sum(cross_probs * grad_cprob, axis=2, keepdims=True)
    grad_cscore = (cross_probs * (grad_cprob - cross_inner)).astype(LOW)
    grad_cq = (
        (jnp.einsum("htk,khd->thd", grad_cscore, ck_heads, preferred_element_type=WIDE) * key_scale)
        .reshape(tok_rows, model_width)
        .astype(LOW)
    )
    grad_ck = (
        jnp.einsum("htk,thd->hdk", grad_cscore, cq_heads, preferred_element_type=WIDE) * key_scale
    ).reshape(model_width, 2, text_rows)
    grad_cv = jnp.einsum(
        "htk,thd->hdk", cross_low, grad_cmix, preferred_element_type=WIDE
    ).reshape(model_width, 2, text_rows)
    slots = jnp.arange(clip_total, dtype=jnp.int32)
    in_first, in_second = (
        (slots == clip).astype(WIDE)[None, :, None] for clip in (first, second)
    )
    text_sums = [
        (part[:, :1] * in_first + part[:, 1:] * in_second).reshape(model_width, -1)
        for part in (grad_ck, grad_cv)
    ]
    text_sums = jnp.concatenate(text_sums, axis=1)
    text_cols = text_sums.shape[1]
    text_sums = jnp.pad(text_sums, ((0, 0), (0, -text_cols % 256)))
    grad_xquery = left_t(normed_two, grad_cq)
    grad_norm_two = right_t(grad_cq, full_xquery)
    norm_two_part, grad_gain_two, grad_bias_two = norm_back(after_self, gain_two, grad_norm_two)
    grad_self_res = grad_cross_res + norm_two_part
    branch_one = grad_self_res.astype(LOW)
    grad_output = left_t(attended, branch_one)
    fin_xoutput, fin_xquery, fin_output, text_share = summed_rows(
        [grad_xoutput, grad_xquery, grad_output, text_sums]
    )
    text_whole = lax.all_gather(text_share.astype(LOW), "shard", axis=0, tiled=True)
    flat_rows = clip_total * text_rows

    grad_attended = right_t(branch_one, full_output).astype(LOW)
    halves = jnp.transpose(grad_attended.reshape(tok_rows, 2, half_width), (1, 0, 2))
    chip_grad = core_pair(
        pick(halves, core, 0),
        swap(pick(halves, 1 - core, 0), BOTH, lambda i: i ^ 1),
        core,
        0,
    )
    calls = 2 if pairs % 2 == 0 else 1
    backs = ()
    for call in range(calls):
        backs = attend_back(
            offsets,
            queries,
            window,
            chip_mixed,
            logs,
            chip_grad,
            reach,
            call * pairs // calls,
            pairs // calls,
            tuple(backs),
        )
    chip_dq, grad_window = backs
    grad_pair = left_t(normed_around, grad_window)
    grad_wq = left_t(normed_chip, chip_dq)
    _, own_down, own_up, after_late, activ_late = lax.optimization_barrier(
        (grad_wq, own_down, own_up, after_cross, activ)
    )
    down_halves = rep_pair(own_down)
    fin_down = jnp.concatenate(down_halves, axis=0).reshape(w_down.shape).astype(WIDE)
    up_halves = rep_pair(own_up)
    fin_up = jnp.stack(
        [half.reshape(w_up.shape[0], 2, shard_count, chunk) for half in up_halves], axis=1
    )
    fin_up = jnp.transpose(fin_up, (0, 3, 1, 2, 4)).reshape(w_up.shape).astype(WIDE)
    mixed_both = matmul(activ_late[:, :quarter], half_down[0]) + matmul(
        activ_late[:, quarter:], half_down[1]
    )
    block_out = (
        after_late
        + mixed_both[:tok_rows]
        + swap(mixed_both[tok_rows:].astype(LOW), "rep", lambda i: i ^ 1).astype(WIDE)
    ).astype(LOW)
    fin_halves = summed_halves(grad_pair, grad_wq).reshape(shard_rows, 2, 3 * half_width)
    fin_pair = fin_halves[:, :, :model_width].reshape(shard_rows, 2, pairs, 2, 2 * HD)
    fin_query = fin_halves[:, :, model_width:].reshape(w_query.shape)
    fin_key = fin_pair[:, :, :, 0].reshape(w_query.shape)
    fin_value = fin_pair[:, :, :, 1].reshape(w_query.shape)
    grad_around = right_t(grad_window, part_pair)
    grad_chip = grad_around[halo_rows:] + right_t(chip_dq, part_query)
    around_sums = [
        jnp.sum(grad_around[:halo_rows] * normed_plain[:halo_rows], axis=0)
        + jnp.sum(grad_chip * normed_plain[halo_rows:], axis=0),
        jnp.sum(grad_around[:halo_rows], axis=0) + jnp.sum(grad_chip, axis=0),
    ]
    grad_halo = grad_around[:halo_rows].astype(LOW)
    _, text_whole = lax.optimization_barrier((grad_halo, text_whole))
    key_round, value_round = (
        text_whole[:, :flat_rows],
        text_whole[:, flat_rows : 2 * flat_rows],
    )
    col_start = lax.axis_index("shard") * shard_rows
    text_flat = text_states.reshape(flat_rows, model_width)
    text_slice = lax.dynamic_slice_in_dim(text_flat, col_start, shard_rows, 1)

    def mixed_dims(left, right):
        return lax.dot_general(
            left, right, (((0,), (1,)), ((), ())), preferred_element_type=WIDE
        )

    grad_xkey = mixed_dims(text_slice, key_round)
    grad_xvalue = mixed_dims(text_slice, value_round)
    grad_text = mixed_dims(key_round, full_xkey) + mixed_dims(value_round, full_xvalue)
    grad_text = grad_text.reshape(clip_total, text_rows, model_width)
    units = jnp.concatenate([grad_halo[tok_rows:], grad_chip.astype(LOW)], axis=0)
    units = units.reshape(3, 2, tok_rows, model_width)
    sent = jnp.concatenate([pick(units, 1 - core, 1), grad_halo[None, :tok_rows]], axis=0)
    partner = swap(sent, BOTH, lambda i: i ^ 1)
    sums = add_low(pick(units, core, 1), partner[:3])
    low_sum = add_low(grad_halo[:tok_rows], partner[3])
    back = swap(sums[1], BOTH, lambda i: i ^ 2).astype(WIDE)
    back_half = swap(low_sum, BOTH, lambda i: i ^ 2 if i % 2 == 1 else -1)
    to_below = (
        sums[0].astype(WIDE) + jnp.where(side == 0, back_half.astype(WIDE), back)
    ).astype(LOW)
    grad_norm_one = (
        sums[2].astype(WIDE)
        + jnp.where(side == 0, back, 0.0)
        + swap(to_below, BOTH, lambda i: i - 4).astype(WIDE)
        + swap(back_half, BOTH, lambda i: i - 8 if i % 4 == 3 else -1).astype(WIDE)
    )
    norm_one_part, _, _ = norm_back(resid, gain_one, grad_norm_one)
    grad_gain_one, grad_bias_one = around_sums
    grad_hidden = (grad_self_res + norm_one_part).astype(LOW)
    vectors = summed_vectors(
        jnp.stack(
            [
                grad_gain_one,
                grad_bias_one,
                grad_gain_two,
                grad_bias_two,
                grad_gain_three,
                grad_bias_three,
            ]
        ),
    )
    fin_gain_one, fin_bias_one, fin_gain_two, fin_bias_two, fin_gain_three, fin_bias_three = (
        lax.dynamic_slice_in_dim(vectors, col_start, shard_rows, 1)
    )
    return (
        block_out,
        grad_hidden,
        grad_text,
        fin_gain_one,
        fin_bias_one,
        fin_query,
        fin_key,
        fin_value,
        fin_output,
        fin_gain_two,
        fin_bias_two,
        fin_xquery,
        grad_xkey,
        grad_xvalue,
        fin_xoutput,
        fin_gain_three,
        fin_bias_three,
        fin_up,
        fin_down,
    )


def solution(mesh):
    rows, vector, tokens = P("shard", None), P("shard"), P(BOTH, None)
    placed = (
        (tokens, P(), P(BOTH), P(BOTH))
        + (vector, vector, rows, rows, rows, rows)
        + (vector, vector, rows, rows, rows, rows)
        + (vector, vector, rows, rows, tokens)
    )
    return jax.shard_map(
        on_device,
        mesh=mesh,
        in_specs=placed,
        out_specs=(
            (tokens, tokens, P())
            + (vector, vector, rows, rows, rows, rows)
            + (vector, vector, rows, rows, rows, rows)
            + (vector, vector, rows, rows)
        ),
        check_vma=False,
    )
```

```python
import functools

import jax
import jax.numpy as jnp
from jax import lax
from jax.experimental import pallas as pl
from jax.experimental.pallas import tpu as pltpu
from jax.sharding import PartitionSpec as P


HD = 64
CLIP_MAX = 1280
EPSILON = 1e-05
NEGATIVE = -1e30
BLOCK = 256
BOTH = ("rep", "shard")
LOW = jnp.bfloat16
WIDE = jnp.float32


def normalize(values):
    centre = values - jnp.mean(values, axis=-1, keepdims=True)
    spread = jnp.mean(centre * centre, axis=-1, keepdims=True)
    return centre * lax.rsqrt(spread + EPSILON)


def scaled_norm(values, scale_vec):
    return normalize(values) * scale_vec


def gelu_parts(values):
    below = 0.5 + 0.5 * lax.erf(values * (0.5**0.5))
    density = jnp.exp(-0.5 * values * values) * ((2.0 * jnp.pi) ** -0.5)
    return values * below, below + values * density


def matmul(left, right):
    return jnp.dot(left, right, preferred_element_type=WIDE)


def left_t(left, right):
    return lax.dot_general(left, right, (((0,), (0,)), ((), ())), preferred_element_type=WIDE)


def right_t(left, right):
    return lax.dot_general(left, right, (((1,), (1,)), ((), ())), preferred_element_type=WIDE)


def norm_back(values, scale_vec, upstream):
    _, pull = jax.vjp(scaled_norm, values, scale_vec.astype(WIDE))
    grad_values, grad_scale = pull(upstream)
    return (grad_values, grad_scale, jnp.sum(upstream, axis=0))


def pick(array, index, axis):
    return lax.dynamic_index_in_dim(array, index, axis, False)


def axis_length(axis):
    return lax.axis_size(axis)


def swap(array, axis, pairing, log=None):
    length = axis_length(axis)
    pairs = [(i, pairing(i)) for i in range(length)]
    if log is not None:
        log.append(array)
    return lax.ppermute(array, axis, [(i, j) for i, j in pairs if 0 <= j < length])


def after(values, earlier):
    return lax.optimization_barrier((values, list(earlier)))[0]


def add_low(left, right):
    return (left.astype(WIDE) + right.astype(WIDE)).astype(LOW)


def gather_rows(array):
    return lax.all_gather(array, "shard", axis=0, tiled=True)


def joined(parts):
    return parts[0] if len(parts) == 1 else jnp.concatenate(parts, axis=-1)


def positions(grads):
    index, rep = lax.axis_index("shard"), lax.axis_index("rep")
    grads, index, rep = lax.optimization_barrier((grads, index, rep))
    return grads, index % 2, (index // 2) % 2, index // 4, rep


def across_cores(grads, core):
    rows = grads[0].shape[0] // 16
    parts = [grad.reshape(8, 2, rows, grad.shape[1]) for grad in grads]
    away = joined([pick(part, 1 - core, 1) for part in parts])
    held = joined([pick(part, core, 1) for part in parts])
    return add_low(held, swap(away, "shard", lambda i: i ^ 1))


def level_sends(both, level, log=None):
    axis = both.ndim - 3
    return [
        swap(pick(both, (level + step) % 4, axis), "shard", lambda i: (i + 4 * step) % 16, log)
        for step in range(1, 4)
    ]


def level_total(both, got, level):
    total = pick(both, level, both.ndim - 3).astype(WIDE)
    for part in got:
        total = total + part.astype(WIDE)
    return total.astype(LOW)


def box_middle(firsts, seconds, side, rep, log):
    rows = firsts[0].shape[-2]
    firsts = [part.reshape(4, 2, *part.shape[-2:]) for part in firsts]
    seconds = [part.reshape(4, 2, 2, rows // 2, part.shape[-1]) for part in seconds]
    second = add_low(
        joined([pick(part, rep, 2) for part in seconds]),
        swap(joined([pick(part, 1 - rep, 2) for part in seconds]), "rep", lambda i: i ^ 1, log),
    )
    first = add_low(
        joined([pick(part, side, 1) for part in firsts]),
        swap(joined([pick(part, 1 - side, 1) for part in firsts]), "shard", lambda i: i ^ 2, log),
    )
    first = first.reshape(4, 2, rows // 2, first.shape[-1])
    first = add_low(
        pick(first, rep, 1),
        swap(pick(first, 1 - rep, 1), "rep", lambda i: i ^ 1, log),
    )
    second = add_low(
        pick(second, side, 1),
        swap(pick(second, 1 - side, 1), "shard", lambda i: i ^ 2, log),
    )
    return jnp.concatenate([first, second], axis=2)


def plane_middle(grad):
    grad, core, side, level, _ = positions(grad)
    count, rows, width = grad.shape[0], grad.shape[1] // 16, grad.shape[2]
    parts = grad.reshape(count, 8, 2, rows, width)
    held = add_low(
        pick(parts, core, 2),
        swap(pick(parts, 1 - core, 2), "shard", lambda i: i ^ 1),
    ).reshape(count, 4, 2, rows, width)
    held = add_low(
        pick(held, side, 2),
        swap(pick(held, 1 - side, 2), "shard", lambda i: i ^ 2),
    )
    return held, level_sends(held, level), level


def rep_pair(own, earlier=()):
    other = swap(own, "rep", lambda i: i ^ 1)
    if earlier:
        own, other = after((own, other), earlier)
    rep = lax.axis_index("rep")
    return jnp.where(rep == 0, own, other), jnp.where(rep == 0, other, own)


def rep_rows(own, earlier=()):
    low, high = rep_pair(own, earlier)
    return jnp.concatenate([low, high], axis=0)


def plain_rows(grads):
    share = lax.psum_scatter(joined(grads), "shard", scatter_dimension=0, tiled=True)
    return lax.psum(share.astype(WIDE), "rep").astype(LOW)


def head_lanes(which):
    lane = lax.broadcasted_iota(jnp.int32, (BLOCK, 2 * HD), 1)
    return lane < HD if which == 0 else lane >= HD


def open_pairs(offsets, step, reach):
    base = (reach - step) * BLOCK
    keys = lax.broadcasted_iota(jnp.int32, (BLOCK, BLOCK), 0)
    column = lax.broadcasted_iota(jnp.int32, (1, BLOCK), 1)
    allowed = keys >= (column - offsets) + base
    if base == 0:
        allowed = allowed & (keys <= lax.broadcasted_iota(jnp.int32, (BLOCK, BLOCK), 1))
    return allowed


def attend_kernel(reach, offset_ref, query_ref, window_ref, out_ref, log_ref, held):
    start = pl.program_id(1) * BLOCK
    offsets = offset_ref[...]
    scaled = query_ref[...] * jnp.asarray(HD**-0.5, LOW)
    mixed = []
    for head in range(2):
        query = jnp.where(head_lanes(head), scaled, jnp.zeros_like(scaled))
        peak = jnp.full((1, BLOCK), NEGATIVE, WIDE)
        for step in range(reach + 1):
            rows = pl.ds(pl.multiple_of(start + step * BLOCK, BLOCK), BLOCK)
            scores = right_t(window_ref[rows, : 2 * HD], query)
            scores = jnp.where(open_pairs(offsets, step, reach), scores, NEGATIVE)
            held[head, step] = scores
            peak = jnp.maximum(peak, jnp.max(scores, axis=0, keepdims=True))
        total = jnp.zeros((1, BLOCK), WIDE)
        blend = jnp.zeros((2 * HD, BLOCK), WIDE)
        for step in range(reach + 1):
            rows = pl.ds(pl.multiple_of(start + step * BLOCK, BLOCK), BLOCK)
            expo = jnp.exp(held[head, step] - peak)
            total = total + jnp.sum(expo, axis=0, keepdims=True)
            blend = blend + left_t(window_ref[rows, 2 * HD :], expo.astype(LOW))
        mixed.append((blend / total)[head * HD : (head + 1) * HD])
        log_ref[0, pl.ds(head, 1), :] = peak + jnp.log(total)
    out_ref[...] = jnp.concatenate(mixed, axis=0).T.astype(LOW)


def attend(offsets, queries, window, reach):
    rows, width = queries.shape
    pairs, blocks, context = width // (2 * HD), rows // BLOCK, window.shape[0]
    work = pairs * 2 * rows * (reach + 1) * BLOCK
    return pl.pallas_call(
        functools.partial(attend_kernel, reach),
        grid=(pairs, blocks),
        in_specs=[
            pl.BlockSpec((1, BLOCK), lambda p, b: (0, b)),
            pl.BlockSpec((BLOCK, 2 * HD), lambda p, b: (b, p)),
            pl.BlockSpec((context, 4 * HD), lambda p, b: (0, p)),
        ],
        out_specs=[
            pl.BlockSpec((BLOCK, 2 * HD), lambda p, b: (b, p)),
            pl.BlockSpec((1, 2, BLOCK), lambda p, b: (p, 0, b)),
        ],
        out_shape=[
            jax.ShapeDtypeStruct((rows, width), LOW),
            jax.ShapeDtypeStruct((pairs, 2, rows), WIDE),
        ],
        scratch_shapes=[pltpu.VMEM((2, reach + 1, BLOCK, BLOCK), WIDE)],
        cost_estimate=pl.CostEstimate(
            flops=16 * HD * work, transcendentals=work, bytes_accessed=8 * rows * width
        ),
        name="attend_forward",
    )(offsets, queries, window)


def attend_back_kernel(
    reach,
    offset_ref,
    query_ref,
    window_ref,
    out_ref,
    log_ref,
    grad_ref,
    *rest,
):
    grad_query_ref, grad_window_ref, grad_keys, grad_values = rest[-4:]
    block = pl.program_id(1)
    start = block * BLOCK

    @pl.when(block == 0)
    def _():
        grad_keys[...] = jnp.zeros_like(grad_keys)
        grad_values[...] = jnp.zeros_like(grad_values)

    offsets = offset_ref[...]
    scaled = query_ref[...] * jnp.asarray(HD**-0.5, LOW)
    grads = grad_ref[...]
    inner = (grads.astype(WIDE) * out_ref[...].astype(WIDE)).T
    query, grad, inners, logs = [], [], [], []
    for head in range(2):
        lanes = head_lanes(head)
        query.append(jnp.where(lanes, scaled, jnp.zeros_like(scaled)))
        grad.append(jnp.where(lanes, grads, jnp.zeros_like(grads)))
        inners.append(jnp.sum(inner[head * HD : (head + 1) * HD], axis=0, keepdims=True))
        logs.append(log_ref[0, pl.ds(head, 1), :])
    back = [jnp.zeros((2 * HD, BLOCK), WIDE) for _ in range(2)]
    for step in range(reach + 1):
        rows = pl.ds(pl.multiple_of(start + step * BLOCK, BLOCK), BLOCK)
        key, value = window_ref[rows, : 2 * HD], window_ref[rows, 2 * HD :]
        allowed = open_pairs(offsets, step, reach)
        to_key = jnp.zeros((BLOCK, 2 * HD), WIDE)
        to_value = jnp.zeros((BLOCK, 2 * HD), WIDE)
        for head in range(2):
            scores = jnp.where(allowed, right_t(key, query[head]), NEGATIVE)
            probs = jnp.exp(scores - logs[head])
            to_value = to_value + matmul(probs.astype(LOW), grad[head])
            grad_probs = right_t(value, grad[head])
            grad_scores = (probs * (grad_probs - inners[head])).astype(LOW)
            to_key = to_key + matmul(grad_scores, query[head])
            back[head] = back[head] + left_t(key, grad_scores)
        grad_keys[rows, :] += to_key
        grad_values[rows, :] += to_value
    back = jnp.concatenate([back[0][:HD], back[1][HD:]], axis=0) * (HD**-0.5)
    grad_query_ref[...] = back.T.astype(LOW)

    @pl.when(block == pl.num_programs(1) - 1)
    def _():
        grad_window_ref[:, : 2 * HD] = grad_keys[...].astype(LOW)
        grad_window_ref[:, 2 * HD :] = grad_values[...].astype(LOW)


def attend_back(offsets, queries, window, out, logs, grads, reach, begin, pairs, filled):
    rows, width = queries.shape
    blocks, context = rows // BLOCK, window.shape[0]
    work = pairs * 2 * rows * (reach + 1) * BLOCK
    row_block = pl.BlockSpec((BLOCK, 2 * HD), lambda p, b: (b, p + begin))
    window_block = pl.BlockSpec((context, 4 * HD), lambda p, b: (0, p + begin))
    return pl.pallas_call(
        functools.partial(attend_back_kernel, reach),
        grid=(pairs, blocks),
        in_specs=[
            pl.BlockSpec((1, BLOCK), lambda p, b: (0, b)),
            row_block,
            window_block,
            row_block,
            pl.BlockSpec((1, 2, BLOCK), lambda p, b: (p + begin, 0, b)),
            row_block,
        ]
        + [pl.BlockSpec(memory_space=pl.ANY)] * len(filled),
        out_specs=[row_block, window_block],
        out_shape=[
            jax.ShapeDtypeStruct((rows, width), LOW),
            jax.ShapeDtypeStruct(window.shape, LOW),
        ],
        input_output_aliases={6 + i: i for i in range(len(filled))},
        scratch_shapes=[
            pltpu.VMEM((context, 2 * HD), WIDE),
            pltpu.VMEM((context, 2 * HD), WIDE),
        ],
        cost_estimate=pl.CostEstimate(
            flops=40 * HD * work, transcendentals=work, bytes_accessed=16 * rows * width
        ),
        name="attend_backward",
    )(offsets, queries, window, out, logs, grads, *filled)


def unpack_kernel(width, own_ref, got_ref, *outs):
    core = lax.axis_index("shard") % 2
    for half in range(2):
        base = half * width // 2
        whole = jnp.where(core == half, own_ref[...], got_ref[...]).astype(WIDE)
        for pair in range(width // (4 * HD)):
            lanes = slice(base + pair * 2 * HD, base + (pair + 1) * 2 * HD)
            for kind in range(2):
                start = (2 * pair + kind) * 2 * HD
                outs[1 + kind][:, lanes] = whole[:, start : start + 2 * HD]
        outs[0][:, base : base + width // 2] = whole[:, width:]


def unpack(own, got):
    rows, width = own.shape[0], own.shape[1] * 2 // 3
    return pl.pallas_call(
        functools.partial(unpack_kernel, width),
        out_shape=[jax.ShapeDtypeStruct((rows, width), WIDE)] * 3,
        cost_estimate=pl.CostEstimate(
            flops=0, transcendentals=0, bytes_accessed=18 * rows * width
        ),
        name="unpack_query_key_value",
    )(own, got)


def core_pair(own, got, core, axis):
    return jnp.where(
        core == 0,
        jnp.concatenate([own, got], axis=axis),
        jnp.concatenate([got, own], axis=axis),
    )


def on_device(
    hidden,
    text_states,
    clip_index,
    frame_offset,
    self_gain,
    self_bias,
    w_query,
    w_key,
    w_value,
    w_output,
    cross_gain,
    cross_bias,
    x_query,
    x_key,
    x_value,
    x_output,
    final_gain,
    final_bias,
    w_up,
    w_down,
    cotangent,
):
    tok_rows, model_width = hidden.shape
    head_count = model_width // HD
    half_width = model_width // 2
    reach = (CLIP_MAX - 2) // tok_rows + 1
    key_scale = HD ** (-0.5)
    clip_total = text_states.shape[0]
    text_rows = text_states.shape[1]
    shard_count, rep_count = axis_length("shard"), axis_length("rep")
    shard_rows = x_key.shape[0]
    place = lax.axis_index("rep") * shard_count + lax.axis_index("shard")
    core, side = place % 2, (place // 2) % 2

    params = jnp.stack(
        [self_gain, self_bias, cross_gain, cross_bias, final_gain, final_bias], axis=1
    )
    params = jnp.pad(params, ((0, 0), (0, 128 - params.shape[1])))
    pairs = head_count // 4
    pair_split = (shard_rows, 2, pairs, 1, 2 * HD)
    key_value = jnp.concatenate([w_key.reshape(pair_split), w_value.reshape(pair_split)], axis=3)
    key_value = key_value.reshape(shard_rows, 2, model_width)
    first_group = gather_rows(
        jnp.concatenate(
            [
                part
                for h in range(2)
                for part in (w_query[:, h * half_width : (h + 1) * half_width], key_value[:, h])
            ]
            + [w_output, params],
            axis=1,
        ),
    )
    full_output = first_group[:, 3 * model_width : 4 * model_width]
    gain_one, bias_one, gain_two, bias_two, gain_three, bias_three = (
        first_group[:, 4 * model_width + i].astype(WIDE) for i in range(6)
    )
    part_all = lax.dynamic_slice_in_dim(
        first_group, core * (3 * half_width), 3 * half_width, 1
    )
    part_query, part_pair = part_all[:, :half_width], part_all[:, half_width:]
    second_group = gather_rows(jnp.concatenate([x_query, x_key, x_value, x_output], axis=1))
    full_xquery, full_xkey, full_xvalue, full_xoutput = (
        second_group[:, i * model_width : (i + 1) * model_width] for i in range(4)
    )
    rep_index = lax.axis_index("rep")
    down_rows = w_down.shape[0]
    chunk = down_rows // 4
    some_up = pick(w_up.reshape(w_up.shape[0], shard_count, 2, 2, chunk), rep_index, 2)
    some_up = jnp.transpose(some_up, (0, 2, 1, 3)).reshape(w_up.shape[0], -1)
    some_down = pick(w_down.reshape(2, 2, chunk, model_width), rep_index, 0)
    hidden_half = some_up.shape[1]
    third_group = gather_rows(jnp.concatenate([some_up, some_down[0], some_down[1]], axis=1))
    half_up = third_group[:, :hidden_half]
    half_down = [
        third_group[:, hidden_half + i * model_width : hidden_half + (i + 1) * model_width]
        for i in range(2)
    ]
    upstream = jnp.concatenate([cotangent, swap(cotangent, "rep", lambda i: i ^ 1)], axis=0)

    offsets = core_pair(frame_offset, swap(frame_offset, BOTH, lambda i: i ^ 1), core, 0)[None, :]
    resid = hidden.astype(WIDE)
    below = swap(hidden, BOTH, lambda i: i + 4)
    far = swap(hidden, BOTH, lambda i: i + 8 if i % 4 == 3 else -1)
    across = swap(jnp.where(side == 0, hidden, below), BOTH, lambda i: i ^ 2)
    third = swap(jnp.where(side == 0, below, far), BOTH, lambda i: i ^ 2 if i % 2 == 1 else -1)
    shards = jnp.stack([below, across, hidden, third])
    partner = swap(shards, BOTH, lambda i: i ^ 1)
    paired = core_pair(shards[:3], partner[:3], core, 1)
    around = jnp.concatenate(
        [jnp.where(core == 1, third, partner[3]), paired[0], paired[1], paired[2]], axis=0
    )
    chip_rows = 2 * tok_rows
    halo_rows = tok_rows + 2 * chip_rows
    normed_plain = normalize(around.astype(WIDE))
    normed_around = (normed_plain * gain_one + bias_one).astype(LOW)
    normed_plain = normed_plain.astype(LOW)
    normed_chip = normed_around[halo_rows:]
    window = matmul(normed_around, part_pair).astype(LOW)
    queries = matmul(normed_chip, part_query).astype(LOW)
    chip_mixed, logs = attend(offsets, queries, window, reach)

    def to_tokens(chip_rows_array):
        mine = lax.dynamic_slice_in_dim(chip_rows_array, core * tok_rows, tok_rows, 0)
        away = lax.dynamic_slice_in_dim(chip_rows_array, (1 - core) * tok_rows, tok_rows, 0)
        return core_pair(mine, swap(away, BOTH, lambda i: i ^ 1), core, 1)

    attended = to_tokens(chip_mixed)
    after_self = resid + matmul(attended, full_output)
    normed_two = (scaled_norm(after_self, gain_two) + bias_two).astype(LOW)
    cross_q = matmul(normed_two, full_xquery).astype(LOW)
    first = clip_index[0]
    second = jnp.minimum(first + 1, clip_total - 1)
    chosen = jnp.concatenate(
        [
            lax.dynamic_index_in_dim(text_states, first, 0, False),
            lax.dynamic_index_in_dim(text_states, second, 0, False),
        ],
        axis=0,
    )
    cross_k = matmul(chosen, full_xkey).astype(LOW)
    cross_v = matmul(chosen, full_xvalue).astype(LOW)
    slot = jnp.arange(2 * text_rows, dtype=jnp.int32) // text_rows
    slot_clip = jnp.where(slot == 0, first, second)
    open_slot = (slot == 0) | (second != first)
    cross_mask = (clip_index[:, None] == slot_clip[None, :]) & open_slot[None, :]
    cq_heads = cross_q.reshape(tok_rows, head_count, HD)
    ck_heads = cross_k.reshape(2 * text_rows, head_count, HD)
    cv_heads = cross_v.reshape(2 * text_rows, head_count, HD)
    cross_scores = (
        jnp.einsum("thd,khd->htk", cq_heads, ck_heads, preferred_element_type=WIDE) * key_scale
    )
    cross_scores = jnp.where(cross_mask[None], cross_scores, NEGATIVE)
    cross_probs = jax.nn.softmax(cross_scores, axis=2)
    cross_low = cross_probs.astype(LOW)
    cross_mix = (
        jnp.einsum("htk,khd->thd", cross_low, cv_heads, preferred_element_type=WIDE)
        .reshape(tok_rows, model_width)
        .astype(LOW)
    )
    after_cross = after_self + matmul(cross_mix, full_xoutput)
    normed_three = (scaled_norm(after_cross, gain_three) + bias_three).astype(LOW)
    both_three = jnp.concatenate([normed_three, swap(normed_three, "rep", lambda i: i ^ 1)], axis=0)
    quarter = hidden_half // 2
    activ, slope, grad_pre = [], [], []
    for i in range(2):
        pre_act = matmul(both_three, half_up[:, i * quarter : (i + 1) * quarter])
        shaped, steep = gelu_parts(pre_act)
        shaped, steep = lax.optimization_barrier((shaped.astype(LOW), steep))
        activ.append(shaped)
        slope.append(steep)
    for i in range(2):
        grad_pre.append((slope[i] * right_t(upstream, half_down[i])).astype(LOW))
    activ, grad_pre = jnp.concatenate(activ, axis=1), jnp.concatenate(grad_pre, axis=1)
    grad_both = right_t(grad_pre, half_up)
    grad_norm_three = grad_both[:tok_rows] + swap(
        grad_both[tok_rows:].astype(LOW), "rep", lambda i: i ^ 1
    ).astype(WIDE)
    grad_down = left_t(activ, upstream).astype(LOW).reshape(2, -1, model_width)
    grad_up = left_t(both_three, grad_pre).astype(LOW)
    if shard_count == 16:
        down_held, down_got, down_level = plane_middle(grad_down)
        up_held, up_got, up_level = plane_middle(grad_up[None])
    norm_three_part, grad_gain_three, grad_bias_three = norm_back(
        after_cross, gain_three, grad_norm_three
    )
    grad_cross_res = cotangent.astype(WIDE) + norm_three_part
    branch_two = grad_cross_res.astype(LOW)
    grad_xoutput = left_t(cross_mix, branch_two)
    grad_cmix = right_t(branch_two, full_xoutput).astype(LOW)
    grad_cmix = grad_cmix.reshape(tok_rows, head_count, HD)
    grad_cprob = jnp.einsum("thd,khd->htk", grad_cmix, cv_heads, preferred_element_type=WIDE)
    cross_inner = jnp.sum(cross_probs * grad_cprob, axis=2, keepdims=True)
    grad_cscore = (cross_probs * (grad_cprob - cross_inner)).astype(LOW)
    grad_cq = (
        (jnp.einsum("htk,khd->thd", grad_cscore, ck_heads, preferred_element_type=WIDE) * key_scale)
        .reshape(tok_rows, model_width)
        .astype(LOW)
    )
    grad_ck = (
        jnp.einsum("htk,thd->hdk", grad_cscore, cq_heads, preferred_element_type=WIDE) * key_scale
    ).reshape(model_width, 2 * text_rows)
    grad_cv = jnp.einsum(
        "htk,thd->hdk", cross_low, grad_cmix, preferred_element_type=WIDE
    ).reshape(model_width, 2 * text_rows)
    text_pair = jnp.concatenate([grad_ck, grad_cv], axis=1).astype(LOW)
    flat_rows = clip_total * text_rows
    text_cols = 2 * flat_rows
    target = jnp.concatenate([slot_clip, slot_clip + clip_total]) * text_rows
    target = target + jnp.arange(4 * text_rows, dtype=jnp.int32) % text_rows
    spread_text = target[:, None] == jnp.arange(text_cols, dtype=jnp.int32)[None, :]
    text_sums = matmul(text_pair, spread_text.astype(LOW)).astype(LOW)
    grad_xquery = left_t(normed_two, grad_cq)
    grad_norm_two = right_t(grad_cq, full_xquery)
    norm_two_part, grad_gain_two, grad_bias_two = norm_back(after_self, gain_two, grad_norm_two)
    grad_self_res = grad_cross_res + norm_two_part
    branch_one = grad_self_res.astype(LOW)
    grad_output = left_t(attended, branch_one)
    text_share = lax.psum_scatter(text_sums, BOTH, scatter_dimension=0, tiled=True)
    staged = shard_count == 16 and rep_count == 2
    if staged:
        grads, x_core, x_side, x_level, x_rep = positions(
            [grad.astype(LOW) for grad in (grad_xoutput, grad_xquery, grad_output)]
        )
        held = across_cores(grads, x_core)
        middle = held.shape[-1] // 2
        x_both = box_middle([held[..., :middle]], [held[..., middle:]], x_side, x_rep, [])
        x_got = level_sends(x_both, x_level)
    grad_attended = right_t(branch_one, full_output).astype(LOW)
    halves = jnp.transpose(grad_attended.reshape(tok_rows, 2, half_width), (1, 0, 2))
    chip_grad = core_pair(
        pick(halves, core, 0),
        swap(pick(halves, 1 - core, 0), BOTH, lambda i: i ^ 1),
        core,
        0,
    )
    calls = 2 if pairs % 2 == 0 else 1
    backs = ()
    for call in range(calls):
        backs = attend_back(
            offsets,
            queries,
            window,
            chip_mixed,
            logs,
            chip_grad,
            reach,
            call * pairs // calls,
            pairs // calls,
            tuple(backs),
        )
    chip_dq, grad_window = backs
    grad_pair = left_t(normed_around, grad_window)
    grad_wq = left_t(normed_chip, chip_dq)
    grad_pair, grad_wq = grad_pair.astype(LOW), grad_wq.astype(LOW)
    sent_first, sent_last = [], []
    if staged:
        (wide, narrow), q_core, q_side, q_level, q_rep = positions((grad_pair, grad_wq))
        wide, narrow = (part.reshape(8, -1, part.shape[1]) for part in (wide, narrow))
        middle = 3 * half_width // 2
        q_both = box_middle(
            [wide[..., :middle]], [wide[..., middle:], narrow], q_side, q_rep, sent_first
        )
    text_share, grad_window, chip_dq = after((text_share, grad_window, chip_dq), sent_first[:2])
    text_whole = lax.all_gather(text_share, BOTH, axis=0, tiled=True)
    grad_halo = right_t(grad_window[:halo_rows], part_pair)
    halo_sums = [
        jnp.sum(grad_halo * normed_plain[:halo_rows].astype(WIDE), axis=0),
        jnp.sum(grad_halo, axis=0),
    ]
    grad_chip = right_t(
        jnp.concatenate([chip_dq, grad_window[halo_rows:]], axis=1), part_all
    )
    chip_sums = [
        jnp.sum(grad_chip * normed_plain[halo_rows:].astype(WIDE), axis=0),
        jnp.sum(grad_chip, axis=0),
    ]
    around_sums = [halo_sums[i] + chip_sums[i] for i in range(2)]
    grad_halo = grad_halo.astype(LOW)
    units = jnp.concatenate([grad_halo[tok_rows:], grad_chip.astype(LOW)], axis=0)
    units = units.reshape(3, 2, tok_rows, model_width)
    sent = jnp.concatenate([pick(units, 1 - core, 1), grad_halo[None, :tok_rows]], axis=0)
    partner = swap(sent, BOTH, lambda i: i ^ 1)
    sums = add_low(pick(units, core, 1), partner[:3])
    low_sum = add_low(grad_halo[:tok_rows], partner[3])
    if staged:
        q_both = after(q_both, [sums, low_sum])
        q_got = level_sends(q_both, q_level, sent_last)
        q_own = level_total(q_both, q_got, q_level)
        parts = rep_rows(q_own).reshape(2, shard_rows, 3 * half_width)
        q_swapped = swap(pick(parts, 1 - q_core, 0), "shard", lambda i: i ^ 1)
        fin_query, fin_key, fin_value = unpack(pick(parts, q_core, 0), q_swapped)
        x_own = level_total(x_both, after(x_got, sent_first[2:]), x_level)
        fin_x = rep_rows(x_own, sent_last)
    else:
        filled = joined([grad_pair, grad_wq])
        fin_halves = plain_rows([core_pair(filled, jnp.zeros_like(filled), core, 1)])
        fin_x = plain_rows([grad.astype(LOW) for grad in (grad_xoutput, grad_xquery, grad_output)])
        fin_halves = fin_halves.astype(WIDE).reshape(shard_rows, 2, 3 * half_width)
        fin_pair = fin_halves[:, :, :model_width].reshape(shard_rows, 2, pairs, 2, 2 * HD)
        fin_query = fin_halves[:, :, model_width:].reshape(w_query.shape)
        fin_key = fin_pair[:, :, :, 0].reshape(w_query.shape)
        fin_value = fin_pair[:, :, :, 1].reshape(w_query.shape)
    fin_xoutput, fin_xquery, fin_output = (
        fin_x[:, i * model_width : (i + 1) * model_width].astype(WIDE) for i in range(3)
    )
    if staged:
        down_got, up_got = after((down_got, up_got), sent_first[2:])
        own_down = level_total(down_held, down_got, down_level)
        own_up = level_total(up_held, up_got, up_level)
    else:
        own_down = lax.psum_scatter(grad_down, "shard", scatter_dimension=1, tiled=True)
        own_up = lax.psum_scatter(grad_up[None], "shard", scatter_dimension=1, tiled=True)
    down_halves = rep_pair(own_down, sent_last)
    fin_down = jnp.concatenate(down_halves, axis=0).reshape(w_down.shape).astype(WIDE)
    up_halves = rep_pair(own_up, sent_last)
    fin_up = jnp.stack(
        [half.reshape(w_up.shape[0], 2, shard_count, chunk) for half in up_halves], axis=1
    )
    fin_up = jnp.transpose(fin_up, (0, 3, 1, 2, 4)).reshape(w_up.shape).astype(WIDE)
    activ_late, after_late = after((activ, after_cross), [grad_chip])
    mixed_both = matmul(activ_late[:, :quarter], half_down[0]) + matmul(
        activ_late[:, quarter:], half_down[1]
    )
    y_got = swap(mixed_both[tok_rows:].astype(LOW), "rep", lambda i: i ^ 1)
    y_own, y_got, after_late = after((mixed_both[:tok_rows], y_got, after_late), sent_last)
    block_out = (after_late + y_own + y_got.astype(WIDE)).astype(LOW)
    text_whole = after(text_whole, sent_last)
    key_round, value_round = (
        text_whole[:, :flat_rows],
        text_whole[:, flat_rows : 2 * flat_rows],
    )
    col_start = lax.axis_index("shard") * shard_rows
    text_flat = text_states.reshape(flat_rows, model_width)
    text_slice = lax.dynamic_slice_in_dim(text_flat, col_start, shard_rows, 1)

    def mixed_dims(left, right):
        return lax.dot_general(
            left, right, (((0,), (1,)), ((), ())), preferred_element_type=WIDE
        )

    grad_xkey = mixed_dims(text_slice, key_round)
    grad_xvalue = mixed_dims(text_slice, value_round)
    grad_text = mixed_dims(key_round, full_xkey) + mixed_dims(value_round, full_xvalue)
    grad_text = grad_text.reshape(clip_total, text_rows, model_width)
    back = swap(sums[1], BOTH, lambda i: i ^ 2).astype(WIDE)
    back_half = swap(low_sum, BOTH, lambda i: i ^ 2 if i % 2 == 1 else -1)
    to_below = (
        sums[0].astype(WIDE) + jnp.where(side == 0, back_half.astype(WIDE), back)
    ).astype(LOW)
    grad_norm_one = (
        sums[2].astype(WIDE)
        + jnp.where(side == 0, back, 0.0)
        + swap(to_below, BOTH, lambda i: i - 4).astype(WIDE)
        + swap(back_half, BOTH, lambda i: i - 8 if i % 4 == 3 else -1).astype(WIDE)
    )
    norm_one_part, _, _ = norm_back(resid, gain_one, grad_norm_one)
    grad_gain_one, grad_bias_one = around_sums
    grad_hidden = (grad_self_res + norm_one_part).astype(LOW)
    vectors = lax.all_gather(
        jnp.stack(
            [
                grad_gain_one,
                grad_bias_one,
                grad_gain_two,
                grad_bias_two,
                grad_gain_three,
                grad_bias_three,
            ]
        ),
        BOTH,
    )
    _, vectors = lax.optimization_barrier((to_below, vectors))
    vectors = jnp.sum(vectors, axis=0)
    fin_gain_one, fin_bias_one, fin_gain_two, fin_bias_two, fin_gain_three, fin_bias_three = (
        lax.dynamic_slice_in_dim(vectors, col_start, shard_rows, 1)
    )
    return (
        block_out,
        grad_hidden,
        grad_text,
        fin_gain_one,
        fin_bias_one,
        fin_query,
        fin_key,
        fin_value,
        fin_output,
        fin_gain_two,
        fin_bias_two,
        fin_xquery,
        grad_xkey,
        grad_xvalue,
        fin_xoutput,
        fin_gain_three,
        fin_bias_three,
        fin_up,
        fin_down,
    )


def solution(mesh):
    rows, vector, tokens = P("shard", None), P("shard"), P(BOTH, None)
    placed = (
        (tokens, P(), P(BOTH), P(BOTH))
        + (vector, vector, rows, rows, rows, rows)
        + (vector, vector, rows, rows, rows, rows)
        + (vector, vector, rows, rows, tokens)
    )
    return jax.shard_map(
        on_device,
        mesh=mesh,
        in_specs=placed,
        out_specs=(
            (tokens, tokens, P())
            + (vector, vector, rows, rows, rows, rows)
            + (vector, vector, rows, rows, rows, rows)
            + (vector, vector, rows, rows)
        ),
        check_vma=False,
    )
```

```python
import functools

import jax
import jax.numpy as jnp
from jax import lax
from jax.experimental import pallas as pl
from jax.experimental.pallas import tpu as pltpu
from jax.sharding import PartitionSpec as P


HD = 64
CLIP_MAX = 1280
EPSILON = 1e-05
NEGATIVE = -1e30
BLOCK = 256
BOTH = ("rep", "shard")
LOW = jnp.bfloat16
WIDE = jnp.float32


def normalize(values):
    centre = values - jnp.mean(values, axis=-1, keepdims=True)
    spread = jnp.mean(centre * centre, axis=-1, keepdims=True)
    return centre * lax.rsqrt(spread + EPSILON)


def scaled_norm(values, scale_vec):
    return normalize(values) * scale_vec


def gelu_parts(values):
    below = 0.5 + 0.5 * lax.erf(values * (0.5**0.5))
    density = jnp.exp(-0.5 * values * values) * ((2.0 * jnp.pi) ** -0.5)
    return values * below, below + values * density


def matmul(left, right):
    return jnp.dot(left, right, preferred_element_type=WIDE)


def left_t(left, right):
    return lax.dot_general(left, right, (((0,), (0,)), ((), ())), preferred_element_type=WIDE)


def right_t(left, right):
    return lax.dot_general(left, right, (((1,), (1,)), ((), ())), preferred_element_type=WIDE)


def norm_back(values, scale_vec, upstream):
    _, pull = jax.vjp(scaled_norm, values, scale_vec.astype(WIDE))
    grad_values, grad_scale = pull(upstream)
    return (grad_values, grad_scale, jnp.sum(upstream, axis=0))


def pick(array, index, axis):
    return lax.dynamic_index_in_dim(array, index, axis, False)


def axis_length(axis):
    return lax.axis_size(axis)


def swap(array, axis, pairing, log=None):
    length = axis_length(axis)
    pairs = [(i, pairing(i)) for i in range(length)]
    if log is not None:
        log.append(array)
    return lax.ppermute(array, axis, [(i, j) for i, j in pairs if 0 <= j < length])


def after(values, earlier):
    return lax.optimization_barrier((values, list(earlier)))[0]


def add_low(left, right):
    return (left.astype(WIDE) + right.astype(WIDE)).astype(LOW)


def gather_rows(array):
    return lax.all_gather(array, "shard", axis=0, tiled=True)


def joined(parts):
    return parts[0] if len(parts) == 1 else jnp.concatenate(parts, axis=-1)


def positions(grads):
    index, rep = lax.axis_index("shard"), lax.axis_index("rep")
    grads, index, rep = lax.optimization_barrier((grads, index, rep))
    return grads, index % 2, (index // 2) % 2, index // 4, rep


def across_cores(grads, core):
    rows = grads[0].shape[0] // 16
    parts = [grad.reshape(8, 2, rows, grad.shape[1]) for grad in grads]
    away = joined([pick(part, 1 - core, 1) for part in parts])
    held = joined([pick(part, core, 1) for part in parts])
    return add_low(held, swap(away, "shard", lambda i: i ^ 1))


def level_sends(both, level, log=None):
    axis = both.ndim - 3
    return [
        swap(pick(both, (level + step) % 4, axis), "shard", lambda i: (i + 4 * step) % 16, log)
        for step in range(1, 4)
    ]


def level_total(both, got, level):
    total = pick(both, level, both.ndim - 3).astype(WIDE)
    for part in got:
        total = total + part.astype(WIDE)
    return total.astype(LOW)


def box_middle(firsts, seconds, side, rep, log):
    rows = firsts[0].shape[-2]
    firsts = [part.reshape(4, 2, *part.shape[-2:]) for part in firsts]
    seconds = [part.reshape(4, 2, 2, rows // 2, part.shape[-1]) for part in seconds]
    second = add_low(
        joined([pick(part, rep, 2) for part in seconds]),
        swap(joined([pick(part, 1 - rep, 2) for part in seconds]), "rep", lambda i: i ^ 1, log),
    )
    first = add_low(
        joined([pick(part, side, 1) for part in firsts]),
        swap(joined([pick(part, 1 - side, 1) for part in firsts]), "shard", lambda i: i ^ 2, log),
    )
    first = first.reshape(4, 2, rows // 2, first.shape[-1])
    first = add_low(
        pick(first, rep, 1),
        swap(pick(first, 1 - rep, 1), "rep", lambda i: i ^ 1, log),
    )
    second = add_low(
        pick(second, side, 1),
        swap(pick(second, 1 - side, 1), "shard", lambda i: i ^ 2, log),
    )
    return jnp.concatenate([first, second], axis=2)


def plane_middle(grad):
    grad, core, side, level, _ = positions(grad)
    count, rows, width = grad.shape[0], grad.shape[1] // 16, grad.shape[2]
    parts = grad.reshape(count, 8, 2, rows, width)
    held = add_low(
        pick(parts, core, 2),
        swap(pick(parts, 1 - core, 2), "shard", lambda i: i ^ 1),
    ).reshape(count, 4, 2, rows, width)
    held = add_low(
        pick(held, side, 2),
        swap(pick(held, 1 - side, 2), "shard", lambda i: i ^ 2),
    )
    return held, level_sends(held, level), level


def rep_pair(own, earlier=()):
    other = swap(own, "rep", lambda i: i ^ 1)
    if earlier:
        own, other = after((own, other), earlier)
    rep = lax.axis_index("rep")
    return jnp.where(rep == 0, own, other), jnp.where(rep == 0, other, own)


def rep_rows(own, earlier=()):
    low, high = rep_pair(own, earlier)
    return jnp.concatenate([low, high], axis=0)


def plain_rows(grads):
    share = lax.psum_scatter(joined(grads), "shard", scatter_dimension=0, tiled=True)
    return lax.psum(share.astype(WIDE), "rep").astype(LOW)


def head_lanes(which):
    lane = lax.broadcasted_iota(jnp.int32, (BLOCK, 2 * HD), 1)
    return lane < HD if which == 0 else lane >= HD


def open_pairs(offsets, step, reach):
    base = (reach - step) * BLOCK
    keys = lax.broadcasted_iota(jnp.int32, (BLOCK, BLOCK), 0)
    column = lax.broadcasted_iota(jnp.int32, (1, BLOCK), 1)
    allowed = keys >= (column - offsets) + base
    if base == 0:
        allowed = allowed & (keys <= lax.broadcasted_iota(jnp.int32, (BLOCK, BLOCK), 1))
    return allowed


def attend_kernel(reach, offset_ref, query_ref, window_ref, out_ref, log_ref, held):
    start = pl.program_id(1) * BLOCK
    offsets = offset_ref[...]
    scaled = query_ref[...] * jnp.asarray(HD**-0.5, LOW)
    mixed = []
    for head in range(2):
        query = jnp.where(head_lanes(head), scaled, jnp.zeros_like(scaled))
        peak = jnp.full((1, BLOCK), NEGATIVE, WIDE)
        for step in range(reach + 1):
            rows = pl.ds(pl.multiple_of(start + step * BLOCK, BLOCK), BLOCK)
            scores = right_t(window_ref[rows, : 2 * HD], query)
            scores = jnp.where(open_pairs(offsets, step, reach), scores, NEGATIVE)
            held[head, step] = scores
            peak = jnp.maximum(peak, jnp.max(scores, axis=0, keepdims=True))
        total = jnp.zeros((1, BLOCK), WIDE)
        blend = jnp.zeros((2 * HD, BLOCK), WIDE)
        for step in range(reach + 1):
            rows = pl.ds(pl.multiple_of(start + step * BLOCK, BLOCK), BLOCK)
            expo = jnp.exp(held[head, step] - peak)
            total = total + jnp.sum(expo, axis=0, keepdims=True)
            blend = blend + left_t(window_ref[rows, 2 * HD :], expo.astype(LOW))
        mixed.append((blend / total)[head * HD : (head + 1) * HD])
        log_ref[0, pl.ds(head, 1), :] = peak + jnp.log(total)
    out_ref[...] = jnp.concatenate(mixed, axis=0).T.astype(LOW)


def attend(offsets, queries, window, reach):
    rows, width = queries.shape
    pairs, blocks, context = width // (2 * HD), rows // BLOCK, window.shape[0]
    work = pairs * 2 * rows * (reach + 1) * BLOCK
    return pl.pallas_call(
        functools.partial(attend_kernel, reach),
        grid=(pairs, blocks),
        in_specs=[
            pl.BlockSpec((1, BLOCK), lambda p, b: (0, b)),
            pl.BlockSpec((BLOCK, 2 * HD), lambda p, b: (b, p)),
            pl.BlockSpec((context, 4 * HD), lambda p, b: (0, p)),
        ],
        out_specs=[
            pl.BlockSpec((BLOCK, 2 * HD), lambda p, b: (b, p)),
            pl.BlockSpec((1, 2, BLOCK), lambda p, b: (p, 0, b)),
        ],
        out_shape=[
            jax.ShapeDtypeStruct((rows, width), LOW),
            jax.ShapeDtypeStruct((pairs, 2, rows), WIDE),
        ],
        scratch_shapes=[pltpu.VMEM((2, reach + 1, BLOCK, BLOCK), WIDE)],
        cost_estimate=pl.CostEstimate(
            flops=16 * HD * work, transcendentals=work, bytes_accessed=8 * rows * width
        ),
        name="attend_forward",
    )(offsets, queries, window)


def attend_back_kernel(
    reach,
    offset_ref,
    query_ref,
    window_ref,
    out_ref,
    log_ref,
    grad_ref,
    *rest,
):
    grad_query_ref, grad_window_ref, grad_keys, grad_values = rest[-4:]
    block = pl.program_id(1)
    start = block * BLOCK

    @pl.when(block == 0)
    def _():
        grad_keys[...] = jnp.zeros_like(grad_keys)
        grad_values[...] = jnp.zeros_like(grad_values)

    offsets = offset_ref[...]
    scaled = query_ref[...] * jnp.asarray(HD**-0.5, LOW)
    grads = grad_ref[...]
    inner = (grads.astype(WIDE) * out_ref[...].astype(WIDE)).T
    query, grad, inners, logs = [], [], [], []
    for head in range(2):
        lanes = head_lanes(head)
        query.append(jnp.where(lanes, scaled, jnp.zeros_like(scaled)))
        grad.append(jnp.where(lanes, grads, jnp.zeros_like(grads)))
        inners.append(jnp.sum(inner[head * HD : (head + 1) * HD], axis=0, keepdims=True))
        logs.append(log_ref[0, pl.ds(head, 1), :])
    back = [jnp.zeros((2 * HD, BLOCK), WIDE) for _ in range(2)]
    for step in range(reach + 1):
        rows = pl.ds(pl.multiple_of(start + step * BLOCK, BLOCK), BLOCK)
        key, value = window_ref[rows, : 2 * HD], window_ref[rows, 2 * HD :]
        allowed = open_pairs(offsets, step, reach)
        to_key = jnp.zeros((BLOCK, 2 * HD), WIDE)
        to_value = jnp.zeros((BLOCK, 2 * HD), WIDE)
        for head in range(2):
            scores = jnp.where(allowed, right_t(key, query[head]), NEGATIVE)
            probs = jnp.exp(scores - logs[head])
            to_value = to_value + matmul(probs.astype(LOW), grad[head])
            grad_probs = right_t(value, grad[head])
            grad_scores = (probs * (grad_probs - inners[head])).astype(LOW)
            to_key = to_key + matmul(grad_scores, query[head])
            back[head] = back[head] + left_t(key, grad_scores)
        grad_keys[rows, :] += to_key
        grad_values[rows, :] += to_value
    back = jnp.concatenate([back[0][:HD], back[1][HD:]], axis=0) * (HD**-0.5)
    grad_query_ref[...] = back.T.astype(LOW)

    @pl.when(block == pl.num_programs(1) - 1)
    def _():
        grad_window_ref[:, : 2 * HD] = grad_keys[...].astype(LOW)
        grad_window_ref[:, 2 * HD :] = grad_values[...].astype(LOW)


def attend_back(offsets, queries, window, out, logs, grads, reach, begin, pairs, filled):
    rows, width = queries.shape
    blocks, context = rows // BLOCK, window.shape[0]
    work = pairs * 2 * rows * (reach + 1) * BLOCK
    row_block = pl.BlockSpec((BLOCK, 2 * HD), lambda p, b: (b, p + begin))
    window_block = pl.BlockSpec((context, 4 * HD), lambda p, b: (0, p + begin))
    return pl.pallas_call(
        functools.partial(attend_back_kernel, reach),
        grid=(pairs, blocks),
        in_specs=[
            pl.BlockSpec((1, BLOCK), lambda p, b: (0, b)),
            row_block,
            window_block,
            row_block,
            pl.BlockSpec((1, 2, BLOCK), lambda p, b: (p + begin, 0, b)),
            row_block,
        ]
        + [pl.BlockSpec(memory_space=pl.ANY)] * len(filled),
        out_specs=[row_block, window_block],
        out_shape=[
            jax.ShapeDtypeStruct((rows, width), LOW),
            jax.ShapeDtypeStruct(window.shape, LOW),
        ],
        input_output_aliases={6 + i: i for i in range(len(filled))},
        scratch_shapes=[
            pltpu.VMEM((context, 2 * HD), WIDE),
            pltpu.VMEM((context, 2 * HD), WIDE),
        ],
        cost_estimate=pl.CostEstimate(
            flops=40 * HD * work, transcendentals=work, bytes_accessed=16 * rows * width
        ),
        name="attend_backward",
    )(offsets, queries, window, out, logs, grads, *filled)


def unpack_kernel(width, own_ref, got_ref, *outs):
    core = lax.axis_index("shard") % 2
    for half in range(2):
        base = half * width // 2
        whole = jnp.where(core == half, own_ref[...], got_ref[...]).astype(WIDE)
        for pair in range(width // (4 * HD)):
            lanes = slice(base + pair * 2 * HD, base + (pair + 1) * 2 * HD)
            for kind in range(2):
                start = (2 * pair + kind) * 2 * HD
                outs[1 + kind][:, lanes] = whole[:, start : start + 2 * HD]
        outs[0][:, base : base + width // 2] = whole[:, width:]


def unpack(own, got):
    rows, width = own.shape[0], own.shape[1] * 2 // 3
    return pl.pallas_call(
        functools.partial(unpack_kernel, width),
        out_shape=[jax.ShapeDtypeStruct((rows, width), WIDE)] * 3,
        cost_estimate=pl.CostEstimate(
            flops=0, transcendentals=0, bytes_accessed=18 * rows * width
        ),
        name="unpack_query_key_value",
    )(own, got)


def interleave_kernel(count, chunk, own_ref, other_ref, out_ref):
    rep = lax.axis_index("rep")
    own, other = own_ref[...].astype(WIDE), other_ref[...].astype(WIDE)
    halves = jnp.where(rep == 0, own, other), jnp.where(rep == 0, other, own)
    for index in range(count):
        parts = [
            half[:, (j * count + index) * chunk : (j * count + index + 1) * chunk]
            for half in halves
            for j in range(2)
        ]
        out_ref[:, 4 * chunk * index : 4 * chunk * (index + 1)] = jnp.concatenate(parts, axis=1)


def interleave(own, other, count, chunk):
    rows, width = own.shape
    return pl.pallas_call(
        functools.partial(interleave_kernel, count, chunk),
        out_shape=jax.ShapeDtypeStruct((rows, 2 * width), WIDE),
        cost_estimate=pl.CostEstimate(
            flops=0, transcendentals=0, bytes_accessed=12 * rows * width
        ),
        name="interleave_up",
    )(own, other)


def core_pair(own, got, core, axis):
    return jnp.where(
        core == 0,
        jnp.concatenate([own, got], axis=axis),
        jnp.concatenate([got, own], axis=axis),
    )


def on_device(
    hidden,
    text_states,
    clip_index,
    frame_offset,
    self_gain,
    self_bias,
    w_query,
    w_key,
    w_value,
    w_output,
    cross_gain,
    cross_bias,
    x_query,
    x_key,
    x_value,
    x_output,
    final_gain,
    final_bias,
    w_up,
    w_down,
    cotangent,
):
    tok_rows, model_width = hidden.shape
    head_count = model_width // HD
    half_width = model_width // 2
    reach = (CLIP_MAX - 2) // tok_rows + 1
    key_scale = HD ** (-0.5)
    clip_total = text_states.shape[0]
    text_rows = text_states.shape[1]
    shard_count, rep_count = axis_length("shard"), axis_length("rep")
    shard_rows = x_key.shape[0]
    place = lax.axis_index("rep") * shard_count + lax.axis_index("shard")
    core, side = place % 2, (place // 2) % 2

    params = jnp.stack(
        [self_gain, self_bias, cross_gain, cross_bias, final_gain, final_bias], axis=1
    )
    params = jnp.pad(params, ((0, 0), (0, 128 - params.shape[1])))
    pairs = head_count // 4
    pair_split = (shard_rows, 2, pairs, 1, 2 * HD)
    key_value = jnp.concatenate([w_key.reshape(pair_split), w_value.reshape(pair_split)], axis=3)
    key_value = key_value.reshape(shard_rows, 2, model_width)
    first_group = gather_rows(
        jnp.concatenate(
            [
                part
                for h in range(2)
                for part in (w_query[:, h * half_width : (h + 1) * half_width], key_value[:, h])
            ]
            + [w_output, params],
            axis=1,
        ),
    )
    full_output = first_group[:, 3 * model_width : 4 * model_width]
    gain_one, bias_one, gain_two, bias_two, gain_three, bias_three = (
        first_group[:, 4 * model_width + i].astype(WIDE) for i in range(6)
    )
    part_all = lax.dynamic_slice_in_dim(
        first_group, core * (3 * half_width), 3 * half_width, 1
    )
    part_query, part_pair = part_all[:, :half_width], part_all[:, half_width:]
    second_group = gather_rows(jnp.concatenate([x_query, x_key, x_value, x_output], axis=1))
    full_xquery, full_xkey, full_xvalue, full_xoutput = (
        second_group[:, i * model_width : (i + 1) * model_width] for i in range(4)
    )
    rep_index = lax.axis_index("rep")
    down_rows = w_down.shape[0]
    chunk = down_rows // 4
    some_up = pick(w_up.reshape(w_up.shape[0], shard_count, 2, 2, chunk), rep_index, 2)
    some_up = jnp.transpose(some_up, (0, 2, 1, 3)).reshape(w_up.shape[0], -1)
    some_down = pick(w_down.reshape(2, 2, chunk, model_width), rep_index, 0)
    hidden_half = some_up.shape[1]
    third_group = gather_rows(jnp.concatenate([some_up, some_down[0], some_down[1]], axis=1))
    half_up = third_group[:, :hidden_half]
    half_down = [
        third_group[:, hidden_half + i * model_width : hidden_half + (i + 1) * model_width]
        for i in range(2)
    ]
    upstream = jnp.concatenate([cotangent, swap(cotangent, "rep", lambda i: i ^ 1)], axis=0)

    offsets = core_pair(frame_offset, swap(frame_offset, BOTH, lambda i: i ^ 1), core, 0)[None, :]
    resid = hidden.astype(WIDE)
    below = swap(hidden, BOTH, lambda i: i + 4)
    far = swap(hidden, BOTH, lambda i: i + 8 if i % 4 == 3 else -1)
    across = swap(jnp.where(side == 0, hidden, below), BOTH, lambda i: i ^ 2)
    third = swap(jnp.where(side == 0, below, far), BOTH, lambda i: i ^ 2 if i % 2 == 1 else -1)
    shards = jnp.stack([below, across, hidden, third])
    partner = swap(shards, BOTH, lambda i: i ^ 1)
    paired = core_pair(shards[:3], partner[:3], core, 1)
    around = jnp.concatenate(
        [jnp.where(core == 1, third, partner[3]), paired[0], paired[1], paired[2]], axis=0
    )
    chip_rows = 2 * tok_rows
    halo_rows = tok_rows + 2 * chip_rows
    normed_plain = normalize(around.astype(WIDE))
    normed_around = (normed_plain * gain_one + bias_one).astype(LOW)
    normed_plain = normed_plain.astype(LOW)
    normed_chip = normed_around[halo_rows:]
    window = matmul(normed_around, part_pair).astype(LOW)
    queries = matmul(normed_chip, part_query).astype(LOW)
    chip_mixed, logs = attend(offsets, queries, window, reach)

    def to_tokens(chip_rows_array):
        mine = lax.dynamic_slice_in_dim(chip_rows_array, core * tok_rows, tok_rows, 0)
        away = lax.dynamic_slice_in_dim(chip_rows_array, (1 - core) * tok_rows, tok_rows, 0)
        return core_pair(mine, swap(away, BOTH, lambda i: i ^ 1), core, 1)

    attended = to_tokens(chip_mixed)
    after_self = resid + matmul(attended, full_output)
    normed_two = (scaled_norm(after_self, gain_two) + bias_two).astype(LOW)
    cross_q = matmul(normed_two, full_xquery).astype(LOW)
    first = clip_index[0]
    second = jnp.minimum(first + 1, clip_total - 1)
    chosen = jnp.concatenate(
        [
            lax.dynamic_index_in_dim(text_states, first, 0, False),
            lax.dynamic_index_in_dim(text_states, second, 0, False),
        ],
        axis=0,
    )
    cross_k = matmul(chosen, full_xkey).astype(LOW)
    cross_v = matmul(chosen, full_xvalue).astype(LOW)
    slot = jnp.arange(2 * text_rows, dtype=jnp.int32) // text_rows
    slot_clip = jnp.where(slot == 0, first, second)
    open_slot = (slot == 0) | (second != first)
    cross_mask = (clip_index[:, None] == slot_clip[None, :]) & open_slot[None, :]
    cq_heads = cross_q.reshape(tok_rows, head_count, HD)
    ck_heads = cross_k.reshape(2 * text_rows, head_count, HD)
    cv_heads = cross_v.reshape(2 * text_rows, head_count, HD)
    cross_scores = (
        jnp.einsum("thd,khd->htk", cq_heads, ck_heads, preferred_element_type=WIDE) * key_scale
    )
    cross_scores = jnp.where(cross_mask[None], cross_scores, NEGATIVE)
    cross_probs = jax.nn.softmax(cross_scores, axis=2)
    cross_low = cross_probs.astype(LOW)
    cross_mix = (
        jnp.einsum("htk,khd->thd", cross_low, cv_heads, preferred_element_type=WIDE)
        .reshape(tok_rows, model_width)
        .astype(LOW)
    )
    after_cross = after_self + matmul(cross_mix, full_xoutput)
    normed_three = (scaled_norm(after_cross, gain_three) + bias_three).astype(LOW)
    both_three = jnp.concatenate([normed_three, swap(normed_three, "rep", lambda i: i ^ 1)], axis=0)
    quarter = hidden_half // 2
    activ, slope, grad_pre = [], [], []
    for i in range(2):
        pre_act = matmul(both_three, half_up[:, i * quarter : (i + 1) * quarter])
        shaped, steep = gelu_parts(pre_act)
        shaped, steep = lax.optimization_barrier((shaped.astype(LOW), steep))
        activ.append(shaped)
        slope.append(steep)
    for i in range(2):
        grad_pre.append((slope[i] * right_t(upstream, half_down[i])).astype(LOW))
    activ, grad_pre = jnp.concatenate(activ, axis=1), jnp.concatenate(grad_pre, axis=1)
    grad_both = right_t(grad_pre, half_up)
    grad_norm_three = grad_both[:tok_rows] + swap(
        grad_both[tok_rows:].astype(LOW), "rep", lambda i: i ^ 1
    ).astype(WIDE)
    grad_down = left_t(activ, upstream).astype(LOW).reshape(2, -1, model_width)
    grad_up = left_t(both_three, grad_pre).astype(LOW)
    if shard_count == 16:
        down_held, down_got, down_level = plane_middle(grad_down)
        up_held, up_got, up_level = plane_middle(grad_up[None])
    norm_three_part, grad_gain_three, grad_bias_three = norm_back(
        after_cross, gain_three, grad_norm_three
    )
    grad_cross_res = cotangent.astype(WIDE) + norm_three_part
    branch_two = grad_cross_res.astype(LOW)
    grad_xoutput = left_t(cross_mix, branch_two)
    grad_cmix = right_t(branch_two, full_xoutput).astype(LOW)
    grad_cmix = grad_cmix.reshape(tok_rows, head_count, HD)
    grad_cprob = jnp.einsum("thd,khd->htk", grad_cmix, cv_heads, preferred_element_type=WIDE)
    cross_inner = jnp.sum(cross_probs * grad_cprob, axis=2, keepdims=True)
    grad_cscore = (cross_probs * (grad_cprob - cross_inner)).astype(LOW)
    grad_cq = (
        (jnp.einsum("htk,khd->thd", grad_cscore, ck_heads, preferred_element_type=WIDE) * key_scale)
        .reshape(tok_rows, model_width)
        .astype(LOW)
    )
    grad_ck = (
        jnp.einsum("htk,thd->hdk", grad_cscore, cq_heads, preferred_element_type=WIDE) * key_scale
    ).reshape(model_width, 2 * text_rows)
    grad_cv = jnp.einsum(
        "htk,thd->hdk", cross_low, grad_cmix, preferred_element_type=WIDE
    ).reshape(model_width, 2 * text_rows)
    text_pair = jnp.concatenate([grad_ck, grad_cv], axis=1).astype(LOW)
    flat_rows = clip_total * text_rows
    text_cols = 2 * flat_rows
    target = jnp.concatenate([slot_clip, slot_clip + clip_total]) * text_rows
    target = target + jnp.arange(4 * text_rows, dtype=jnp.int32) % text_rows
    spread_text = target[:, None] == jnp.arange(text_cols, dtype=jnp.int32)[None, :]
    text_sums = matmul(text_pair, spread_text.astype(LOW)).astype(LOW)
    grad_xquery = left_t(normed_two, grad_cq)
    grad_norm_two = right_t(grad_cq, full_xquery)
    norm_two_part, grad_gain_two, grad_bias_two = norm_back(after_self, gain_two, grad_norm_two)
    grad_self_res = grad_cross_res + norm_two_part
    branch_one = grad_self_res.astype(LOW)
    grad_output = left_t(attended, branch_one)
    text_share = lax.psum_scatter(text_sums, BOTH, scatter_dimension=0, tiled=True)
    staged = shard_count == 16 and rep_count == 2
    if staged:
        grads, x_core, x_side, x_level, x_rep = positions(
            [grad.astype(LOW) for grad in (grad_xoutput, grad_xquery, grad_output)]
        )
        held = across_cores(grads, x_core)
        middle = held.shape[-1] // 2
        x_both = box_middle([held[..., :middle]], [held[..., middle:]], x_side, x_rep, [])
        x_got = level_sends(x_both, x_level)
    grad_attended = right_t(branch_one, full_output).astype(LOW)
    halves = jnp.transpose(grad_attended.reshape(tok_rows, 2, half_width), (1, 0, 2))
    chip_grad = core_pair(
        pick(halves, core, 0),
        swap(pick(halves, 1 - core, 0), BOTH, lambda i: i ^ 1),
        core,
        0,
    )
    calls = 2 if pairs % 2 == 0 else 1
    backs = ()
    for call in range(calls):
        backs = attend_back(
            offsets,
            queries,
            window,
            chip_mixed,
            logs,
            chip_grad,
            reach,
            call * pairs // calls,
            pairs // calls,
            tuple(backs),
        )
    chip_dq, grad_window = backs
    grad_pair = left_t(normed_around, grad_window)
    grad_wq = left_t(normed_chip, chip_dq)
    grad_pair, grad_wq = grad_pair.astype(LOW), grad_wq.astype(LOW)
    sent_first, sent_last = [], []
    if staged:
        (wide, narrow), q_core, q_side, q_level, q_rep = positions((grad_pair, grad_wq))
        wide, narrow = (part.reshape(8, -1, part.shape[1]) for part in (wide, narrow))
        middle = 3 * half_width // 2
        q_both = box_middle(
            [wide[..., :middle]], [wide[..., middle:], narrow], q_side, q_rep, sent_first
        )
    text_share, grad_window, chip_dq = after((text_share, grad_window, chip_dq), sent_first[:2])
    text_whole = lax.all_gather(text_share, BOTH, axis=0, tiled=True)
    grad_halo = right_t(grad_window[:halo_rows], part_pair)
    halo_sums = [
        jnp.sum(grad_halo * normed_plain[:halo_rows].astype(WIDE), axis=0),
        jnp.sum(grad_halo, axis=0),
    ]
    grad_chip = right_t(chip_dq, part_query) + right_t(grad_window[halo_rows:], part_pair)
    chip_sums = [
        jnp.sum(grad_chip * normed_plain[halo_rows:].astype(WIDE), axis=0),
        jnp.sum(grad_chip, axis=0),
    ]
    around_sums = [halo_sums[i] + chip_sums[i] for i in range(2)]
    grad_halo = grad_halo.astype(LOW)
    units = jnp.concatenate([grad_halo[tok_rows:], grad_chip.astype(LOW)], axis=0)
    units = units.reshape(3, 2, tok_rows, model_width)
    sent = jnp.concatenate([pick(units, 1 - core, 1), grad_halo[None, :tok_rows]], axis=0)
    partner = swap(sent, BOTH, lambda i: i ^ 1)
    sums = add_low(pick(units, core, 1), partner[:3])
    low_sum = add_low(grad_halo[:tok_rows], partner[3])
    if staged:
        down_got = after(down_got, [chip_dq])
        up_got = after(up_got, sent_first[2:])
        own_down = level_total(down_held, down_got, down_level)
        own_up = level_total(up_held, up_got, up_level)
    else:
        own_down = lax.psum_scatter(grad_down, "shard", scatter_dimension=1, tiled=True)
        own_up = lax.psum_scatter(grad_up[None], "shard", scatter_dimension=1, tiled=True)
    activ_late, after_late = after((activ, after_cross), sent_first[2:] if staged else [grad_chip])
    mixed_both = matmul(activ_late[:, :quarter], half_down[0]) + matmul(
        activ_late[:, quarter:], half_down[1]
    )
    y_got = swap(mixed_both[tok_rows:].astype(LOW), "rep", lambda i: i ^ 1)
    if staged:
        q_both = after(q_both, [sums, low_sum])
        q_got = level_sends(q_both, q_level, sent_last)
    text_whole = after(text_whole, sent_last)
    key_round, value_round = (
        text_whole[:, :flat_rows],
        text_whole[:, flat_rows : 2 * flat_rows],
    )
    col_start = lax.axis_index("shard") * shard_rows
    text_flat = text_states.reshape(flat_rows, model_width)
    text_slice = lax.dynamic_slice_in_dim(text_flat, col_start, shard_rows, 1)

    def mixed_dims(left, right):
        return lax.dot_general(
            left, right, (((0,), (1,)), ((), ())), preferred_element_type=WIDE
        )

    grad_xkey = mixed_dims(text_slice, key_round)
    grad_xvalue = mixed_dims(text_slice, value_round)
    grad_text = mixed_dims(key_round, full_xkey) + mixed_dims(value_round, full_xvalue)
    grad_text = grad_text.reshape(clip_total, text_rows, model_width)
    filler = sent_last + [grad_text, grad_xkey, grad_xvalue] if staged else []
    if staged:
        q_own = level_total(q_both, q_got, q_level)
        parts = rep_rows(q_own).reshape(2, shard_rows, 3 * half_width)
        q_swapped = swap(pick(parts, 1 - q_core, 0), "shard", lambda i: i ^ 1)
        fin_query, fin_key, fin_value = unpack(pick(parts, q_core, 0), q_swapped)
        x_own = level_total(x_both, after(x_got, sent_first[2:] + [own_down, own_up, mixed_both]), x_level)
        fin_x = rep_rows(x_own, filler)
    else:
        filled = joined([grad_pair, grad_wq])
        fin_halves = plain_rows([core_pair(filled, jnp.zeros_like(filled), core, 1)])
        fin_x = plain_rows([grad.astype(LOW) for grad in (grad_xoutput, grad_xquery, grad_output)])
        fin_halves = fin_halves.astype(WIDE).reshape(shard_rows, 2, 3 * half_width)
        fin_pair = fin_halves[:, :, :model_width].reshape(shard_rows, 2, pairs, 2, 2 * HD)
        fin_query = fin_halves[:, :, model_width:].reshape(w_query.shape)
        fin_key = fin_pair[:, :, :, 0].reshape(w_query.shape)
        fin_value = fin_pair[:, :, :, 1].reshape(w_query.shape)
    fin_xoutput, fin_xquery, fin_output = (
        fin_x[:, i * model_width : (i + 1) * model_width].astype(WIDE) for i in range(3)
    )
    down_halves = rep_pair(own_down, filler)
    fin_down = jnp.concatenate(down_halves, axis=0).reshape(w_down.shape).astype(WIDE)
    other_up = swap(own_up, "rep", lambda i: i ^ 1)
    own_up, other_up = after((own_up, other_up), filler)
    fin_up = interleave(own_up[0], other_up[0], shard_count, chunk)
    y_own, y_got, after_late = after((mixed_both[:tok_rows], y_got, after_late), sent_last)
    block_out = (after_late + y_own + y_got.astype(WIDE)).astype(LOW)
    back = swap(sums[1], BOTH, lambda i: i ^ 2).astype(WIDE)
    back_half = swap(low_sum, BOTH, lambda i: i ^ 2 if i % 2 == 1 else -1)
    to_below = (
        sums[0].astype(WIDE) + jnp.where(side == 0, back_half.astype(WIDE), back)
    ).astype(LOW)
    down_part = swap(to_below, BOTH, lambda i: i - 4)
    far_part = swap(back_half, BOTH, lambda i: i - 8 if i % 4 == 3 else -1)
    if staged:
        down_part, far_part = after((down_part, far_part), [q_own])
    grad_norm_one = (
        sums[2].astype(WIDE)
        + jnp.where(side == 0, back, 0.0)
        + down_part.astype(WIDE)
        + far_part.astype(WIDE)
    )
    norm_one_part, _, _ = norm_back(resid, gain_one, grad_norm_one)
    grad_gain_one, grad_bias_one = around_sums
    grad_hidden = (grad_self_res + norm_one_part).astype(LOW)
    vectors = lax.all_gather(
        jnp.stack(
            [
                grad_gain_one,
                grad_bias_one,
                grad_gain_two,
                grad_bias_two,
                grad_gain_three,
                grad_bias_three,
            ]
        ),
        BOTH,
    )
    _, vectors = lax.optimization_barrier((to_below, vectors))
    vectors = jnp.sum(vectors, axis=0)
    fin_gain_one, fin_bias_one, fin_gain_two, fin_bias_two, fin_gain_three, fin_bias_three = (
        lax.dynamic_slice_in_dim(vectors, col_start, shard_rows, 1)
    )
    return (
        block_out,
        grad_hidden,
        grad_text,
        fin_gain_one,
        fin_bias_one,
        fin_query,
        fin_key,
        fin_value,
        fin_output,
        fin_gain_two,
        fin_bias_two,
        fin_xquery,
        grad_xkey,
        grad_xvalue,
        fin_xoutput,
        fin_gain_three,
        fin_bias_three,
        fin_up,
        fin_down,
    )


def solution(mesh):
    rows, vector, tokens = P("shard", None), P("shard"), P(BOTH, None)
    placed = (
        (tokens, P(), P(BOTH), P(BOTH))
        + (vector, vector, rows, rows, rows, rows)
        + (vector, vector, rows, rows, rows, rows)
        + (vector, vector, rows, rows, tokens)
    )
    return jax.shard_map(
        on_device,
        mesh=mesh,
        in_specs=placed,
        out_specs=(
            (tokens, tokens, P())
            + (vector, vector, rows, rows, rows, rows)
            + (vector, vector, rows, rows, rows, rows)
            + (vector, vector, rows, rows)
        ),
        check_vma=False,
    )
```

```python
import functools

import jax
import jax.numpy as jnp
from jax import lax
from jax.experimental import pallas as pl
from jax.experimental.pallas import tpu as pltpu
from jax.sharding import PartitionSpec as P


HD = 64
CLIP_MAX = 1280
EPSILON = 1e-05
NEGATIVE = -1e30
BLOCK = 256
BOTH = ("rep", "shard")
LOW = jnp.bfloat16
WIDE = jnp.float32


def normalize(values):
    centre = values - jnp.mean(values, axis=-1, keepdims=True)
    spread = jnp.mean(centre * centre, axis=-1, keepdims=True)
    return centre * lax.rsqrt(spread + EPSILON)


def scaled_norm(values, scale_vec):
    return normalize(values) * scale_vec


def gelu_parts(values):
    below = 0.5 + 0.5 * lax.erf(values * (0.5**0.5))
    density = jnp.exp(-0.5 * values * values) * ((2.0 * jnp.pi) ** -0.5)
    return values * below, below + values * density


def matmul(left, right):
    return jnp.dot(left, right, preferred_element_type=WIDE)


def left_t(left, right):
    return lax.dot_general(left, right, (((0,), (0,)), ((), ())), preferred_element_type=WIDE)


def right_t(left, right):
    return lax.dot_general(left, right, (((1,), (1,)), ((), ())), preferred_element_type=WIDE)


def norm_back(values, scale_vec, upstream):
    _, pull = jax.vjp(scaled_norm, values, scale_vec.astype(WIDE))
    grad_values, grad_scale = pull(upstream)
    return (grad_values, grad_scale, jnp.sum(upstream, axis=0))


def pick(array, index, axis):
    return lax.dynamic_index_in_dim(array, index, axis, False)


def axis_length(axis):
    return lax.axis_size(axis)


def swap(array, axis, pairing, log=None):
    length = axis_length(axis)
    pairs = [(i, pairing(i)) for i in range(length)]
    if log is not None:
        log.append(array)
    return lax.ppermute(array, axis, [(i, j) for i, j in pairs if 0 <= j < length])


def after(values, earlier):
    return lax.optimization_barrier((values, list(earlier)))[0]


def add_low(left, right):
    return (left.astype(WIDE) + right.astype(WIDE)).astype(LOW)


def gather_rows(array):
    return lax.all_gather(array, "shard", axis=0, tiled=True)


def joined(parts):
    return parts[0] if len(parts) == 1 else jnp.concatenate(parts, axis=-1)


def positions(grads):
    index, rep = lax.axis_index("shard"), lax.axis_index("rep")
    grads, index, rep = lax.optimization_barrier((grads, index, rep))
    return grads, index % 2, (index // 2) % 2, index // 4, rep


def away_kernel(_, *refs):
    out_ref, start = refs[-1], 0
    for ref in refs[:-1]:
        out_ref[0, :, start : start + ref.shape[1]] = ref[...]
        start += ref.shape[1]


def away_rows(grads, core):
    rows = grads[0].shape[0] // 16
    width = sum(grad.shape[1] for grad in grads)
    return pl.pallas_call(
        away_kernel,
        grid_spec=pltpu.PrefetchScalarGridSpec(
            num_scalar_prefetch=1,
            grid=(8,),
            in_specs=[
                pl.BlockSpec((rows, grad.shape[1]), lambda i, c: (2 * i + 1 - c[0], 0))
                for grad in grads
            ],
            out_specs=pl.BlockSpec((1, rows, width), lambda i, c: (i, 0, 0)),
        ),
        out_shape=jax.ShapeDtypeStruct((8, rows, width), LOW),
        cost_estimate=pl.CostEstimate(
            flops=0, transcendentals=0, bytes_accessed=32 * rows * width
        ),
    )(core[None], *grads)


def first_sends_kernel(_, wide_ref, *refs):
    pieces, side_ref, rep_ref = refs[:-2], refs[-2], refs[-1]
    half = side_ref.shape[-1]
    side_ref[0] = wide_ref[:, :half]
    rest = wide_ref.shape[1] - half
    for side in range(2):
        rep_ref[0, side, :, :rest] = pieces[side][:, half:]
        rep_ref[0, side, :, rest:] = pieces[2 + side][...]


def first_sends(wide, narrow, side, rep):
    rows = wide.shape[0] // 8
    half = (wide.shape[1] + narrow.shape[1]) // 2

    def part(array, which):
        return pl.BlockSpec(
            (rows // 2, array.shape[1]), lambda z, p: (4 * z + 2 * which + 1 - p[1], 0)
        )

    return pl.pallas_call(
        first_sends_kernel,
        grid_spec=pltpu.PrefetchScalarGridSpec(
            num_scalar_prefetch=1,
            grid=(4,),
            in_specs=[
                pl.BlockSpec((rows, wide.shape[1]), lambda z, p: (2 * z + 1 - p[0], 0)),
                part(wide, 0),
                part(wide, 1),
                part(narrow, 0),
                part(narrow, 1),
            ],
            out_specs=[
                pl.BlockSpec((1, rows, half), lambda z, p: (z, 0, 0)),
                pl.BlockSpec((1, 2, rows // 2, half), lambda z, p: (z, 0, 0, 0)),
            ],
        ),
        out_shape=[
            jax.ShapeDtypeStruct((4, rows, half), LOW),
            jax.ShapeDtypeStruct((4, 2, rows // 2, half), LOW),
        ],
        cost_estimate=pl.CostEstimate(
            flops=0, transcendentals=0, bytes_accessed=32 * rows * half
        ),
    )(jnp.stack([side, rep]), wide, wide, wide, narrow, narrow)


def across_cores(grads, core):
    rows = grads[0].shape[0] // 16
    parts = [grad.reshape(8, 2, rows, grad.shape[1]) for grad in grads]
    away = away_rows(grads, core)
    held = joined([pick(part, core, 1) for part in parts])
    return add_low(held, swap(away, "shard", lambda i: i ^ 1))


def level_sends(both, level, log=None):
    axis = both.ndim - 3
    return [
        swap(pick(both, (level + step) % 4, axis), "shard", lambda i: (i + 4 * step) % 16, log)
        for step in range(1, 4)
    ]


def level_total(both, got, level):
    total = pick(both, level, both.ndim - 3).astype(WIDE)
    for part in got:
        total = total + part.astype(WIDE)
    return total.astype(LOW)


def box_middle(firsts, seconds, side, rep, log, sends=None):
    rows = firsts[0].shape[-2]
    firsts = [part.reshape(4, 2, *part.shape[-2:]) for part in firsts]
    seconds = [part.reshape(4, 2, 2, rows // 2, part.shape[-1]) for part in seconds]
    if sends is None:
        sends = (
            joined([pick(part, 1 - side, 1) for part in firsts]),
            joined([pick(part, 1 - rep, 2) for part in seconds]),
        )
    second = add_low(
        joined([pick(part, rep, 2) for part in seconds]),
        swap(sends[1], "rep", lambda i: i ^ 1, log),
    )
    first = add_low(
        joined([pick(part, side, 1) for part in firsts]),
        swap(sends[0], "shard", lambda i: i ^ 2, log),
    )
    first = first.reshape(4, 2, rows // 2, first.shape[-1])
    first = add_low(
        pick(first, rep, 1),
        swap(pick(first, 1 - rep, 1), "rep", lambda i: i ^ 1, log),
    )
    second = add_low(
        pick(second, side, 1),
        swap(pick(second, 1 - side, 1), "shard", lambda i: i ^ 2, log),
    )
    return jnp.concatenate([first, second], axis=2)


def plane_middle(grad):
    grad, core, side, level, _ = positions(grad)
    count, rows, width = grad.shape[0], grad.shape[1] // 16, grad.shape[2]
    parts = grad.reshape(count, 8, 2, rows, width)
    away = pick(parts, 1 - core, 2)
    held = add_low(
        pick(parts, core, 2), swap(away, "shard", lambda i: i ^ 1)
    ).reshape(count, 4, 2, rows, width)
    held = add_low(
        pick(held, side, 2),
        swap(pick(held, 1 - side, 2), "shard", lambda i: i ^ 2),
    )
    return held, level_sends(held, level), level


def rep_pair(own, earlier=()):
    other = swap(own, "rep", lambda i: i ^ 1)
    if earlier:
        own, other = after((own, other), earlier)
    rep = lax.axis_index("rep")
    return jnp.where(rep == 0, own, other), jnp.where(rep == 0, other, own)


def rep_rows(own, earlier=()):
    low, high = rep_pair(own, earlier)
    return jnp.concatenate([low, high], axis=0)


def plain_rows(grads):
    share = lax.psum_scatter(joined(grads), "shard", scatter_dimension=0, tiled=True)
    return lax.psum(share.astype(WIDE), "rep").astype(LOW)


def head_lanes(which):
    lane = lax.broadcasted_iota(jnp.int32, (BLOCK, 2 * HD), 1)
    return lane < HD if which == 0 else lane >= HD


def open_pairs(offsets, step, reach):
    base = (reach - step) * BLOCK
    keys = lax.broadcasted_iota(jnp.int32, (BLOCK, BLOCK), 0)
    column = lax.broadcasted_iota(jnp.int32, (1, BLOCK), 1)
    allowed = keys >= (column - offsets) + base
    if base == 0:
        allowed = allowed & (keys <= lax.broadcasted_iota(jnp.int32, (BLOCK, BLOCK), 1))
    return allowed


def attend_kernel(reach, offset_ref, query_ref, window_ref, out_ref, log_ref, held):
    start = pl.program_id(1) * BLOCK
    offsets = offset_ref[...]
    scaled = query_ref[...] * jnp.asarray(HD**-0.5, LOW)
    mixed = []
    for head in range(2):
        query = jnp.where(head_lanes(head), scaled, jnp.zeros_like(scaled))
        peak = jnp.full((1, BLOCK), NEGATIVE, WIDE)
        for step in range(reach + 1):
            rows = pl.ds(pl.multiple_of(start + step * BLOCK, BLOCK), BLOCK)
            scores = right_t(window_ref[rows, : 2 * HD], query)
            scores = jnp.where(open_pairs(offsets, step, reach), scores, NEGATIVE)
            held[head, step] = scores
            peak = jnp.maximum(peak, jnp.max(scores, axis=0, keepdims=True))
        total = jnp.zeros((1, BLOCK), WIDE)
        blend = jnp.zeros((2 * HD, BLOCK), WIDE)
        for step in range(reach + 1):
            rows = pl.ds(pl.multiple_of(start + step * BLOCK, BLOCK), BLOCK)
            expo = jnp.exp(held[head, step] - peak)
            total = total + jnp.sum(expo, axis=0, keepdims=True)
            blend = blend + left_t(window_ref[rows, 2 * HD :], expo.astype(LOW))
        mixed.append((blend / total)[head * HD : (head + 1) * HD])
        log_ref[0, pl.ds(head, 1), :] = peak + jnp.log(total)
    out_ref[...] = jnp.concatenate(mixed, axis=0).T.astype(LOW)


def attend(offsets, queries, window, reach):
    rows, width = queries.shape
    pairs, blocks, context = width // (2 * HD), rows // BLOCK, window.shape[0]
    work = pairs * 2 * rows * (reach + 1) * BLOCK
    return pl.pallas_call(
        functools.partial(attend_kernel, reach),
        grid=(pairs, blocks),
        in_specs=[
            pl.BlockSpec((1, BLOCK), lambda p, b: (0, b)),
            pl.BlockSpec((BLOCK, 2 * HD), lambda p, b: (b, p)),
            pl.BlockSpec((context, 4 * HD), lambda p, b: (0, p)),
        ],
        out_specs=[
            pl.BlockSpec((BLOCK, 2 * HD), lambda p, b: (b, p)),
            pl.BlockSpec((1, 2, BLOCK), lambda p, b: (p, 0, b)),
        ],
        out_shape=[
            jax.ShapeDtypeStruct((rows, width), LOW),
            jax.ShapeDtypeStruct((pairs, 2, rows), WIDE),
        ],
        scratch_shapes=[pltpu.VMEM((2, reach + 1, BLOCK, BLOCK), WIDE)],
        cost_estimate=pl.CostEstimate(
            flops=16 * HD * work, transcendentals=work, bytes_accessed=8 * rows * width
        ),
        name="attend_forward",
    )(offsets, queries, window)


def attend_back_kernel(
    reach,
    offset_ref,
    query_ref,
    window_ref,
    out_ref,
    log_ref,
    grad_ref,
    *rest,
):
    grad_query_ref, grad_window_ref, grad_keys, grad_values = rest[-4:]
    block = pl.program_id(1)
    start = block * BLOCK

    @pl.when(block == 0)
    def _():
        grad_keys[...] = jnp.zeros_like(grad_keys)
        grad_values[...] = jnp.zeros_like(grad_values)

    offsets = offset_ref[...]
    scaled = query_ref[...] * jnp.asarray(HD**-0.5, LOW)
    grads = grad_ref[...]
    inner = (grads.astype(WIDE) * out_ref[...].astype(WIDE)).T
    query, grad, inners, logs = [], [], [], []
    for head in range(2):
        lanes = head_lanes(head)
        query.append(jnp.where(lanes, scaled, jnp.zeros_like(scaled)))
        grad.append(jnp.where(lanes, grads, jnp.zeros_like(grads)))
        inners.append(jnp.sum(inner[head * HD : (head + 1) * HD], axis=0, keepdims=True))
        logs.append(log_ref[0, pl.ds(head, 1), :])
    back = [jnp.zeros((2 * HD, BLOCK), WIDE) for _ in range(2)]
    for step in range(reach + 1):
        rows = pl.ds(pl.multiple_of(start + step * BLOCK, BLOCK), BLOCK)
        key, value = window_ref[rows, : 2 * HD], window_ref[rows, 2 * HD :]
        allowed = open_pairs(offsets, step, reach)
        to_key = jnp.zeros((BLOCK, 2 * HD), WIDE)
        to_value = jnp.zeros((BLOCK, 2 * HD), WIDE)
        for head in range(2):
            scores = jnp.where(allowed, right_t(key, query[head]), NEGATIVE)
            probs = jnp.exp(scores - logs[head])
            to_value = to_value + matmul(probs.astype(LOW), grad[head])
            grad_probs = right_t(value, grad[head])
            grad_scores = (probs * (grad_probs - inners[head])).astype(LOW)
            to_key = to_key + matmul(grad_scores, query[head])
            back[head] = back[head] + left_t(key, grad_scores)
        grad_keys[rows, :] += to_key
        grad_values[rows, :] += to_value
    back = jnp.concatenate([back[0][:HD], back[1][HD:]], axis=0) * (HD**-0.5)
    grad_query_ref[...] = back.T.astype(LOW)

    @pl.when(block == pl.num_programs(1) - 1)
    def _():
        grad_window_ref[:, : 2 * HD] = grad_keys[...].astype(LOW)
        grad_window_ref[:, 2 * HD :] = grad_values[...].astype(LOW)


def attend_back(offsets, queries, window, out, logs, grads, reach, begin, pairs, filled):
    rows, width = queries.shape
    blocks, context = rows // BLOCK, window.shape[0]
    work = pairs * 2 * rows * (reach + 1) * BLOCK
    row_block = pl.BlockSpec((BLOCK, 2 * HD), lambda p, b: (b, p + begin))
    window_block = pl.BlockSpec((context, 4 * HD), lambda p, b: (0, p + begin))
    return pl.pallas_call(
        functools.partial(attend_back_kernel, reach),
        grid=(pairs, blocks),
        in_specs=[
            pl.BlockSpec((1, BLOCK), lambda p, b: (0, b)),
            row_block,
            window_block,
            row_block,
            pl.BlockSpec((1, 2, BLOCK), lambda p, b: (p + begin, 0, b)),
            row_block,
        ]
        + [pl.BlockSpec(memory_space=pl.ANY)] * len(filled),
        out_specs=[row_block, window_block],
        out_shape=[
            jax.ShapeDtypeStruct((rows, width), LOW),
            jax.ShapeDtypeStruct(window.shape, LOW),
        ],
        input_output_aliases={6 + i: i for i in range(len(filled))},
        scratch_shapes=[
            pltpu.VMEM((context, 2 * HD), WIDE),
            pltpu.VMEM((context, 2 * HD), WIDE),
        ],
        cost_estimate=pl.CostEstimate(
            flops=40 * HD * work, transcendentals=work, bytes_accessed=16 * rows * width
        ),
        name="attend_backward",
    )(offsets, queries, window, out, logs, grads, *filled)


def unpack_kernel(width, own_ref, got_ref, *outs):
    core = lax.axis_index("shard") % 2
    for half in range(2):
        base = half * width // 2
        whole = jnp.where(core == half, own_ref[...], got_ref[...]).astype(WIDE)
        for pair in range(width // (4 * HD)):
            lanes = slice(base + pair * 2 * HD, base + (pair + 1) * 2 * HD)
            for kind in range(2):
                start = (2 * pair + kind) * 2 * HD
                outs[1 + kind][:, lanes] = whole[:, start : start + 2 * HD]
        outs[0][:, base : base + width // 2] = whole[:, width:]


def unpack(own, got):
    rows, width = own.shape[0], own.shape[1] * 2 // 3
    return pl.pallas_call(
        functools.partial(unpack_kernel, width),
        out_shape=[jax.ShapeDtypeStruct((rows, width), WIDE)] * 3,
        cost_estimate=pl.CostEstimate(
            flops=0, transcendentals=0, bytes_accessed=18 * rows * width
        ),
        name="unpack_query_key_value",
    )(own, got)


def interleave_kernel(count, chunk, own_ref, other_ref, out_ref):
    rep = lax.axis_index("rep")
    own, other = own_ref[...].astype(WIDE), other_ref[...].astype(WIDE)
    halves = jnp.where(rep == 0, own, other), jnp.where(rep == 0, other, own)
    for index in range(count):
        parts = [
            half[:, (j * count + index) * chunk : (j * count + index + 1) * chunk]
            for half in halves
            for j in range(2)
        ]
        out_ref[:, 4 * chunk * index : 4 * chunk * (index + 1)] = jnp.concatenate(parts, axis=1)


def interleave(own, other, count, chunk):
    rows, width = own.shape
    return pl.pallas_call(
        functools.partial(interleave_kernel, count, chunk),
        out_shape=jax.ShapeDtypeStruct((rows, 2 * width), WIDE),
        cost_estimate=pl.CostEstimate(
            flops=0, transcendentals=0, bytes_accessed=12 * rows * width
        ),
        name="interleave_up",
    )(own, other)


def core_pair(own, got, core, axis):
    return jnp.where(
        core == 0,
        jnp.concatenate([own, got], axis=axis),
        jnp.concatenate([got, own], axis=axis),
    )


def on_device(
    hidden,
    text_states,
    clip_index,
    frame_offset,
    self_gain,
    self_bias,
    w_query,
    w_key,
    w_value,
    w_output,
    cross_gain,
    cross_bias,
    x_query,
    x_key,
    x_value,
    x_output,
    final_gain,
    final_bias,
    w_up,
    w_down,
    cotangent,
):
    tok_rows, model_width = hidden.shape
    head_count = model_width // HD
    half_width = model_width // 2
    reach = (CLIP_MAX - 2) // tok_rows + 1
    key_scale = HD ** (-0.5)
    clip_total = text_states.shape[0]
    text_rows = text_states.shape[1]
    shard_count, rep_count = axis_length("shard"), axis_length("rep")
    shard_rows = x_key.shape[0]
    place = lax.axis_index("rep") * shard_count + lax.axis_index("shard")
    core, side = place % 2, (place // 2) % 2

    params = jnp.stack(
        [self_gain, self_bias, cross_gain, cross_bias, final_gain, final_bias], axis=1
    )
    params = jnp.pad(params, ((0, 0), (0, 128 - params.shape[1])))
    pairs = head_count // 4
    pair_split = (shard_rows, 2, pairs, 1, 2 * HD)
    key_value = jnp.concatenate([w_key.reshape(pair_split), w_value.reshape(pair_split)], axis=3)
    key_value = key_value.reshape(shard_rows, 2, model_width)
    first_group = gather_rows(
        jnp.concatenate(
            [
                part
                for h in range(2)
                for part in (w_query[:, h * half_width : (h + 1) * half_width], key_value[:, h])
            ]
            + [w_output, params],
            axis=1,
        ),
    )
    full_output = first_group[:, 3 * model_width : 4 * model_width]
    gain_one, bias_one, gain_two, bias_two, gain_three, bias_three = (
        first_group[:, 4 * model_width + i].astype(WIDE) for i in range(6)
    )
    part_all = lax.dynamic_slice_in_dim(
        first_group, core * (3 * half_width), 3 * half_width, 1
    )
    part_query, part_pair = part_all[:, :half_width], part_all[:, half_width:]
    second_group = gather_rows(jnp.concatenate([x_query, x_key, x_value, x_output], axis=1))
    full_xquery, full_xkey, full_xvalue, full_xoutput = (
        second_group[:, i * model_width : (i + 1) * model_width] for i in range(4)
    )
    rep_index = lax.axis_index("rep")
    down_rows = w_down.shape[0]
    chunk = down_rows // 4
    some_up = pick(w_up.reshape(w_up.shape[0], shard_count, 2, 2, chunk), rep_index, 2)
    some_up = jnp.transpose(some_up, (0, 2, 1, 3)).reshape(w_up.shape[0], -1)
    some_down = pick(w_down.reshape(2, 2, chunk, model_width), rep_index, 0)
    hidden_half = some_up.shape[1]
    third_group = gather_rows(jnp.concatenate([some_up, some_down[0], some_down[1]], axis=1))
    half_up = third_group[:, :hidden_half]
    half_down = [
        third_group[:, hidden_half + i * model_width : hidden_half + (i + 1) * model_width]
        for i in range(2)
    ]
    upstream = jnp.concatenate([cotangent, swap(cotangent, "rep", lambda i: i ^ 1)], axis=0)

    offsets = core_pair(frame_offset, swap(frame_offset, BOTH, lambda i: i ^ 1), core, 0)[None, :]
    resid = hidden.astype(WIDE)
    below = swap(hidden, BOTH, lambda i: i + 4)
    far = swap(hidden, BOTH, lambda i: i + 8 if i % 4 == 3 else -1)
    across = swap(jnp.where(side == 0, hidden, below), BOTH, lambda i: i ^ 2)
    third = swap(jnp.where(side == 0, below, far), BOTH, lambda i: i ^ 2 if i % 2 == 1 else -1)
    shards = jnp.stack([below, across, hidden, third])
    partner = swap(shards, BOTH, lambda i: i ^ 1)
    paired = core_pair(shards[:3], partner[:3], core, 1)
    around = jnp.concatenate(
        [jnp.where(core == 1, third, partner[3]), paired[0], paired[1], paired[2]], axis=0
    )
    chip_rows = 2 * tok_rows
    halo_rows = tok_rows + 2 * chip_rows
    normed_plain = normalize(around.astype(WIDE))
    normed_around = (normed_plain * gain_one + bias_one).astype(LOW)
    normed_plain = normed_plain.astype(LOW)
    normed_chip = normed_around[halo_rows:]
    window = matmul(normed_around, part_pair).astype(LOW)
    queries = matmul(normed_chip, part_query).astype(LOW)
    chip_mixed, logs = attend(offsets, queries, window, reach)

    def to_tokens(chip_rows_array):
        mine = lax.dynamic_slice_in_dim(chip_rows_array, core * tok_rows, tok_rows, 0)
        away = lax.dynamic_slice_in_dim(chip_rows_array, (1 - core) * tok_rows, tok_rows, 0)
        return core_pair(mine, swap(away, BOTH, lambda i: i ^ 1), core, 1)

    attended = to_tokens(chip_mixed)
    after_self = resid + matmul(attended, full_output)
    normed_two = (scaled_norm(after_self, gain_two) + bias_two).astype(LOW)
    cross_q = matmul(normed_two, full_xquery).astype(LOW)
    first = clip_index[0]
    second = jnp.minimum(first + 1, clip_total - 1)
    chosen = jnp.concatenate(
        [
            lax.dynamic_index_in_dim(text_states, first, 0, False),
            lax.dynamic_index_in_dim(text_states, second, 0, False),
        ],
        axis=0,
    )
    cross_k = matmul(chosen, full_xkey).astype(LOW)
    cross_v = matmul(chosen, full_xvalue).astype(LOW)
    slot = jnp.arange(2 * text_rows, dtype=jnp.int32) // text_rows
    slot_clip = jnp.where(slot == 0, first, second)
    open_slot = (slot == 0) | (second != first)
    cross_mask = (clip_index[:, None] == slot_clip[None, :]) & open_slot[None, :]
    cq_heads = cross_q.reshape(tok_rows, head_count, HD)
    ck_heads = cross_k.reshape(2 * text_rows, head_count, HD)
    cv_heads = cross_v.reshape(2 * text_rows, head_count, HD)
    cross_scores = (
        jnp.einsum("thd,khd->htk", cq_heads, ck_heads, preferred_element_type=WIDE) * key_scale
    )
    cross_scores = jnp.where(cross_mask[None], cross_scores, NEGATIVE)
    cross_probs = jax.nn.softmax(cross_scores, axis=2)
    cross_low = cross_probs.astype(LOW)
    cross_mix = (
        jnp.einsum("htk,khd->thd", cross_low, cv_heads, preferred_element_type=WIDE)
        .reshape(tok_rows, model_width)
        .astype(LOW)
    )
    after_cross = after_self + matmul(cross_mix, full_xoutput)
    normed_three = (scaled_norm(after_cross, gain_three) + bias_three).astype(LOW)
    both_three = jnp.concatenate([normed_three, swap(normed_three, "rep", lambda i: i ^ 1)], axis=0)
    quarter = hidden_half // 2
    activ, slope, grad_pre = [], [], []
    for i in range(2):
        pre_act = matmul(both_three, half_up[:, i * quarter : (i + 1) * quarter])
        shaped, steep = gelu_parts(pre_act)
        shaped, steep = lax.optimization_barrier((shaped.astype(LOW), steep))
        activ.append(shaped)
        slope.append(steep)
    for i in range(2):
        grad_pre.append((slope[i] * right_t(upstream, half_down[i])).astype(LOW))
    activ, grad_pre = jnp.concatenate(activ, axis=1), jnp.concatenate(grad_pre, axis=1)
    grad_both = right_t(grad_pre, half_up)
    grad_norm_three = grad_both[:tok_rows] + swap(
        grad_both[tok_rows:].astype(LOW), "rep", lambda i: i ^ 1
    ).astype(WIDE)
    grad_down = left_t(activ, upstream).astype(LOW).reshape(2, -1, model_width)
    grad_up = left_t(both_three, grad_pre).astype(LOW)
    if shard_count == 16:
        down_held, down_got, down_level = plane_middle(grad_down)
        up_held, up_got, up_level = plane_middle(grad_up[None])
    norm_three_part, grad_gain_three, grad_bias_three = norm_back(
        after_cross, gain_three, grad_norm_three
    )
    grad_cross_res = cotangent.astype(WIDE) + norm_three_part
    branch_two = grad_cross_res.astype(LOW)
    grad_xoutput = left_t(cross_mix, branch_two)
    grad_cmix = right_t(branch_two, full_xoutput).astype(LOW)
    grad_cmix = grad_cmix.reshape(tok_rows, head_count, HD)
    grad_cprob = jnp.einsum("thd,khd->htk", grad_cmix, cv_heads, preferred_element_type=WIDE)
    cross_inner = jnp.sum(cross_probs * grad_cprob, axis=2, keepdims=True)
    grad_cscore = (cross_probs * (grad_cprob - cross_inner)).astype(LOW)
    grad_cq = (
        (jnp.einsum("htk,khd->thd", grad_cscore, ck_heads, preferred_element_type=WIDE) * key_scale)
        .reshape(tok_rows, model_width)
        .astype(LOW)
    )
    grad_ck = (
        jnp.einsum("htk,thd->hdk", grad_cscore, cq_heads, preferred_element_type=WIDE) * key_scale
    ).reshape(model_width, 2 * text_rows)
    grad_cv = jnp.einsum(
        "htk,thd->hdk", cross_low, grad_cmix, preferred_element_type=WIDE
    ).reshape(model_width, 2 * text_rows)
    text_pair = jnp.concatenate([grad_ck, grad_cv], axis=1).astype(LOW)
    flat_rows = clip_total * text_rows
    text_cols = 2 * flat_rows
    target = jnp.concatenate([slot_clip, slot_clip + clip_total]) * text_rows
    target = target + jnp.arange(4 * text_rows, dtype=jnp.int32) % text_rows
    spread_text = target[:, None] == jnp.arange(text_cols, dtype=jnp.int32)[None, :]
    text_sums = matmul(text_pair, spread_text.astype(LOW)).astype(LOW)
    grad_xquery = left_t(normed_two, grad_cq)
    grad_norm_two = right_t(grad_cq, full_xquery)
    norm_two_part, grad_gain_two, grad_bias_two = norm_back(after_self, gain_two, grad_norm_two)
    grad_self_res = grad_cross_res + norm_two_part
    branch_one = grad_self_res.astype(LOW)
    grad_output = left_t(attended, branch_one)
    text_share = lax.psum_scatter(text_sums, BOTH, scatter_dimension=0, tiled=True)
    staged = shard_count == 16 and rep_count == 2
    if staged:
        grads, x_core, x_side, x_level, x_rep = positions(
            [grad.astype(LOW) for grad in (grad_xoutput, grad_xquery, grad_output)]
        )
        held = across_cores(grads, x_core)
        middle = held.shape[-1] // 4
        x_both = box_middle([held[..., :middle]], [held[..., middle:]], x_side, x_rep, [])
        x_got = level_sends(x_both, x_level)
    grad_attended = right_t(branch_one, full_output).astype(LOW)
    halves = jnp.transpose(grad_attended.reshape(tok_rows, 2, half_width), (1, 0, 2))
    chip_grad = core_pair(
        pick(halves, core, 0),
        swap(pick(halves, 1 - core, 0), BOTH, lambda i: i ^ 1),
        core,
        0,
    )
    calls = 2 if pairs % 2 == 0 else 1
    backs = ()
    for call in range(calls):
        backs = attend_back(
            offsets,
            queries,
            window,
            chip_mixed,
            logs,
            chip_grad,
            reach,
            call * pairs // calls,
            pairs // calls,
            tuple(backs),
        )
    chip_dq, grad_window = backs
    grad_pair = left_t(normed_around, grad_window)
    grad_wq = left_t(normed_chip, chip_dq)
    grad_pair, grad_wq = grad_pair.astype(LOW), grad_wq.astype(LOW)
    sent_first, sent_last = [], []
    if staged:
        (wide, narrow), q_core, q_side, q_level, q_rep = positions((grad_pair, grad_wq))
        q_sends = first_sends(wide, narrow, q_side, q_rep)
        wide, narrow = (part.reshape(8, -1, part.shape[1]) for part in (wide, narrow))
        middle = 3 * half_width // 2
        q_both = box_middle(
            [wide[..., :middle]], [wide[..., middle:], narrow], q_side, q_rep, sent_first, q_sends
        )
    text_share, grad_window, chip_dq = after((text_share, grad_window, chip_dq), sent_first[:2])
    text_whole = lax.all_gather(text_share, BOTH, axis=0, tiled=True)
    grad_halo = right_t(grad_window[:halo_rows], part_pair)
    halo_sums = [
        jnp.sum(grad_halo * normed_plain[:halo_rows].astype(WIDE), axis=0),
        jnp.sum(grad_halo, axis=0),
    ]
    grad_chip = right_t(chip_dq, part_query) + right_t(grad_window[halo_rows:], part_pair)
    chip_sums = [
        jnp.sum(grad_chip * normed_plain[halo_rows:].astype(WIDE), axis=0),
        jnp.sum(grad_chip, axis=0),
    ]
    around_sums = [halo_sums[i] + chip_sums[i] for i in range(2)]
    grad_halo = grad_halo.astype(LOW)
    units = jnp.concatenate([grad_halo[tok_rows:], grad_chip.astype(LOW)], axis=0)
    units = units.reshape(3, 2, tok_rows, model_width)
    sent = jnp.concatenate([pick(units, 1 - core, 1), grad_halo[None, :tok_rows]], axis=0)
    partner = swap(sent, BOTH, lambda i: i ^ 1)
    sums = add_low(pick(units, core, 1), partner[:3])
    low_sum = add_low(grad_halo[:tok_rows], partner[3])
    if staged:
        down_got = after(down_got, [chip_dq])
        up_got = after(up_got, sent_first[2:])
        own_down = level_total(down_held, down_got, down_level)
        own_up = level_total(up_held, up_got, up_level)
    else:
        own_down = lax.psum_scatter(grad_down, "shard", scatter_dimension=1, tiled=True)
        own_up = lax.psum_scatter(grad_up[None], "shard", scatter_dimension=1, tiled=True)
    activ_late, after_late = after((activ, after_cross), sent_first[2:] if staged else [grad_chip])
    mixed_both = matmul(activ_late[:, :quarter], half_down[0]) + matmul(
        activ_late[:, quarter:], half_down[1]
    )
    y_got = swap(mixed_both[tok_rows:].astype(LOW), "rep", lambda i: i ^ 1)
    if staged:
        q_both = after(q_both, [sums, low_sum])
        q_got = level_sends(q_both, q_level, sent_last)
    text_whole = after(text_whole, sent_last)
    key_round, value_round = (
        text_whole[:, :flat_rows],
        text_whole[:, flat_rows : 2 * flat_rows],
    )
    col_start = lax.axis_index("shard") * shard_rows
    text_flat = text_states.reshape(flat_rows, model_width)
    text_slice = lax.dynamic_slice_in_dim(text_flat, col_start, shard_rows, 1)

    def mixed_dims(left, right):
        return lax.dot_general(
            left, right, (((0,), (1,)), ((), ())), preferred_element_type=WIDE
        )

    grad_xkey = mixed_dims(text_slice, key_round)
    grad_xvalue = mixed_dims(text_slice, value_round)
    grad_text = mixed_dims(key_round, full_xkey) + mixed_dims(value_round, full_xvalue)
    grad_text = grad_text.reshape(clip_total, text_rows, model_width)
    filler = sent_last + [grad_text, grad_xkey, grad_xvalue] if staged else []
    if staged:
        q_own = level_total(q_both, q_got, q_level)
        parts = rep_rows(q_own).reshape(2, shard_rows, 3 * half_width)
        q_swapped = swap(pick(parts, 1 - q_core, 0), "shard", lambda i: i ^ 1)
        fin_query, fin_key, fin_value = unpack(pick(parts, q_core, 0), q_swapped)
        x_own = level_total(x_both, after(x_got, sent_first[2:] + [own_down, own_up, mixed_both]), x_level)
        fin_x = rep_rows(x_own, filler)
    else:
        filled = joined([grad_pair, grad_wq])
        fin_halves = plain_rows([core_pair(filled, jnp.zeros_like(filled), core, 1)])
        fin_x = plain_rows([grad.astype(LOW) for grad in (grad_xoutput, grad_xquery, grad_output)])
        fin_halves = fin_halves.astype(WIDE).reshape(shard_rows, 2, 3 * half_width)
        fin_pair = fin_halves[:, :, :model_width].reshape(shard_rows, 2, pairs, 2, 2 * HD)
        fin_query = fin_halves[:, :, model_width:].reshape(w_query.shape)
        fin_key = fin_pair[:, :, :, 0].reshape(w_query.shape)
        fin_value = fin_pair[:, :, :, 1].reshape(w_query.shape)
    fin_xoutput, fin_xquery, fin_output = (
        fin_x[:, i * model_width : (i + 1) * model_width].astype(WIDE) for i in range(3)
    )
    down_halves = rep_pair(own_down, filler)
    fin_down = jnp.concatenate(down_halves, axis=0).reshape(w_down.shape).astype(WIDE)
    other_up = swap(own_up, "rep", lambda i: i ^ 1)
    own_up, other_up = after((own_up, other_up), filler)
    fin_up = interleave(own_up[0], other_up[0], shard_count, chunk)
    y_own, y_got, after_late = after((mixed_both[:tok_rows], y_got, after_late), sent_last)
    block_out = (after_late + y_own + y_got.astype(WIDE)).astype(LOW)
    back = swap(sums[1], BOTH, lambda i: i ^ 2).astype(WIDE)
    back_half = swap(low_sum, BOTH, lambda i: i ^ 2 if i % 2 == 1 else -1)
    to_below = (
        sums[0].astype(WIDE) + jnp.where(side == 0, back_half.astype(WIDE), back)
    ).astype(LOW)
    down_part = swap(to_below, BOTH, lambda i: i - 4)
    far_part = swap(back_half, BOTH, lambda i: i - 8 if i % 4 == 3 else -1)
    if staged:
        down_part, far_part = after((down_part, far_part), [q_own])
    grad_norm_one = (
        sums[2].astype(WIDE)
        + jnp.where(side == 0, back, 0.0)
        + down_part.astype(WIDE)
        + far_part.astype(WIDE)
    )
    norm_one_part, _, _ = norm_back(resid, gain_one, grad_norm_one)
    grad_gain_one, grad_bias_one = around_sums
    grad_hidden = (grad_self_res + norm_one_part).astype(LOW)
    vectors = lax.all_gather(
        jnp.stack(
            [
                grad_gain_one,
                grad_bias_one,
                grad_gain_two,
                grad_bias_two,
                grad_gain_three,
                grad_bias_three,
            ]
        ).astype(LOW),
        BOTH,
    )
    vectors = after(vectors, [to_below, fin_query])
    vectors = jnp.sum(vectors.astype(WIDE), axis=0)
    fin_gain_one, fin_bias_one, fin_gain_two, fin_bias_two, fin_gain_three, fin_bias_three = (
        lax.dynamic_slice_in_dim(vectors, col_start, shard_rows, 1)
    )
    return (
        block_out,
        grad_hidden,
        grad_text,
        fin_gain_one,
        fin_bias_one,
        fin_query,
        fin_key,
        fin_value,
        fin_output,
        fin_gain_two,
        fin_bias_two,
        fin_xquery,
        grad_xkey,
        grad_xvalue,
        fin_xoutput,
        fin_gain_three,
        fin_bias_three,
        fin_up,
        fin_down,
    )


def solution(mesh):
    rows, vector, tokens = P("shard", None), P("shard"), P(BOTH, None)
    placed = (
        (tokens, P(), P(BOTH), P(BOTH))
        + (vector, vector, rows, rows, rows, rows)
        + (vector, vector, rows, rows, rows, rows)
        + (vector, vector, rows, rows, tokens)
    )
    return jax.shard_map(
        on_device,
        mesh=mesh,
        in_specs=placed,
        out_specs=(
            (tokens, tokens, P())
            + (vector, vector, rows, rows, rows, rows)
            + (vector, vector, rows, rows, rows, rows)
            + (vector, vector, rows, rows)
        ),
        check_vma=False,
    )
```
